8 devices in a mesh: replica: 1 (over z), data: 2 (over y), model: 4 (over x, core).
Axes of the slice: x: 2, y: 2, z: 1, core: 2. Of those that a mesh axis runs over, the one named last changes fastest.
Arguments:
- x_in: bfloat16 [16384, 512], P(('replica', 'data'))
- w_in: bfloat16 [512, 512], P(('replica', 'model'))
- w_mid: bfloat16 [512, 512], P(('replica', 'model'))
- w_out: bfloat16 [512, 512], P(('replica', 'model'))
- u_in: float32 [512], P(('replica', 'model'))
- u_mid: float32 [512], P(('replica', 'model'))
- u_out: float32 [512], P(('replica', 'model'))
- target: bfloat16 [16384, 512], P(('replica', 'data'), 'model')
Outputs:
- output 1: float32 [1], P('replica')
- output 2: bfloat16 [16384, 512], P(('replica', 'data'))
- output 3: float32 [512, 512], P(('replica', 'model'))
- output 4: float32 [512, 512], P(('replica', 'model'))
- output 5: float32 [512, 512], P(('replica', 'model'))
- output 6: float32 [512], P(('replica', 'model'))
- output 7: float32 [512], P(('replica', 'model'))
- output 8: float32 [512], P(('replica', 'model'))
- output 9: float32 [512], P('replica')
- output 10: float32 [512], P('replica')
- output 11: float32 [512], P('replica')
- output 12: float32 [3], P('replica')
All inputs are finite; a program needn't handle non-finite values.
Results may differ from the reference program's by a relative error of at most 0.0166482.
Values are sent between devices in bfloat16 or wider.
A program may use at most 1 GiB of HBM per device.

```python
import jax
import jax.numpy as jnp

MODEL_DIM = 512
HIDDEN_DIM = 512
BATCH_ROWS = 16384


def draw_weight(key_w, rows_out, cols_in):
    key_bulk, key_left, key_right = jax.random.split(key_w, 3)
    bulk_part = jax.random.normal(key_bulk, (rows_out, cols_in), jnp.float32) * cols_in ** -0.5
    left_vec = jax.random.normal(key_left, (rows_out,), jnp.float32)
    left_vec = left_vec / jnp.sqrt(jnp.sum(left_vec * left_vec))
    right_vec = jax.random.normal(key_right, (cols_in,), jnp.float32)
    right_vec = right_vec / jnp.sqrt(jnp.sum(right_vec * right_vec))
    strength = 1.5 * (1.0 + (rows_out / cols_in) ** 0.5)
    weight = bulk_part + strength * left_vec[:, None] * right_vec[None, :]
    return weight.astype(jnp.bfloat16), left_vec


def draw_u(key_u, left_vec, cosine):
    other_vec = jax.random.normal(key_u, left_vec.shape, jnp.float32)
    other_vec = other_vec - jnp.sum(other_vec * left_vec) * left_vec
    other_vec = other_vec / jnp.sqrt(jnp.sum(other_vec * other_vec))
    return cosine * left_vec + (1.0 - cosine * cosine) ** 0.5 * other_vec


def power_step(weight, u_vec):
    w_full = weight.astype(jnp.float32)
    p_vec = jnp.dot(u_vec, w_full)
    v_vec = p_vec / jnp.maximum(jnp.sqrt(jnp.sum(p_vec * p_vec)), 1e-12)
    s_vec = jnp.dot(w_full, v_vec)
    sigma_val = jnp.sqrt(jnp.sum(s_vec * s_vec))
    return s_vec / sigma_val, v_vec, sigma_val


def forward_stack(x_in, weights, u_vecs):
    saved_in = []
    saved_out = []
    layer_stats = []
    for layer_idx in range(3):
        if layer_idx == 0:
            layer_in = x_in
        else:
            layer_in = jax.nn.leaky_relu(saved_out[-1], 0.2).astype(jnp.bfloat16)
        u_next, v_vec, sigma_val = power_step(weights[layer_idx], u_vecs[layer_idx])
        y_val = jnp.dot(layer_in, weights[layer_idx].T, preferred_element_type=jnp.float32) / sigma_val
        saved_in.append(layer_in)
        saved_out.append(y_val)
        layer_stats.append((u_next, v_vec, sigma_val))
    return saved_in, saved_out, layer_stats


def setup_inputs(seed: int = 0, part: int = 0) -> dict:
    key_part = jax.random.fold_in(jax.random.key(seed), part)
    key_list = jax.random.split(key_part, 8)
    w_in, left_in = draw_weight(key_list[0], HIDDEN_DIM, MODEL_DIM)
    w_mid, left_mid = draw_weight(key_list[1], HIDDEN_DIM, HIDDEN_DIM)
    w_out, left_out = draw_weight(key_list[2], MODEL_DIM, HIDDEN_DIM)
    u_in = draw_u(key_list[3], left_in, 0.65)
    u_mid = draw_u(key_list[4], left_mid, 0.7)
    u_out = draw_u(key_list[5], left_out, 0.6)
    x_in = jax.random.normal(key_list[6], (BATCH_ROWS, MODEL_DIM), jnp.float32).astype(jnp.bfloat16)
    y_last = forward_stack(x_in, [w_in, w_mid, w_out], [u_in, u_mid, u_out])[1][2]
    y_scale = jnp.sqrt(jnp.mean(y_last * y_last))
    noise_part = jax.random.normal(key_list[7], (BATCH_ROWS, MODEL_DIM), jnp.float32)
    target = (0.6 * y_last + 0.8 * y_scale * noise_part).astype(jnp.bfloat16)
    return {"x_in": x_in, "w_in": w_in, "w_mid": w_mid, "w_out": w_out, "u_in": u_in, "u_mid": u_mid, "u_out": u_out, "target": target}


def reference(x_in, w_in, w_mid, w_out, u_in, u_mid, u_out, target):
    weights = [w_in, w_mid, w_out]
    saved_in, saved_out, layer_stats = forward_stack(x_in, weights, [u_in, u_mid, u_out])
    residual = saved_out[2] - target.astype(jnp.float32)
    loss_val = 0.5 / BATCH_ROWS * jnp.sum(residual * residual)
    grad_y = residual / BATCH_ROWS
    grads_w = [None, None, None]
    for layer_idx in (2, 1, 0):
        u_next, v_vec, sigma_val = layer_stats[layer_idx]
        grad_b = grad_y.astype(jnp.bfloat16)
        corr_sum = jnp.sum(grad_y * saved_out[layer_idx])
        g_mat = jnp.dot(grad_b.T, saved_in[layer_idx], preferred_element_type=jnp.float32)
        grads_w[layer_idx] = g_mat / sigma_val - (corr_sum / sigma_val) * jnp.outer(u_next, v_vec)
        grad_x = (jnp.dot(grad_b, weights[layer_idx], preferred_element_type=jnp.float32) / sigma_val).astype(jnp.bfloat16)
        if layer_idx > 0:
            grad_y = grad_x.astype(jnp.float32) * jnp.where(saved_out[layer_idx - 1] > 0, 1.0, 0.2)
    return (loss_val.reshape(1), grad_x, grads_w[0], grads_w[1], grads_w[2],
            layer_stats[0][0], layer_stats[1][0], layer_stats[2][0],
            layer_stats[0][1], layer_stats[1][1], layer_stats[2][1],
            jnp.stack([layer_stats[0][2], layer_stats[1][2], layer_stats[2][2]]))
```

```python
import functools

import jax
import jax.numpy as jnp
from jax import lax
from jax.experimental import pallas as pl
from jax.experimental.pallas import tpu as pltpu
from jax.sharding import PartitionSpec as P

MESH = pl.DeviceIdType.MESH
F32 = jnp.float32
BF16 = jnp.bfloat16
NT = 16


def dot_nt(lhs, rhs):
    return lax.dot_general(lhs, rhs, (((1,), (1,)), ((), ())), preferred_element_type=F32)


def dot_nn(lhs, rhs):
    return lax.dot_general(lhs, rhs, (((1,), (0,)), ((), ())), preferred_element_type=F32)


def dot_tn(lhs, rhs):
    return lax.dot_general(lhs, rhs, (((0,), (0,)), ((), ())), preferred_element_type=F32)


def split_rows(vec):
    width = vec.shape[1]
    high = vec.astype(BF16).astype(F32)
    rest = vec - high
    mid = rest.astype(BF16).astype(F32)
    low = rest - mid
    row = lax.broadcasted_iota(jnp.int32, (16, width), 0)
    stacked = jnp.where(row == 0, high, jnp.where(row == 1, mid, jnp.where(row == 2, low, 0.0)))
    return stacked.astype(BF16)


def main_kernel(inv_batch, x_hbm, w0_hbm, w1_hbm, w2_hbm, u0_hbm, u1_hbm, u2_hbm, t_hbm,
                e_out, w_out, dw_out, v0_out, v1_out, v2_out, n0_out, n1_out, n2_out, sig_out,
                x0, x1, x2, y0, y1, y2, tbuf, wbuf, ubuf, ebuf, estage, acc, rbuf, stat, rstat, sstat, srow,
                w_send, w_recv, u_send, u_recv, t_send, t_recv, e_send, e_recv, d_send, d_recv,
                l_w, l_u, l_t, l_x, l_e, l_o):
    rep, dat, mod = lax.axis_index("replica"), lax.axis_index("data"), lax.axis_index("model")
    core = lax.rem(mod, 2)
    chip = mod // 2
    sib = mod + 1 - 2 * core
    cnt = lax.rem(mod + 2, 4)
    crs = lax.rem(sib + 2, 4)
    peers = [(rep, dat, sib), (rep, dat, cnt), (rep, dat, crs)]
    rows_own = x0.shape[0]
    chunk = rows_own // NT
    row_base = core * rows_own
    w_hbm = [w0_hbm, w1_hbm, w2_hbm]
    u_hbm = [u0_hbm, u1_hbm, u2_hbm]
    xs = [x0, x1, x2]
    ys = [y0, y1, y2]
    v_outs = [v0_out, v1_out, v2_out]
    n_outs = [n0_out, n1_out, n2_out]

    def remote(src, dst, ssem, rsem, peer):
        return pltpu.make_async_remote_copy(src_ref=src, dst_ref=dst, send_sem=ssem, recv_sem=rsem,
                                            device_id=peer, device_id_type=MESH)

    def wrow(idx):
        return pl.ds(pl.multiple_of(idx * 128, 128), 128)

    def w_copy(layer, kind):
        if kind == 2:
            src = wbuf.at[layer, wrow(cnt)]
            return remote(src, src, w_send.at[layer, 2], w_recv.at[layer, 2], peers[0])
        return remote(w_hbm[layer], wbuf.at[layer, wrow(mod)], w_send.at[layer, kind], w_recv.at[layer, kind], peers[kind])

    def u_copy(layer, kind):
        return remote(u_hbm[layer], ubuf.at[layer, mod], u_send.at[layer, kind], u_recv.at[layer, kind], peers[kind])

    def t_copy(kind, c):
        other_core = core if kind == 1 else 1 - core
        src = t_hbm.at[pl.ds(pl.multiple_of(other_core * rows_own + c * chunk, chunk), chunk)]
        dst = tbuf.at[mod, pl.ds(pl.multiple_of(c * chunk, chunk), chunk)]
        return remote(src, dst, t_send.at[kind, c], t_recv.at[kind, c], peers[kind])

    barrier = pltpu.get_barrier_semaphore()
    for peer in peers:
        pl.semaphore_signal(barrier, inc=1, device_id=peer, device_id_type=MESH)
    local_x = pltpu.make_async_copy(x_hbm.at[pl.ds(pl.multiple_of(row_base, rows_own), rows_own)], x0, l_x)
    local_x.start()
    local_w = [pltpu.make_async_copy(w_hbm[k], wbuf.at[k, wrow(mod)], l_w.at[k]) for k in range(3)]
    local_u = [pltpu.make_async_copy(u_hbm[k], ubuf.at[k, mod], l_u.at[k]) for k in range(3)]
    for k in range(3):
        local_w[k].start()
        local_u[k].start()
    local_t = pltpu.make_async_copy(t_hbm.at[pl.ds(pl.multiple_of(row_base, rows_own), rows_own)], tbuf.at[mod], l_t)
    local_t.start()
    pl.semaphore_wait(barrier, 3)

    for k in range(3):
        for kind in range(3):
            u_copy(k, kind).start()
    for k in range(3):
        w_copy(k, 1).start()
        w_copy(k, 0).start()

    def start_targets(c, carry):
        t_copy(1, c).start()
        t_copy(2, c).start()
        t_copy(0, c).start()
        return carry

    lax.fori_loop(0, NT, start_targets, 0)
    acc[...] = jnp.zeros_like(acc)
    stat[...] = jnp.zeros_like(stat)
    local_x.wait()

    inv_sigma = []
    w_full_copy = pltpu.make_async_copy(wbuf.at[0], w_out, l_o)
    for k in range(3):
        w_copy(k, 1).wait_recv()
        w_copy(k, 2).start()
        local_w[k].wait()
        local_u[k].wait()
        for kind in range(3):
            u_copy(k, kind).wait_recv()
        w_copy(k, 0).wait_recv()
        w_copy(k, 2).wait_recv()
        if k == 0:
            w_full_copy.start()
        u_row = jnp.concatenate([ubuf[k, j] for j in range(4)], axis=1)
        p_vec = jnp.sum(dot_nn(split_rows(u_row), wbuf[k]), axis=0, keepdims=True)
        norm = jnp.sqrt(jnp.sum(p_vec * p_vec, axis=1, keepdims=True))
        v_vec = p_vec / jnp.maximum(norm, 1e-12)
        s_vec = jnp.sum(dot_nt(split_rows(v_vec), wbuf[k]), axis=0, keepdims=True)
        sigma = jnp.sqrt(jnp.sum(s_vec * s_vec, axis=1, keepdims=True))
        v_outs[k][...] = v_vec
        srow[k] = jnp.broadcast_to(s_vec / sigma, srow.shape[1:])
        n_outs[k][...] = srow[k, 0:1, wrow(mod)]
        sig_out[k:k + 1, :] = jnp.broadcast_to(sigma, (1, 128))
        inv = 1.0 / sigma
        inv_sigma.append(inv)

        def forward(c, carry, k=k, inv=inv):
            rows = pl.ds(pl.multiple_of(c * chunk, chunk), chunk)
            y_val = dot_nt(xs[k][rows, :], wbuf[k]) * inv
            ys[k][rows, :] = y_val
            if k < 2:
                xs[k + 1][rows, :] = jnp.maximum(y_val, 0.2 * y_val).astype(BF16)
            return carry

        lax.fori_loop(0, NT, forward, 0)

    local_t.wait()
    own_cols = pl.ds(pl.multiple_of(chip * 256, 256), 256)

    def fold(val):
        return jnp.sum(val.reshape(val.shape[0] // 8, 8, val.shape[1]), axis=0)

    def add_grad(k, rows):
        part = dot_tn(ebuf[k, :, own_cols], xs[k][rows, :])
        acc[k, 0] += part[:128]
        acc[k, 1] += part[128:]

    def e_local(c):
        rows = pl.ds(pl.multiple_of(c * chunk, chunk), chunk)
        out_rows = pl.ds(pl.multiple_of(row_base + c * chunk, chunk), chunk)
        return pltpu.make_async_copy(estage.at[rows], e_out.at[out_rows], l_e.at[c])

    def e_remote(c):
        rows = pl.ds(pl.multiple_of(c * chunk, chunk), chunk)
        out_rows = pl.ds(pl.multiple_of(row_base + c * chunk, chunk), chunk)
        return remote(estage.at[rows], e_out.at[out_rows], e_send.at[c], e_recv.at[c], peers[0])

    def backward(c, carry):
        rows = pl.ds(pl.multiple_of(c * chunk, chunk), chunk)
        for kind in range(3):
            t_copy(kind, c).wait_recv()
        for j in range(4):
            cols = slice(128 * j, 128 * j + 128)
            y_val = y2[rows, cols]
            res = y_val - tbuf[j, rows, :].astype(F32)
            grad = res * inv_batch
            stat[0, :, cols] += fold(res * res)
            stat[1, :, cols] += fold(grad * y_val)
            ebuf[2, :, cols] = grad.astype(BF16)
        for k in (2, 1):
            back = (dot_nn(ebuf[k], wbuf[k]) * inv_sigma[k]).astype(BF16).astype(F32)
            y_val = ys[k - 1][rows, :]
            grad = back * jnp.where(y_val > 0, 1.0, 0.2)
            stat[4 - k] += fold(grad * y_val)
            e_val = grad.astype(BF16)
            ebuf[k - 1] = e_val
            if k == 1:
                estage[rows, :] = e_val
            add_grad(k, rows)
        add_grad(0, rows)
        e_local(c).start()
        e_remote(c).start()
        return carry

    lax.fori_loop(0, NT, backward, 0)

    row = lax.broadcasted_iota(jnp.int32, sstat.shape, 0)
    mine = jnp.zeros(sstat.shape, F32)
    for i in range(4):
        mine = jnp.where(row == i, jnp.sum(stat[i], axis=0, keepdims=True), mine)
    sstat[...] = mine
    d_copies = [remote(acc.at[k, 1 - core], rbuf.at[k], d_send.at[k], d_recv.at[k], peers[0]) for k in range(3)]
    d_copies.append(remote(sstat, rstat, d_send.at[3], d_recv.at[3], peers[0]))
    for copy in d_copies:
        copy.start()
    for k in range(3):
        d_copies[k].wait_recv()
        dw_out[128 * k:128 * k + 128, :] = acc[k, core] + rbuf[k]
    d_copies[3].wait_recv()
    dw_out[384:392, :] = sstat[...] + rstat[...]

    for copy in d_copies:
        copy.wait_send()

    def drain(c, carry):
        for kind in range(3):
            t_copy(kind, c).wait_send()
        e_local(c).wait()
        e_remote(c).wait_send()
        e_remote(c).wait_recv()
        return carry

    lax.fori_loop(0, NT, drain, 0)
    for k in range(3):
        for kind in range(3):
            w_copy(k, kind).wait_send()
            u_copy(k, kind).wait_send()
    w_full_copy.wait()


def solution(mesh):
    data_size = mesh.shape["data"]
    row_spec = P(("replica", "model"), None)
    vec_spec = P(("replica", "model"))
    batch_spec = P(("replica", "data"), None)
    target_spec = P(("replica", "data"), "model")
    part_spec = P("replica")

    def local_step(x_in, w_in, w_mid, w_out, u_in, u_mid, u_out, target):
        rows, width = x_in.shape
        half = rows // 2
        chunk = half // NT
        batch_total = rows * data_size
        any_spec = pl.BlockSpec(memory_space=pl.ANY)
        vmem_spec = pl.BlockSpec(memory_space=pltpu.VMEM)
        dma = pltpu.SemaphoreType.DMA
        outs = pl.pallas_call(
            functools.partial(main_kernel, 1.0 / batch_total),
            out_shape=[
                jax.ShapeDtypeStruct((rows, width), BF16),
                jax.ShapeDtypeStruct((width, width), BF16),
                jax.ShapeDtypeStruct((392, width), F32),
            ] + [jax.ShapeDtypeStruct((1, width), F32)] * 3 + [jax.ShapeDtypeStruct((1, 128), F32)] * 3 + [
                jax.ShapeDtypeStruct((8, 128), F32)],
            in_specs=[any_spec] * 8,
            out_specs=[any_spec] * 2 + [vmem_spec] * 8,
            scratch_shapes=[pltpu.VMEM((half, width), BF16)] * 3 + [pltpu.VMEM((half, width), F32)] * 3 + [
                pltpu.VMEM((4, half, 128), BF16),
                pltpu.VMEM((3, width, width), BF16),
                pltpu.VMEM((3, 4, 1, 128), F32),
                pltpu.VMEM((3, chunk, width), BF16),
                pltpu.VMEM((half, width), BF16),
                pltpu.VMEM((3, 2, 128, width), F32),
                pltpu.VMEM((3, 128, width), F32),
                pltpu.VMEM((4, 8, width), F32),
                pltpu.VMEM((8, width), F32),
                pltpu.VMEM((8, width), F32),
                pltpu.VMEM((3, 8, width), F32),
                dma((3, 3)), dma((3, 3)), dma((3, 3)), dma((3, 3)),
                dma((3, NT)), dma((3, NT)), dma((NT,)), dma((NT,)), dma((4,)), dma((4,)),
                dma((3,)), dma((3,)), dma(()), dma(()), dma((NT,)), dma(()),
            ],
            compiler_params=pltpu.CompilerParams(
                collective_id=0, has_side_effects=True, vmem_limit_bytes=63 * 2**20),
            name="fused_step",
        )(x_in, w_in, w_mid, w_out, u_in.reshape(1, 128), u_mid.reshape(1, 128), u_out.reshape(1, 128), target)
        e_all, w_full, dw_part = outs[:3]
        v_vecs, u_next, sig = outs[3:6], outs[6:9], outs[9][:3, 0]
        other = lax.ppermute(dw_part, "data", [(0, 1), (1, 0)])
        grad_x = (jnp.dot(e_all, w_full, preferred_element_type=F32) / sig[0]).astype(BF16)
        total = dw_part + other
        sums = jnp.sum(total[384:388], axis=1)
        loss_val = 0.5 / batch_total * sums[0]
        grads_w = []
        for k in range(3):
            corr = sums[3 - k]
            grads_w.append(total[128 * k:128 * k + 128] / sig[k] - (corr / sig[k]) * (u_next[k].reshape(128, 1) * v_vecs[k]))
        return (loss_val.reshape(1), grad_x, grads_w[0], grads_w[1], grads_w[2],
                u_next[0].reshape(128), u_next[1].reshape(128), u_next[2].reshape(128),
                v_vecs[0].reshape(width), v_vecs[1].reshape(width), v_vecs[2].reshape(width), sig)

    in_specs = (batch_spec, row_spec, row_spec, row_spec, vec_spec, vec_spec, vec_spec, target_spec)
    out_specs = (part_spec, batch_spec, row_spec, row_spec, row_spec, vec_spec, vec_spec, vec_spec, part_spec, part_spec, part_spec, part_spec)
    return jax.shard_map(local_step, mesh=mesh, in_specs=in_specs, out_specs=out_specs, check_vma=False)
```

```python
import functools

import jax
import jax.numpy as jnp
from jax import lax
from jax.experimental import pallas as pl
from jax.experimental.pallas import tpu as pltpu
from jax.sharding import PartitionSpec as P

MESH = pl.DeviceIdType.MESH
F32 = jnp.float32
BF16 = jnp.bfloat16
NT = 16
NF = 4


def dot_nt(lhs, rhs):
    return lax.dot_general(lhs, rhs, (((1,), (1,)), ((), ())), preferred_element_type=F32)


def dot_nn(lhs, rhs):
    return lax.dot_general(lhs, rhs, (((1,), (0,)), ((), ())), preferred_element_type=F32)


def dot_tn(lhs, rhs):
    return lax.dot_general(lhs, rhs, (((0,), (0,)), ((), ())), preferred_element_type=F32)


def split_rows(vec):
    width = vec.shape[1]
    high = vec.astype(BF16).astype(F32)
    rest = vec - high
    mid = rest.astype(BF16).astype(F32)
    low = rest - mid
    row = lax.broadcasted_iota(jnp.int32, (16, width), 0)
    stacked = jnp.where(row == 0, high, jnp.where(row == 1, mid, jnp.where(row == 2, low, 0.0)))
    return stacked.astype(BF16)


def main_kernel(inv_batch, x_hbm, w0_hbm, w1_hbm, w2_hbm, u0_hbm, u1_hbm, u2_hbm, t_hbm,
                e_out, w_out, dw_out, g2_out, v0_out, v1_out, v2_out, n0_out, n1_out, n2_out, sig_out,
                x0, x1, x2, y0, y1, y2, tbuf, wbuf, ubuf, e2, e1, e0, acc, rbuf, g2own, g2other, stat, rstat, sstat, srow,
                w_send, w_recv, u_send, u_recv, t_send, t_recv, s_send, s_recv, e_send, e_recv, d_send, d_recv, g_send, g_recv,
                l_w, l_u, l_t, l_x, l_e, l_o):
    rep, dat, mod = lax.axis_index("replica"), lax.axis_index("data"), lax.axis_index("model")
    core = lax.rem(mod, 2)
    chip = mod // 2
    sib = mod + 1 - 2 * core
    cnt = lax.rem(mod + 2, 4)
    crs = lax.rem(sib + 2, 4)
    p_sib, p_cnt, p_crs, p_y = (rep, dat, sib), (rep, dat, cnt), (rep, dat, crs), (rep, 1 - dat, mod)
    rows_own = x0.shape[0]
    chunk = rows_own // NT
    fwd_chunk = rows_own // NF
    row_base = core * rows_own
    w_hbm = [w0_hbm, w1_hbm, w2_hbm]
    u_hbm = [u0_hbm, u1_hbm, u2_hbm]
    xs = [x0, x1, x2]
    ys = [y0, y1, y2]
    es = [e0, e1, e2]
    v_outs = [v0_out, v1_out, v2_out]
    n_outs = [n0_out, n1_out, n2_out]

    def remote(src, dst, ssem, rsem, peer):
        return pltpu.make_async_remote_copy(src_ref=src, dst_ref=dst, send_sem=ssem, recv_sem=rsem,
                                            device_id=peer, device_id_type=MESH)

    def span(start, size):
        return pl.ds(pl.multiple_of(start, size), size)

    def w_copy(layer, kind):
        ssem, rsem = w_send.at[layer, kind], w_recv.at[layer, kind]
        if kind == 0:
            return remote(w_hbm[layer], wbuf.at[layer, span(128 * mod, 128)], ssem, rsem, p_sib)
        if kind == 1:
            return remote(w_hbm[layer].at[span(64 * dat, 64)], wbuf.at[layer, span(128 * mod + 64 * dat, 64)], ssem, rsem, p_cnt)
        half = 1 - dat if kind == 4 else dat
        ref = wbuf.at[layer, span(128 * cnt + 64 * half, 64)]
        return remote(ref, ref, ssem, rsem, p_y if kind == 2 else p_sib)

    def u_copy(layer, kind):
        return remote(u_hbm[layer], ubuf.at[layer, mod], u_send.at[layer, kind], u_recv.at[layer, kind],
                      (p_sib, p_cnt, p_crs)[kind])

    def t_copy(kind, c):
        other_core = core if kind == 0 else 1 - core
        return remote(t_hbm.at[span(other_core * rows_own + c * chunk, chunk)], tbuf.at[mod, span(c * chunk, chunk)],
                      t_send.at[kind, c], t_recv.at[kind, c], p_cnt if kind == 0 else p_crs)

    barrier = pltpu.get_barrier_semaphore()
    for peer in (p_sib, p_cnt, p_crs, p_y):
        pl.semaphore_signal(barrier, inc=1, device_id=peer, device_id_type=MESH)
    local_x = pltpu.make_async_copy(x_hbm.at[span(row_base, rows_own)], x0, l_x)
    local_w = [pltpu.make_async_copy(w_hbm[k], wbuf.at[k, span(128 * mod, 128)], l_w.at[k]) for k in range(3)]
    local_u = [pltpu.make_async_copy(u_hbm[k], ubuf.at[k, mod], l_u.at[k]) for k in range(3)]
    local_t = pltpu.make_async_copy(t_hbm.at[span(row_base, rows_own)], tbuf.at[mod], l_t)
    for k in range(3):
        local_w[k].start()
        local_u[k].start()
    local_x.start()
    local_t.start()
    pl.semaphore_wait(barrier, 4)

    for k in range(3):
        w_copy(k, 1).start()
        w_copy(k, 0).start()
        for kind in range(3):
            u_copy(k, kind).start()

    def start_targets(c, carry):
        t_copy(0, c).start()
        t_copy(1, c).start()
        return carry

    lax.fori_loop(0, NT, start_targets, 0)
    t_sib = remote(t_hbm.at[span((1 - core) * rows_own, rows_own)], tbuf.at[mod], s_send, s_recv, p_sib)
    t_sib.start()
    acc[...] = jnp.zeros_like(acc)
    stat[...] = jnp.zeros_like(stat)

    def relay_x(k):
        w_copy(k, 1).wait_recv()
        w_copy(k, 2).start()
        w_copy(k, 3).start()

    def relay_y(k):
        w_copy(k, 2).wait_recv()
        w_copy(k, 4).start()

    own_cols = span(256 * chip, 256)

    def fold(val):
        return jnp.sum(val.reshape(val.shape[0] // 8, 8, val.shape[1]), axis=0)

    def add_grad(k, rows):
        part = dot_tn(es[k][rows, own_cols], xs[k][rows, :])
        acc[k, 0] += part[:128]
        acc[k, 1] += part[128:]

    def residual(slab, rows):
        cols = span(128 * slab, 128)
        y_val = y2[rows, cols]
        res = y_val - tbuf[slab, rows, :].astype(F32)
        grad = res * inv_batch
        stat[0, :, cols] += fold(res * res)
        stat[1, :, cols] += fold(grad * y_val)
        e2[rows, cols] = grad.astype(BF16)

    inv_sigma = []
    w_full_copy = pltpu.make_async_copy(wbuf.at[0], w_out, l_o)
    relay_x(0)
    relay_y(0)
    for k in range(3):
        local_w[k].wait()
        local_u[k].wait()
        for kind in range(3):
            u_copy(k, kind).wait_recv()
        for kind in (0, 3, 4):
            w_copy(k, kind).wait_recv()
        if k == 0:
            w_full_copy.start()
        u_row = jnp.concatenate([ubuf[k, j] for j in range(4)], axis=1)
        p_vec = jnp.sum(dot_nn(split_rows(u_row), wbuf[k]), axis=0, keepdims=True)
        norm = jnp.sqrt(jnp.sum(p_vec * p_vec, axis=1, keepdims=True))
        v_vec = p_vec / jnp.maximum(norm, 1e-12)
        s_vec = jnp.sum(dot_nt(split_rows(v_vec), wbuf[k]), axis=0, keepdims=True)
        sigma = jnp.sqrt(jnp.sum(s_vec * s_vec, axis=1, keepdims=True))
        v_outs[k][...] = v_vec
        srow[k] = jnp.broadcast_to(s_vec / sigma, srow.shape[1:])
        n_outs[k][...] = srow[k, 0:1, span(128 * mod, 128)]
        sig_out[k:k + 1, :] = jnp.broadcast_to(sigma, (1, 128))
        inv = 1.0 / sigma
        inv_sigma.append(inv)
        if k < 2:
            relay_x(k + 1)
            relay_y(k + 1)
        if k == 0:
            local_x.wait()
        if k == 2:
            local_t.wait()
            t_sib.wait_recv()

        def forward(c, carry, k=k, inv=inv):
            rows = span(c * fwd_chunk, fwd_chunk)
            y_val = dot_nt(xs[k][rows, :], wbuf[k]) * inv
            ys[k][rows, :] = y_val
            if k < 2:
                xs[k + 1][rows, :] = jnp.maximum(y_val, 0.2 * y_val).astype(BF16)
            else:
                for j in range(2):
                    residual(2 * chip + j, rows)
                add_grad(2, rows)
            return carry

        lax.fori_loop(0, NF, forward, 0)

    def d_copy(k):
        return remote(acc.at[k, 1 - core], rbuf.at[k], d_send.at[k], d_recv.at[k], p_sib)

    g_copy = remote(g2own, g2other, g_send, g_recv, p_y)

    def e_local(c):
        return pltpu.make_async_copy(e0.at[span(c * chunk, chunk)], e_out.at[span(row_base + c * chunk, chunk)], l_e.at[c])

    def e_remote(c):
        return remote(e0.at[span(c * chunk, chunk)], e_out.at[span(row_base + c * chunk, chunk)], e_send.at[c], e_recv.at[c], p_sib)

    def backward(c, carry):
        @pl.when(c == 1)
        def _():
            d_copy(2).start()

        @pl.when(c == 3)
        def _():
            d_copy(2).wait_recv()
            g2own[...] = acc[2, core] + rbuf[2]

        @pl.when(c == 4)
        def _():
            g_copy.start()

        rows = span(c * chunk, chunk)
        for kind in range(2):
            t_copy(kind, c).wait_recv()
        for j in range(2):
            residual(2 - 2 * chip + j, rows)
        for k in (2, 1):
            back = (dot_nn(es[k][rows, :], wbuf[k]) * inv_sigma[k]).astype(BF16).astype(F32)
            y_val = ys[k - 1][rows, :]
            grad = back * jnp.where(y_val > 0, 1.0, 0.2)
            stat[4 - k] += fold(grad * y_val)
            es[k - 1][rows, :] = grad.astype(BF16)
            add_grad(k - 1, rows)
        e_local(c).start()
        e_remote(c).start()
        return carry

    lax.fori_loop(0, NT, backward, 0)

    d_copy(1).start()
    row = lax.broadcasted_iota(jnp.int32, sstat.shape, 0)
    mine = jnp.zeros(sstat.shape, F32)
    for i in range(4):
        mine = jnp.where(row == i, jnp.sum(stat[i], axis=0, keepdims=True), mine)
    sstat[...] = mine
    d_copy(0).start()
    s_copy = remote(sstat, rstat, d_send.at[3], d_recv.at[3], p_sib)
    s_copy.start()
    g_copy.wait_recv()
    g2_out[...] = g2own[...] + g2other[...]
    for i, k in enumerate((1, 0)):
        d_copy(k).wait_recv()
        dw_out[128 * i:128 * i + 128, :] = acc[k, core] + rbuf[k]
    s_copy.wait_recv()
    dw_out[256:264, :] = sstat[...] + rstat[...]

    for k in range(3):
        d_copy(k).wait_send()
    s_copy.wait_send()
    g_copy.wait_send()
    t_sib.wait_send()

    def drain(c, carry):
        for kind in range(2):
            t_copy(kind, c).wait_send()
        e_local(c).wait()
        e_remote(c).wait_send()
        e_remote(c).wait_recv()
        return carry

    lax.fori_loop(0, NT, drain, 0)
    for k in range(3):
        for kind in range(5):
            w_copy(k, kind).wait_send()
        for kind in range(3):
            u_copy(k, kind).wait_send()
    w_full_copy.wait()


def dx_kernel(e_ref, w_ref, sig_ref, v0, v1, v2, n0, n1, n2, dx_ref, v0_out, v1_out, v2_out, n0_out, n1_out, n2_out, sig_out):
    inv = 1.0 / sig_ref[0:1, 0:1]
    dx_ref[...] = (dot_nn(e_ref[...], w_ref[...]) * inv).astype(BF16)

    @pl.when(pl.program_id(0) == 0)
    def _():
        for src, dst in ((v0, v0_out), (v1, v1_out), (v2, v2_out), (n0, n0_out), (n1, n1_out), (n2, n2_out)):
            dst[...] = src[...]
        lane = lax.broadcasted_iota(jnp.int32, (1, 128), 1)
        row = jnp.where(lane == 0, sig_ref[0:1, :], jnp.where(lane == 1, sig_ref[1:2, :], sig_ref[2:3, :]))
        sig_out[...] = row[:, :3]


def final_kernel(loss_scale, own, other, g2, sig_ref, v0, v1, v2, n0, n1, n2, dw0, dw1, dw2, loss_out):
    stats = jnp.sum(own[256:264, :] + other[256:264, :], axis=1, keepdims=True)
    loss_out[...] = loss_scale * stats[0:1]
    grads = (own[128:256, :] + other[128:256, :], own[0:128, :] + other[0:128, :], g2[...])
    for k, (grad, v_ref, n_ref, out) in enumerate(zip(grads, (v0, v1, v2), (n0, n1, n2), (dw0, dw1, dw2))):
        inv = 1.0 / sig_ref[k:k + 1, 0:1]
        u_col = jnp.transpose(jnp.broadcast_to(n_ref[...], (128, 128)))[:, 0:1]
        out[...] = grad * inv - (stats[3 - k:4 - k] * inv) * (u_col * v_ref[...])


def solution(mesh):
    data_size = mesh.shape["data"]
    row_spec = P(("replica", "model"), None)
    vec_spec = P(("replica", "model"))
    batch_spec = P(("replica", "data"), None)
    target_spec = P(("replica", "data"), "model")
    part_spec = P("replica")

    def local_step(x_in, w_in, w_mid, w_out, u_in, u_mid, u_out, target):
        rows, width = x_in.shape
        half = rows // 2
        batch_total = rows * data_size
        any_spec = pl.BlockSpec(memory_space=pl.ANY)
        vmem_spec = pl.BlockSpec(memory_space=pltpu.VMEM)
        dma = pltpu.SemaphoreType.DMA
        small = [jax.ShapeDtypeStruct((1, width), F32)] * 3 + [jax.ShapeDtypeStruct((1, 128), F32)] * 3
        outs = pl.pallas_call(
            functools.partial(main_kernel, 1.0 / batch_total),
            out_shape=[
                jax.ShapeDtypeStruct((rows, width), BF16),
                jax.ShapeDtypeStruct((width, width), BF16),
                jax.ShapeDtypeStruct((264, width), F32),
                jax.ShapeDtypeStruct((128, width), F32),
            ] + small + [jax.ShapeDtypeStruct((8, 128), F32)],
            in_specs=[any_spec] * 8,
            out_specs=[any_spec] * 2 + [vmem_spec] * 9,
            scratch_shapes=[pltpu.VMEM((half, width), BF16)] * 3 + [pltpu.VMEM((half, width), F32)] * 3 + [
                pltpu.VMEM((4, half, 128), BF16),
                pltpu.VMEM((3, width, width), BF16),
                pltpu.VMEM((3, 4, 1, 128), F32),
                pltpu.VMEM((half, width), BF16),
                pltpu.VMEM((half, width), BF16),
                pltpu.VMEM((half, width), BF16),
                pltpu.VMEM((3, 2, 128, width), F32),
                pltpu.VMEM((3, 128, width), F32),
                pltpu.VMEM((128, width), F32),
                pltpu.VMEM((128, width), F32),
                pltpu.VMEM((4, 8, width), F32),
                pltpu.VMEM((8, width), F32),
                pltpu.VMEM((8, width), F32),
                pltpu.VMEM((3, 8, width), F32),
                dma((3, 5)), dma((3, 5)), dma((3, 3)), dma((3, 3)),
                dma((2, NT)), dma((2, NT)), dma(()), dma(()), dma((NT,)), dma((NT,)), dma((4,)), dma((4,)), dma(()), dma(()),
                dma((3,)), dma((3,)), dma(()), dma(()), dma((NT,)), dma(()),
            ],
            compiler_params=pltpu.CompilerParams(
                collective_id=0, has_side_effects=True, vmem_limit_bytes=63 * 2**20),
            name="fused_step",
        )(x_in, w_in, w_mid, w_out, u_in.reshape(1, 128), u_mid.reshape(1, 128), u_out.reshape(1, 128), target)
        e_all, w_full, dw_part, g2_sum = outs[:4]
        vecs, sig = outs[4:10], outs[10]
        other = lax.ppermute(dw_part, "data", [(0, 1), (1, 0)])

        block = 1024
        full = lambda shape: pl.BlockSpec(shape, lambda i: (0, 0))
        vec_specs = [full((1, width))] * 3 + [full((1, 128))] * 3
        passed = pl.pallas_call(
            dx_kernel,
            grid=(rows // block,),
            out_shape=[jax.ShapeDtypeStruct((rows, width), BF16)] + small + [jax.ShapeDtypeStruct((1, 3), F32)],
            in_specs=[pl.BlockSpec((block, width), lambda i: (i, 0)), full((width, width)), full((8, 128))] + vec_specs,
            out_specs=[pl.BlockSpec((block, width), lambda i: (i, 0))] + vec_specs + [full((1, 3))],
            cost_estimate=pl.CostEstimate(flops=2 * rows * width * width, bytes_accessed=4 * rows * width, transcendentals=0),
            compiler_params=pltpu.CompilerParams(vmem_limit_bytes=24 * 2**20),
            name="dx",
        )(e_all, w_full, sig, *vecs)
        grad_x, sig_row = passed[0], passed[7]

        finals = pl.pallas_call(
            functools.partial(final_kernel, 0.5 / batch_total),
            out_shape=[jax.ShapeDtypeStruct((128, width), F32)] * 3 + [jax.ShapeDtypeStruct((1, 1), F32)],
            in_specs=[vmem_spec] * 10,
            out_specs=[vmem_spec] * 4,
            compiler_params=pltpu.CompilerParams(vmem_limit_bytes=8 * 2**20),
            name="finish",
        )(dw_part, other, g2_sum, sig, *vecs)
        v_row, u_row = passed[1:4], passed[4:7]
        return (finals[3].reshape(1), grad_x, finals[0], finals[1], finals[2],
                u_row[0].reshape(128), u_row[1].reshape(128), u_row[2].reshape(128),
                v_row[0].reshape(width), v_row[1].reshape(width), v_row[2].reshape(width), sig_row.reshape(3))

    in_specs = (batch_spec, row_spec, row_spec, row_spec, vec_spec, vec_spec, vec_spec, target_spec)
    out_specs = (part_spec, batch_spec, row_spec, row_spec, row_spec, vec_spec, vec_spec, vec_spec, part_spec, part_spec, part_spec, part_spec)
    return jax.shard_map(local_step, mesh=mesh, in_specs=in_specs, out_specs=out_specs, check_vma=False)
```

```python
import functools

import jax
import jax.numpy as jnp
from jax import lax
from jax.experimental import pallas as pl
from jax.experimental.pallas import tpu as pltpu
from jax.sharding import PartitionSpec as P

MESH = pl.DeviceIdType.MESH
F32 = jnp.float32
BF16 = jnp.bfloat16
NT = 16
NF = 4


def dot_nt(lhs, rhs):
    return lax.dot_general(lhs, rhs, (((1,), (1,)), ((), ())), preferred_element_type=F32)


def dot_nn(lhs, rhs):
    return lax.dot_general(lhs, rhs, (((1,), (0,)), ((), ())), preferred_element_type=F32)


def dot_tn(lhs, rhs):
    return lax.dot_general(lhs, rhs, (((0,), (0,)), ((), ())), preferred_element_type=F32)


def split_rows(vec):
    width = vec.shape[1]
    high = vec.astype(BF16).astype(F32)
    rest = vec - high
    mid = rest.astype(BF16).astype(F32)
    low = rest - mid
    row = lax.broadcasted_iota(jnp.int32, (16, width), 0)
    stacked = jnp.where(row == 0, high, jnp.where(row == 1, mid, jnp.where(row == 2, low, 0.0)))
    return stacked.astype(BF16)


def main_kernel(inv_batch, x_hbm, w0_hbm, w1_hbm, w2_hbm, u0_hbm, u1_hbm, u2_hbm, t_hbm,
                e_out, w_out, dw_out, g2_out, pack_out,
                x0, x1, x2, y0, y1, y2, tbuf, wbuf, ubuf, e2, e1, e0, acc, rbuf, g2own, g2other, stat, rstat, sstat, srow,
                w_send, w_recv, u_send, u_recv, t_send, t_recv, s_send, s_recv, e_send, e_recv, d_send, d_recv, g_send, g_recv,
                l_w, l_u, l_t, l_x, l_e, l_o):
    rep, dat, mod = lax.axis_index("replica"), lax.axis_index("data"), lax.axis_index("model")
    core = lax.rem(mod, 2)
    chip = mod // 2
    sib = mod + 1 - 2 * core
    cnt = lax.rem(mod + 2, 4)
    crs = lax.rem(sib + 2, 4)
    p_sib, p_cnt, p_crs, p_y = (rep, dat, sib), (rep, dat, cnt), (rep, dat, crs), (rep, 1 - dat, mod)
    rows_own = x0.shape[0]
    chunk = rows_own // NT
    fwd_chunk = rows_own // NF
    row_base = core * rows_own
    w_hbm = [w0_hbm, w1_hbm, w2_hbm]
    u_hbm = [u0_hbm, u1_hbm, u2_hbm]
    xs = [x0, x1, x2]
    ys = [y0, y1, y2]
    es = [e0, e1, e2]

    def remote(src, dst, ssem, rsem, peer):
        return pltpu.make_async_remote_copy(src_ref=src, dst_ref=dst, send_sem=ssem, recv_sem=rsem,
                                            device_id=peer, device_id_type=MESH)

    def span(start, size):
        return pl.ds(pl.multiple_of(start, size), size)

    def w_copy(layer, kind):
        ssem, rsem = w_send.at[layer, kind], w_recv.at[layer, kind]
        if kind == 0:
            return remote(w_hbm[layer], wbuf.at[layer, span(128 * mod, 128)], ssem, rsem, p_sib)
        if kind == 1:
            return remote(w_hbm[layer].at[span(64 * dat, 64)], wbuf.at[layer, span(128 * mod + 64 * dat, 64)], ssem, rsem, p_cnt)
        half = 1 - dat if kind == 4 else dat
        ref = wbuf.at[layer, span(128 * cnt + 64 * half, 64)]
        return remote(ref, ref, ssem, rsem, p_y if kind == 2 else p_sib)

    def u_copy(layer, kind):
        return remote(u_hbm[layer], ubuf.at[layer, mod], u_send.at[layer, kind], u_recv.at[layer, kind],
                      (p_sib, p_cnt, p_crs)[kind])

    def t_copy(kind, c):
        other_core = core if kind == 0 else 1 - core
        return remote(t_hbm.at[span(other_core * rows_own + c * chunk, chunk)], tbuf.at[mod, span(c * chunk, chunk)],
                      t_send.at[kind, c], t_recv.at[kind, c], p_cnt if kind == 0 else p_crs)

    barrier = pltpu.get_barrier_semaphore()
    for peer in (p_sib, p_cnt, p_crs, p_y):
        pl.semaphore_signal(barrier, inc=1, device_id=peer, device_id_type=MESH)
    local_x = pltpu.make_async_copy(x_hbm.at[span(row_base, rows_own)], x0, l_x)
    local_w = [pltpu.make_async_copy(w_hbm[k], wbuf.at[k, span(128 * mod, 128)], l_w.at[k]) for k in range(3)]
    local_u = [pltpu.make_async_copy(u_hbm[k], ubuf.at[k, mod], l_u.at[k]) for k in range(3)]
    local_t = pltpu.make_async_copy(t_hbm.at[span(row_base, rows_own)], tbuf.at[mod], l_t)
    for k in range(3):
        local_w[k].start()
        local_u[k].start()
    local_x.start()
    local_t.start()
    pl.semaphore_wait(barrier, 4)

    for k in range(3):
        w_copy(k, 1).start()
        w_copy(k, 0).start()
        for kind in range(3):
            u_copy(k, kind).start()

    def start_targets(c, carry):
        t_copy(0, c).start()
        t_copy(1, c).start()
        return carry

    lax.fori_loop(0, NT, start_targets, 0)
    t_sib = remote(t_hbm.at[span((1 - core) * rows_own, rows_own)], tbuf.at[mod], s_send, s_recv, p_sib)
    t_sib.start()
    acc[...] = jnp.zeros_like(acc)
    stat[...] = jnp.zeros_like(stat)

    def relay_x(k):
        w_copy(k, 1).wait_recv()
        w_copy(k, 2).start()
        w_copy(k, 3).start()

    def relay_y(k):
        w_copy(k, 2).wait_recv()
        w_copy(k, 4).start()

    own_cols = span(256 * chip, 256)

    def e_rows(k, rows):
        return slice(None) if k == 1 else rows

    def fold(val):
        return jnp.sum(val.reshape(val.shape[0] // 8, 8, val.shape[1]), axis=0)

    def add_grad(k, rows):
        part = dot_tn(es[k][e_rows(k, rows), own_cols], xs[k][rows, :])
        acc[k, 0] += part[:128]
        acc[k, 1] += part[128:]

    def residual(slab, rows):
        cols = span(128 * slab, 128)
        y_val = y2[rows, cols]
        res = y_val - tbuf[slab, rows, :].astype(F32)
        grad = res * inv_batch
        stat[0, :, cols] += fold(res * res)
        stat[1, :, cols] += fold(grad * y_val)
        e2[rows, cols] = grad.astype(BF16)

    inv_sigma = []
    w_full_copy = pltpu.make_async_copy(wbuf.at[0], w_out, l_o)
    relay_x(0)
    relay_y(0)
    for k in range(3):
        local_w[k].wait()
        local_u[k].wait()
        for kind in range(3):
            u_copy(k, kind).wait_recv()
        for kind in (0, 3, 4):
            w_copy(k, kind).wait_recv()
        if k == 0:
            w_full_copy.start()
        u_row = jnp.concatenate([ubuf[k, j] for j in range(4)], axis=1)
        p_vec = jnp.sum(dot_nn(split_rows(u_row), wbuf[k]), axis=0, keepdims=True)
        norm = jnp.sqrt(jnp.sum(p_vec * p_vec, axis=1, keepdims=True))
        v_vec = p_vec / jnp.maximum(norm, 1e-12)
        s_vec = jnp.sum(dot_nt(split_rows(v_vec), wbuf[k]), axis=0, keepdims=True)
        sigma = jnp.sqrt(jnp.sum(s_vec * s_vec, axis=1, keepdims=True))
        pack_out[k:k + 1, :] = v_vec
        srow[k] = jnp.broadcast_to(s_vec / sigma, srow.shape[1:])
        pack_out[3 + k:4 + k, 0:128] = srow[k, 0:1, span(128 * mod, 128)]
        pack_out[6 + k:7 + k, :] = jnp.broadcast_to(sigma, (1, pack_out.shape[1]))
        inv = 1.0 / sigma
        inv_sigma.append(inv)
        if k < 2:
            relay_x(k + 1)
            relay_y(k + 1)
        if k == 0:
            local_x.wait()
        if k == 2:
            local_t.wait()
            t_sib.wait_recv()

        def forward(c, carry, k=k, inv=inv):
            rows = span(c * fwd_chunk, fwd_chunk)
            y_val = dot_nt(xs[k][rows, :], wbuf[k]) * inv
            ys[k][rows, :] = y_val
            if k < 2:
                xs[k + 1][rows, :] = jnp.maximum(y_val, 0.2 * y_val).astype(BF16)
            else:
                for j in range(2):
                    residual(2 * chip + j, rows)
                add_grad(2, rows)
            return carry

        lax.fori_loop(0, NF, forward, 0)

    def d_copy(k):
        return remote(acc.at[k, 1 - core], rbuf.at[k], d_send.at[k], d_recv.at[k], p_sib)

    g_copy = remote(g2own, g2other, g_send, g_recv, p_y)

    def e_local(c):
        return pltpu.make_async_copy(e0.at[span(c * chunk, chunk)], e_out.at[span(row_base + c * chunk, chunk)], l_e.at[c])

    def e_remote(c):
        return remote(e0.at[span(c * chunk, chunk)], e_out.at[span(row_base + c * chunk, chunk)], e_send.at[c], e_recv.at[c], p_sib)

    def backward(c, carry):
        @pl.when(c == 1)
        def _():
            d_copy(2).start()

        @pl.when(c == 3)
        def _():
            d_copy(2).wait_recv()
            g2own[...] = acc[2, core] + rbuf[2]

        @pl.when(c == 4)
        def _():
            g_copy.start()

        rows = span(c * chunk, chunk)
        for kind in range(2):
            t_copy(kind, c).wait_recv()
        for j in range(2):
            residual(2 - 2 * chip + j, rows)
        for k in (2, 1):
            back = (dot_nn(es[k][e_rows(k, rows), :], wbuf[k]) * inv_sigma[k]).astype(BF16).astype(F32)
            y_val = ys[k - 1][rows, :]
            grad = back * jnp.where(y_val > 0, 1.0, 0.2)
            stat[4 - k] += fold(grad * y_val)
            es[k - 1][e_rows(k - 1, rows), :] = grad.astype(BF16)
            add_grad(k - 1, rows)
        e_local(c).start()
        e_remote(c).start()
        return carry

    lax.fori_loop(0, NT, backward, 0)

    d_copy(1).start()
    row = lax.broadcasted_iota(jnp.int32, sstat.shape, 0)
    mine = jnp.zeros(sstat.shape, F32)
    for i in range(4):
        mine = jnp.where(row == i, jnp.sum(stat[i], axis=0, keepdims=True), mine)
    sstat[...] = mine
    d_copy(0).start()
    s_copy = remote(sstat, rstat, d_send.at[3], d_recv.at[3], p_sib)
    s_copy.start()
    g_copy.wait_recv()
    g2_out[...] = g2own[...] + g2other[...]
    for i, k in enumerate((1, 0)):
        d_copy(k).wait_recv()
        dw_out[128 * i:128 * i + 128, :] = acc[k, core] + rbuf[k]
    s_copy.wait_recv()
    dw_out[256:264, :] = sstat[...] + rstat[...]

    for k in range(3):
        d_copy(k).wait_send()
    s_copy.wait_send()
    g_copy.wait_send()
    t_sib.wait_send()

    def drain(c, carry):
        for kind in range(2):
            t_copy(kind, c).wait_send()
        e_local(c).wait()
        e_remote(c).wait_send()
        e_remote(c).wait_recv()
        return carry

    lax.fori_loop(0, NT, drain, 0)
    for k in range(3):
        for kind in range(5):
            w_copy(k, kind).wait_send()
        for kind in range(3):
            u_copy(k, kind).wait_send()
    w_full_copy.wait()


def dx_kernel(e_ref, w_ref, pack, dx_ref, v0_out, v1_out, v2_out, n0_out, n1_out, n2_out, sig_out):
    inv = 1.0 / pack[6:7, 0:1]
    dx_ref[...] = (dot_nn(e_ref[...], w_ref[...]) * inv).astype(BF16)

    @pl.when(pl.program_id(0) == 0)
    def _():
        for k, (v_out, n_out) in enumerate(((v0_out, n0_out), (v1_out, n1_out), (v2_out, n2_out))):
            v_out[...] = pack[k:k + 1, :]
            n_out[...] = pack[3 + k:4 + k, 0:128]
        lane = lax.broadcasted_iota(jnp.int32, (1, 128), 1)
        row = jnp.where(lane == 0, pack[6:7, 0:128], jnp.where(lane == 1, pack[7:8, 0:128], pack[8:9, 0:128]))
        sig_out[...] = row[:, :3]


def final_kernel(loss_scale, own, other, g2, pack, dw0, dw1, dw2, loss_out):
    stats = jnp.sum(own[256:264, :] + other[256:264, :], axis=1, keepdims=True)
    loss_out[...] = loss_scale * stats[0:1]
    grads = (own[128:256, :] + other[128:256, :], own[0:128, :] + other[0:128, :], g2[...])
    for k, (grad, out) in enumerate(zip(grads, (dw0, dw1, dw2))):
        inv = 1.0 / pack[6 + k:7 + k, 0:1]
        u_col = jnp.transpose(jnp.broadcast_to(pack[3 + k:4 + k, 0:128], (128, 128)))[:, 0:1]
        out[...] = grad * inv - (stats[3 - k:4 - k] * inv) * (u_col * pack[k:k + 1, :])


def solution(mesh):
    data_size = mesh.shape["data"]
    row_spec = P(("replica", "model"), None)
    vec_spec = P(("replica", "model"))
    batch_spec = P(("replica", "data"), None)
    target_spec = P(("replica", "data"), "model")
    part_spec = P("replica")

    def local_step(x_in, w_in, w_mid, w_out, u_in, u_mid, u_out, target):
        rows, width = x_in.shape
        half = rows // 2
        batch_total = rows * data_size
        any_spec = pl.BlockSpec(memory_space=pl.ANY)
        vmem_spec = pl.BlockSpec(memory_space=pltpu.VMEM)
        dma = pltpu.SemaphoreType.DMA
        small = [jax.ShapeDtypeStruct((1, width), F32)] * 3 + [jax.ShapeDtypeStruct((1, 128), F32)] * 3
        outs = pl.pallas_call(
            functools.partial(main_kernel, 1.0 / batch_total),
            out_shape=[
                jax.ShapeDtypeStruct((rows, width), BF16),
                jax.ShapeDtypeStruct((width, width), BF16),
                jax.ShapeDtypeStruct((264, width), F32),
                jax.ShapeDtypeStruct((128, width), F32),
                jax.ShapeDtypeStruct((16, width), F32),
            ],
            in_specs=[any_spec] * 8,
            out_specs=[any_spec] * 2 + [vmem_spec] * 3,
            scratch_shapes=[pltpu.VMEM((half, width), BF16)] * 3 + [pltpu.VMEM((half, width), F32)] * 3 + [
                pltpu.VMEM((4, half, 128), BF16),
                pltpu.VMEM((3, width, width), BF16),
                pltpu.VMEM((3, 4, 1, 128), F32),
                pltpu.VMEM((half, width), BF16),
                pltpu.VMEM((half // NT, width), BF16),
                pltpu.VMEM((half, width), BF16),
                pltpu.VMEM((3, 2, 128, width), F32),
                pltpu.VMEM((3, 128, width), F32),
                pltpu.VMEM((128, width), F32),
                pltpu.VMEM((128, width), F32),
                pltpu.VMEM((4, 8, width), F32),
                pltpu.VMEM((8, width), F32),
                pltpu.VMEM((8, width), F32),
                pltpu.VMEM((3, 8, width), F32),
                dma((3, 5)), dma((3, 5)), dma((3, 3)), dma((3, 3)),
                dma((2, NT)), dma((2, NT)), dma(()), dma(()), dma((NT,)), dma((NT,)), dma((4,)), dma((4,)), dma(()), dma(()),
                dma((3,)), dma((3,)), dma(()), dma(()), dma((NT,)), dma(()),
            ],
            compiler_params=pltpu.CompilerParams(
                collective_id=0, has_side_effects=True, vmem_limit_bytes=63 * 2**20),
            name="fused_step",
        )(x_in, w_in, w_mid, w_out, u_in.reshape(1, 128), u_mid.reshape(1, 128), u_out.reshape(1, 128), target)
        e_all, w_full, dw_part, g2_sum, pack = outs
        other = lax.ppermute(dw_part, "data", [(0, 1), (1, 0)])

        block = 1024
        full = lambda shape: pl.BlockSpec(shape, lambda i: (0, 0))
        vec_specs = [full((1, width))] * 3 + [full((1, 128))] * 3
        passed = pl.pallas_call(
            dx_kernel,
            grid=(rows // block,),
            out_shape=[jax.ShapeDtypeStruct((rows, width), BF16)] + small + [jax.ShapeDtypeStruct((1, 3), F32)],
            in_specs=[pl.BlockSpec((block, width), lambda i: (i, 0)), full((width, width)), full((16, width))],
            out_specs=[pl.BlockSpec((block, width), lambda i: (i, 0))] + vec_specs + [full((1, 3))],
            cost_estimate=pl.CostEstimate(flops=2 * rows * width * width, bytes_accessed=4 * rows * width, transcendentals=0),
            name="dx",
        )(e_all, w_full, pack)
        grad_x, sig_row = passed[0], passed[7]

        finals = pl.pallas_call(
            functools.partial(final_kernel, 0.5 / batch_total),
            out_shape=[jax.ShapeDtypeStruct((128, width), F32)] * 3 + [jax.ShapeDtypeStruct((1, 1), F32)],
            in_specs=[vmem_spec] * 4,
            out_specs=[vmem_spec] * 4,
            compiler_params=pltpu.CompilerParams(vmem_limit_bytes=8 * 2**20),
            name="finish",
        )(dw_part, other, g2_sum, pack)
        v_row, u_row = passed[1:4], passed[4:7]
        return (finals[3].reshape(1), grad_x, finals[0], finals[1], finals[2],
                u_row[0].reshape(128), u_row[1].reshape(128), u_row[2].reshape(128),
                v_row[0].reshape(width), v_row[1].reshape(width), v_row[2].reshape(width), sig_row.reshape(3))

    in_specs = (batch_spec, row_spec, row_spec, row_spec, vec_spec, vec_spec, vec_spec, target_spec)
    out_specs = (part_spec, batch_spec, row_spec, row_spec, row_spec, vec_spec, vec_spec, vec_spec, part_spec, part_spec, part_spec, part_spec)
    return jax.shard_map(local_step, mesh=mesh, in_specs=in_specs, out_specs=out_specs, check_vma=False)
```

```python
import functools

import jax
import jax.numpy as jnp
from jax import lax
from jax.experimental import pallas as pl
from jax.experimental.pallas import tpu as pltpu
from jax.sharding import PartitionSpec as P

MESH = pl.DeviceIdType.MESH
F32 = jnp.float32
BF16 = jnp.bfloat16
DMA_ROWS = 256
FWD_ROWS = 1024
BIG_ROWS = 512
SHARED_ROWS = 512


def dot_nt(lhs, rhs):
    return lax.dot_general(lhs, rhs, (((1,), (1,)), ((), ())), preferred_element_type=F32)


def dot_nn(lhs, rhs):
    return lax.dot_general(lhs, rhs, (((1,), (0,)), ((), ())), preferred_element_type=F32)


def dot_tn(lhs, rhs):
    return lax.dot_general(lhs, rhs, (((0,), (0,)), ((), ())), preferred_element_type=F32)


def split_rows(vec):
    width = vec.shape[1]
    high = vec.astype(BF16).astype(F32)
    rest = vec - high
    mid = rest.astype(BF16).astype(F32)
    low = rest - mid
    row = lax.broadcasted_iota(jnp.int32, (16, width), 0)
    stacked = jnp.where(row == 0, high, jnp.where(row == 1, mid, jnp.where(row == 2, low, 0.0)))
    return stacked.astype(BF16)


def main_kernel(inv_batch, x_hbm, w0_hbm, w1_hbm, w2_hbm, u0_hbm, u1_hbm, u2_hbm, t_hbm,
                dx_out, tot_out, pack_out,
                x1, x2, y0, y1, y2, tbuf, wbuf, ubuf, e2, e1, e0, xfor, acc, facc, rbuf, frbuf, fsend,
                g_own, g_other, p_own, p_other, stat, fstat, sstat, rstat, fsstat, frstat, srow,
                w_send, w_recv, u_send, u_recv, t_send, t_recv, s_send, s_recv, e_send, e_recv, d_send, d_recv,
                f_send, f_recv, h_send, h_recv, l_w, l_u, l_t, l_x):
    rep, dat, mod = lax.axis_index("replica"), lax.axis_index("data"), lax.axis_index("model")
    core = lax.rem(mod, 2)
    chip = mod // 2
    sib = mod + 1 - 2 * core
    cnt = lax.rem(mod + 2, 4)
    crs = lax.rem(sib + 2, 4)
    p_sib, p_cnt, p_crs = (rep, dat, sib), (rep, dat, cnt), (rep, dat, crs)
    p_y, p_ys = (rep, 1 - dat, mod), (rep, 1 - dat, sib)
    rows_own = x_hbm.shape[0] // 2
    shared_at = rows_own - SHARED_ROWS
    row_base = core * rows_own
    n_dma = rows_own // DMA_ROWS
    n_shared = SHARED_ROWS // DMA_ROWS
    w_hbm = [w0_hbm, w1_hbm, w2_hbm]
    u_hbm = [u0_hbm, u1_hbm, u2_hbm]

    def remote(src, dst, ssem, rsem, peer):
        return pltpu.make_async_remote_copy(src_ref=src, dst_ref=dst, send_sem=ssem, recv_sem=rsem,
                                            device_id=peer, device_id_type=MESH)

    def span(start, size):
        return pl.ds(pl.multiple_of(start, size), size)

    def w_copy(layer, kind):
        ssem, rsem = w_send.at[layer, kind], w_recv.at[layer, kind]
        if kind == 0:
            return remote(w_hbm[layer], wbuf.at[layer, span(128 * mod, 128)], ssem, rsem, p_sib)
        if kind == 1:
            return remote(w_hbm[layer].at[span(64 * dat, 64)], wbuf.at[layer, span(128 * mod + 64 * dat, 64)], ssem, rsem, p_cnt)
        half = 1 - dat if kind == 4 else dat
        ref = wbuf.at[layer, span(128 * cnt + 64 * half, 64)]
        return remote(ref, ref, ssem, rsem, p_y if kind == 2 else p_sib)

    def u_copy(layer, kind):
        return remote(u_hbm[layer], ubuf.at[layer, mod], u_send.at[layer, kind], u_recv.at[layer, kind],
                      (p_sib, p_cnt, p_crs)[kind])

    def t_copy(kind, c):
        other_core = core if kind == 0 else 1 - core
        return remote(t_hbm.at[span(other_core * rows_own + c * DMA_ROWS, DMA_ROWS)], tbuf.at[mod, span(c * DMA_ROWS, DMA_ROWS)],
                      t_send.at[kind, c], t_recv.at[kind, c], p_cnt if kind == 0 else p_crs)

    def f_copy(kind):
        if kind == 0:
            src, dst, peer = x_hbm.at[span(row_base + shared_at, SHARED_ROWS)], xfor, p_y
        else:
            other_core = core if kind == 1 else 1 - core
            src = t_hbm.at[span(other_core * rows_own + shared_at, SHARED_ROWS)]
            dst, peer = tbuf.at[mod, span(rows_own, SHARED_ROWS)], p_y if kind == 1 else p_ys
        return remote(src, dst, f_send.at[kind], f_recv.at[kind], peer)

    def h_copy(kind, j):
        ref = tbuf.at[mod if kind == 0 else sib, span(rows_own + j * DMA_ROWS, DMA_ROWS)]
        return remote(ref, ref, h_send.at[kind, j], h_recv.at[kind, j], p_cnt)

    barrier = pltpu.get_barrier_semaphore()
    peers = (p_sib, p_cnt, p_crs, p_y, p_ys)
    for peer in peers:
        pl.semaphore_signal(barrier, inc=1, device_id=peer, device_id_type=MESH)
    local_w = [pltpu.make_async_copy(w_hbm[k], wbuf.at[k, span(128 * mod, 128)], l_w.at[k]) for k in range(3)]
    local_u = [pltpu.make_async_copy(u_hbm[k], ubuf.at[k, mod], l_u.at[k]) for k in range(3)]
    own_rows = span(row_base, rows_own)
    local_x = pltpu.make_async_copy(x_hbm.at[own_rows], dx_out.at[own_rows], l_x)
    local_t = pltpu.make_async_copy(t_hbm.at[own_rows], tbuf.at[mod, pl.ds(0, rows_own)], l_t)
    for k in range(3):
        local_w[k].start()
        local_u[k].start()
    local_x.start()
    local_t.start()
    pl.semaphore_wait(barrier, len(peers))

    for k in range(3):
        w_copy(k, 1).start()
        w_copy(k, 0).start()
        for kind in range(3):
            u_copy(k, kind).start()

    def start_targets(c, carry):
        t_copy(0, c).start()
        t_copy(1, c).start()
        return carry

    lax.fori_loop(0, n_dma, start_targets, 0)
    t_sib = remote(t_hbm.at[span((1 - core) * rows_own, rows_own)], tbuf.at[mod, pl.ds(0, rows_own)], s_send, s_recv, p_sib)
    t_sib.start()
    acc[...] = jnp.zeros_like(acc)
    facc[...] = jnp.zeros_like(facc)
    stat[...] = jnp.zeros_like(stat)
    fstat[...] = jnp.zeros_like(fstat)

    def relay_x(k):
        w_copy(k, 1).wait_recv()
        w_copy(k, 2).start()
        w_copy(k, 3).start()

    def relay_y(k):
        w_copy(k, 2).wait_recv()
        w_copy(k, 4).start()

    own_cols = span(256 * chip, 256)

    def fold(val):
        return jnp.sum(val.reshape(val.shape[0] // 8, 8, val.shape[1]), axis=0)

    def leaky(val):
        return jnp.maximum(val, 0.2 * val).astype(BF16)

    def add_grad(ref, e_val, x_val):
        part = dot_tn(e_val, x_val)
        ref[0] += part[:128]
        ref[1] += part[128:]

    def residual(y_val, slab, rows, sums, at):
        res = y_val - tbuf[slab, rows, :].astype(F32)
        grad = res * inv_batch
        if sums is not None:
            sums[0, :, at:at + 128] += fold(res * res)
            sums[1, :, at:at + 128] += fold(grad * y_val)
        e2[rows, span(128 * slab, 128)] = grad.astype(BF16)

    def last_layer(rows, sums):
        y_val = dot_nt(x2[rows, :], wbuf[2]) * inv_sigma[2]
        first = chip == 0
        own = jnp.where(first, y_val[:, :256], y_val[:, 256:])
        y2[rows, :] = jnp.where(first, y_val[:, 256:], y_val[:, :256])
        for j in range(2):
            residual(own[:, 128 * j:128 * j + 128], 2 * chip + j, rows, sums, 256 + 128 * j)

    inv_sigma = []
    relay_x(0)
    relay_y(0)
    for k in range(3):
        local_w[k].wait()
        local_u[k].wait()
        for kind in range(3):
            u_copy(k, kind).wait_recv()
        for kind in (0, 3, 4):
            w_copy(k, kind).wait_recv()
        u_row = jnp.concatenate([ubuf[k, j] for j in range(4)], axis=1)
        p_vec = jnp.sum(dot_nn(split_rows(u_row), wbuf[k]), axis=0, keepdims=True)
        norm = jnp.sqrt(jnp.sum(p_vec * p_vec, axis=1, keepdims=True))
        v_vec = p_vec / jnp.maximum(norm, 1e-12)
        s_vec = jnp.sum(dot_nt(split_rows(v_vec), wbuf[k]), axis=0, keepdims=True)
        sigma = jnp.sqrt(jnp.sum(s_vec * s_vec, axis=1, keepdims=True))
        pack_out[k:k + 1, :] = v_vec
        srow[k] = jnp.broadcast_to(s_vec / sigma, srow.shape[1:])
        pack_out[3 + k:4 + k, 0:128] = srow[k, 0:1, span(128 * mod, 128)]
        pack_out[6 + k:7 + k, :] = jnp.broadcast_to(sigma, (1, pack_out.shape[1]))
        inv = 1.0 / sigma
        inv_sigma.append(inv)
        if k < 2:
            relay_x(k + 1)
            relay_y(k + 1)
        if k == 0:
            local_x.wait()
        if k == 1:
            for kind in range(3):
                f_copy(kind).start()
        if k == 2:
            local_t.wait()
            t_sib.wait_recv()

        def forward(c, carry, k=k, inv=inv):
            rows = span(c * FWD_ROWS, FWD_ROWS)
            if k == 0:
                y_val = dot_nt(dx_out[span(row_base + c * FWD_ROWS, FWD_ROWS), :], wbuf[0]) * inv
                y0[rows, :] = y_val
                x1[rows, :] = leaky(y_val)
            elif k == 1:
                y_val = dot_nt(x1[rows, :], wbuf[1]) * inv
                y1[rows, :] = y_val
                x2[rows, :] = leaky(y_val)
            else:
                last_layer(rows, stat)
                add_grad(acc.at[2], e2[rows, own_cols], x2[rows, :])
            return carry

        lax.fori_loop(0, rows_own // FWD_ROWS, forward, 0)

    def d_copy(k):
        return remote(acc.at[k, 1 - core], rbuf.at[k], d_send.at[k], d_recv.at[k], p_sib)

    def fd_copy(k):
        return remote(fsend.at[k], frbuf.at[k], d_send.at[4 + k], d_recv.at[4 + k], p_sib)

    s_copy = remote(sstat, rstat, d_send.at[3], d_recv.at[3], p_sib)
    fs_copy = remote(fsstat, frstat, d_send.at[6], d_recv.at[6], p_sib)
    g_copy = remote(g_own, g_other, d_send.at[7], d_recv.at[7], p_y)
    p_copy = remote(p_own, p_other, d_send.at[8], d_recv.at[8], p_y)

    def dx_copy(idx, at, size):
        ref = dx_out.at[span(row_base + at, size)]
        return remote(ref, ref, e_send.at[idx], e_recv.at[idx], p_sib)

    def backward(at, size, sums, grad1, grad0, idx=None):
        rows = span(at, size)
        for j in range(2):
            residual(y2[rows, 128 * j:128 * j + 128], 2 - 2 * chip + j, rows, sums, 128 * j)
        back = (dot_nn(e2[rows, :], wbuf[2]) * inv_sigma[2]).astype(BF16).astype(F32)
        y_val = y1[rows, :]
        grad = back * jnp.where(y_val > 0, 1.0, 0.2)
        sums[2] += fold(grad * y_val)
        e1[:size] = grad.astype(BF16)
        back = (dot_nn(e1[:size], wbuf[1]) * inv_sigma[1]).astype(BF16).astype(F32)
        y_val = y0[rows, :]
        grad = back * jnp.where(y_val > 0, 1.0, 0.2)
        sums[3] += fold(grad * y_val)
        e0[:size] = grad.astype(BF16)
        if idx is None:
            add_grad(grad0, e0[:size, own_cols], xfor[span(at - rows_own, size), :])
            add_grad(grad1, e1[:size, own_cols], x1[rows, :])
        else:
            x_rows = span(row_base + at, size)
            add_grad(grad0, e0[:size, own_cols], dx_out[x_rows, :])
            dx_out[x_rows, :] = (dot_nn(e0[:size], wbuf[0]) * inv_sigma[0]).astype(BF16)
            add_grad(grad1, e1[:size, own_cols], x1[rows, :])
            dx_copy(idx, at, size).start()

    n_big = shared_at // BIG_ROWS - 1
    per_big = BIG_ROWS // DMA_ROWS

    def big_step(i, carry):
        @pl.when(i == 0)
        def _():
            d_copy(2).start()

        @pl.when(i == 1)
        def _():
            d_copy(2).wait_recv()
            g_own[...] = acc[2, core] + rbuf[2]

        @pl.when(i == 2)
        def _():
            g_copy.start()

        @pl.when(i == n_big - 2)
        def _():
            for kind in range(3):
                f_copy(kind).wait_recv()
            for j in range(n_shared):
                h_copy(0, j).start()
                h_copy(1, j).start()

        @pl.when(i == n_big - 1)
        def _():
            rows = pl.ds(rows_own, SHARED_ROWS)
            y_val = dot_nt(xfor[...], wbuf[0]) * inv_sigma[0]
            y0[rows, :] = y_val
            x1[rows, :] = leaky(y_val)
            y_val = dot_nt(x1[rows, :], wbuf[1]) * inv_sigma[1]
            y1[rows, :] = y_val
            x2[rows, :] = leaky(y_val)
            last_layer(rows, None)

        for c in range(per_big):
            t_copy(0, i * per_big + c).wait_recv()
            t_copy(1, i * per_big + c).wait_recv()
        backward(i * BIG_ROWS, BIG_ROWS, stat, acc.at[1], acc.at[0], i)
        return carry

    lax.fori_loop(0, n_big, big_step, 0)

    def small_step(c, carry):
        t_copy(0, c).wait_recv()
        t_copy(1, c).wait_recv()
        backward(c * DMA_ROWS, DMA_ROWS, stat, acc.at[1], acc.at[0], n_big + c - n_big * per_big)
        return carry

    lax.fori_loop(n_big * per_big, n_dma - n_shared, small_step, 0)

    row = lax.broadcasted_iota(jnp.int32, sstat.shape, 0)

    def gather_sums(ref_sums):
        mine = jnp.zeros(sstat.shape, F32)
        for i in range(4):
            mine = jnp.where(row == i, jnp.sum(ref_sums(i), axis=0, keepdims=True), mine)
        return mine

    d_copy(0).start()
    sstat[...] = gather_sums(lambda i: stat[i])
    d_copy(1).start()
    s_copy.start()
    d_copy(0).wait_recv()
    p_own[128:256, :] = acc[0, core] + rbuf[0]
    d_copy(1).wait_recv()
    p_own[0:128, :] = acc[1, core] + rbuf[1]
    s_copy.wait_recv()
    p_own[256:264, :] = sstat[...] + rstat[...]

    def shared_step(j, carry):
        t_copy(0, n_dma - n_shared + j).wait_recv()
        t_copy(1, n_dma - n_shared + j).wait_recv()

        @pl.when(j == 0)
        def _():
            p_copy.start()

        backward(shared_at + j * DMA_ROWS, DMA_ROWS, fstat.at[0], facc.at[0, 1], facc.at[0, 0], n_big + per_big + j)
        return carry

    lax.fori_loop(0, n_shared, shared_step, 0)

    def foreign_step(j, carry):
        h_copy(0, j).wait_recv()
        h_copy(1, j).wait_recv()
        backward(rows_own + j * DMA_ROWS, DMA_ROWS, fstat.at[1], facc.at[1, 1], facc.at[1, 0])
        return carry

    lax.fori_loop(0, n_shared, foreign_step, 0)

    for k in (0, 1):
        fsend[k] = facc[0, k, 1 - core] + facc[1, k, 1 - core]
    fsstat[...] = gather_sums(lambda i: fstat[0, i] + fstat[1, i])
    for k in (0, 1):
        fd_copy(k).start()
    fs_copy.start()
    g_copy.wait_recv()
    tot_out[256:384, :] = g_own[...] + g_other[...]
    p_copy.wait_recv()
    for i, k in enumerate((1, 0)):
        part = slice(128 * i, 128 * i + 128)
        fd_copy(k).wait_recv()
        tot_out[part, :] = (p_own[part, :] + p_other[part, :]) + ((facc[0, k, core] + facc[1, k, core]) + frbuf[k])
    fs_copy.wait_recv()
    tot_out[384:392, :] = (p_own[256:264, :] + p_other[256:264, :]) + (fsstat[...] + frstat[...])

    for k in range(3):
        d_copy(k).wait_send()
        for kind in range(5):
            w_copy(k, kind).wait_send()
        for kind in range(3):
            u_copy(k, kind).wait_send()
        f_copy(k).wait_send()
    for copy in (fd_copy(0), fd_copy(1), s_copy, fs_copy, g_copy, p_copy, t_sib):
        copy.wait_send()

    def drain_targets(c, carry):
        t_copy(0, c).wait_send()
        t_copy(1, c).wait_send()
        return carry

    lax.fori_loop(0, n_dma, drain_targets, 0)
    for j in range(n_shared):
        h_copy(0, j).wait_send()
        h_copy(1, j).wait_send()

    def drain_big(i, carry):
        dx_copy(i, i * BIG_ROWS, BIG_ROWS).wait()
        return carry

    lax.fori_loop(0, n_big, drain_big, 0)

    def drain_small(i, carry):
        dx_copy(n_big + i, n_big * BIG_ROWS + i * DMA_ROWS, DMA_ROWS).wait()
        return carry

    lax.fori_loop(0, per_big + n_shared, drain_small, 0)


def finish_kernel(loss_scale, dx_in, tot, pack, dx_ref, dw0, dw1, dw2, v0, v1, v2, n0, n1, n2, sig_out, loss_out, sems):
    parts = sems.shape[0]
    rows = dx_in.shape[0] // parts
    copies = [pltpu.make_async_copy(dx_in.at[pl.ds(i * rows, rows)], dx_ref.at[pl.ds(i * rows, rows)], sems.at[i]) for i in range(parts)]
    for copy in copies:
        copy.start()
    stats = jnp.sum(tot[384:392, :], axis=1, keepdims=True)
    loss_out[...] = loss_scale * stats[0:1]
    for k, (at, out, v_out, n_out) in enumerate(((128, dw0, v0, n0), (0, dw1, v1, n1), (256, dw2, v2, n2))):
        inv = 1.0 / pack[6 + k:7 + k, 0:1]
        v_out[...] = pack[k:k + 1, :]
        n_out[...] = pack[3 + k:4 + k, 0:128]
        u_col = jnp.transpose(jnp.broadcast_to(pack[3 + k:4 + k, 0:128], (128, 128)))[:, 0:1]
        out[...] = tot[at:at + 128, :] * inv - (stats[3 - k:4 - k] * inv) * (u_col * pack[k:k + 1, :])
    lane = lax.broadcasted_iota(jnp.int32, (1, 128), 1)
    row = jnp.where(lane == 0, pack[6:7, 0:128], jnp.where(lane == 1, pack[7:8, 0:128], pack[8:9, 0:128]))
    sig_out[...] = row[:, :3]
    for copy in copies:
        copy.wait()


def solution(mesh):
    data_size = mesh.shape["data"]
    row_spec = P(("replica", "model"), None)
    vec_spec = P(("replica", "model"))
    batch_spec = P(("replica", "data"), None)
    target_spec = P(("replica", "data"), "model")
    part_spec = P("replica")

    def local_step(x_in, w_in, w_mid, w_out, u_in, u_mid, u_out, target):
        rows, width = x_in.shape
        half = rows // 2
        ext = half + SHARED_ROWS
        batch_total = rows * data_size
        any_spec = pl.BlockSpec(memory_space=pl.ANY)
        vmem_spec = pl.BlockSpec(memory_space=pltpu.VMEM)
        dma = pltpu.SemaphoreType.DMA
        vm = pltpu.VMEM
        n_dma = half // DMA_ROWS
        n_shared = SHARED_ROWS // DMA_ROWS
        n_dx = (half - SHARED_ROWS) // BIG_ROWS - 1 + BIG_ROWS // DMA_ROWS + n_shared
        dx_all, tot, pack = pl.pallas_call(
            functools.partial(main_kernel, 1.0 / batch_total),
            out_shape=[vm((rows, width), BF16), vm((392, width), F32), vm((16, width), F32)],
            in_specs=[any_spec] * 8,
            out_specs=[vmem_spec] * 3,
            scratch_shapes=[
                vm((ext, width), BF16), vm((ext, width), BF16),
                vm((ext, width), F32), vm((ext, width), F32), vm((ext, 256), F32),
                vm((4, ext, 128), BF16),
                vm((3, width, width), BF16),
                vm((3, 4, 1, 128), F32),
                vm((ext, width), BF16), vm((BIG_ROWS, width), BF16), vm((BIG_ROWS, width), BF16),
                vm((SHARED_ROWS, width), BF16),
                vm((3, 2, 128, width), F32), vm((2, 2, 2, 128, width), F32),
                vm((3, 128, width), F32), vm((2, 128, width), F32), vm((2, 128, width), F32),
                vm((128, width), F32), vm((128, width), F32),
                vm((264, width), F32), vm((264, width), F32),
                vm((4, 8, width), F32), vm((2, 4, 8, width), F32),
                vm((8, width), F32), vm((8, width), F32), vm((8, width), F32), vm((8, width), F32),
                vm((3, 8, width), F32),
                dma((3, 5)), dma((3, 5)), dma((3, 3)), dma((3, 3)),
                dma((2, n_dma)), dma((2, n_dma)), dma(()), dma(()), dma((n_dx,)), dma((n_dx,)), dma((9,)), dma((9,)),
                dma((3,)), dma((3,)), dma((2, n_shared)), dma((2, n_shared)),
                dma((3,)), dma((3,)), dma(()), dma(()),
            ],
            compiler_params=pltpu.CompilerParams(
                collective_id=0, has_side_effects=True, vmem_limit_bytes=54 * 2**20),
            name="fused_step",
        )(x_in, w_in, w_mid, w_out, u_in.reshape(1, 128), u_mid.reshape(1, 128), u_out.reshape(1, 128), target)

        f32 = lambda *shape: jax.ShapeDtypeStruct(shape, F32)
        finals = pl.pallas_call(
            functools.partial(finish_kernel, 0.5 / batch_total),
            out_shape=[jax.ShapeDtypeStruct((rows, width), BF16)] + [f32(128, width)] * 3 + [f32(1, width)] * 3 + [
                f32(1, 128)] * 3 + [f32(1, 3), f32(1, 1)],
            in_specs=[vmem_spec] * 3,
            out_specs=[any_spec] + [vmem_spec] * 11,
            scratch_shapes=[dma((4,))],
            compiler_params=pltpu.CompilerParams(vmem_limit_bytes=8 * 2**20),
            name="finish",
        )(dx_all, tot, pack)
        grad_x, dw0, dw1, dw2, v0, v1, v2, n0, n1, n2, sig, loss = finals
        return (loss.reshape(1), grad_x, dw0, dw1, dw2, n0.reshape(128), n1.reshape(128), n2.reshape(128),
                v0.reshape(width), v1.reshape(width), v2.reshape(width), sig.reshape(3))

    in_specs = (batch_spec, row_spec, row_spec, row_spec, vec_spec, vec_spec, vec_spec, target_spec)
    out_specs = (part_spec, batch_spec, row_spec, row_spec, row_spec, vec_spec, vec_spec, vec_spec, part_spec, part_spec, part_spec, part_spec)
    return jax.shard_map(local_step, mesh=mesh, in_specs=in_specs, out_specs=out_specs, check_vma=False)
```

```python
import functools

import jax
import jax.numpy as jnp
from jax import lax
from jax.experimental import pallas as pl
from jax.experimental.pallas import tpu as pltpu
from jax.sharding import PartitionSpec as P

MESH = pl.DeviceIdType.MESH
F32 = jnp.float32
BF16 = jnp.bfloat16
FWD_ROWS = 1024
BIG_ROWS = 512
PLAIN = ((512, 6), (256, 1), (128, 1))
SHARED = ((256, 2), (128, 1))
SHARED_ROWS = sum(size * count for size, count in SHARED)
N_PLAIN = sum(count for _, count in PLAIN)
N_SHARED = sum(count for _, count in SHARED)


def dot_nt(lhs, rhs):
    return lax.dot_general(lhs, rhs, (((1,), (1,)), ((), ())), preferred_element_type=F32)


def dot_nn(lhs, rhs):
    return lax.dot_general(lhs, rhs, (((1,), (0,)), ((), ())), preferred_element_type=F32)


def dot_tn(lhs, rhs):
    return lax.dot_general(lhs, rhs, (((0,), (0,)), ((), ())), preferred_element_type=F32)


def split_rows(vec):
    width = vec.shape[1]
    high = vec.astype(BF16).astype(F32)
    rest = vec - high
    mid = rest.astype(BF16).astype(F32)
    low = rest - mid
    row = lax.broadcasted_iota(jnp.int32, (16, width), 0)
    stacked = jnp.where(row == 0, high, jnp.where(row == 1, mid, jnp.where(row == 2, low, 0.0)))
    return stacked.astype(BF16)


def main_kernel(inv_batch, x_hbm, w0_hbm, w1_hbm, w2_hbm, u0_hbm, u1_hbm, u2_hbm, t_hbm,
                dx_out, tot_out, pack_out,
                x1, x2, y0, y1, y2, tbuf, wbuf, ubuf, e2, e1, e0, xfor, acc, facc, rbuf, frbuf, fsend,
                g_own, g_other, p_own, p_other, stat, fstat, sstat, rstat, fsstat, frstat, srow,
                w_send, w_recv, u_send, u_recv, t_send, t_recv, s_send, s_recv, e_send, e_recv, d_send, d_recv,
                f_send, f_recv, h_send, h_recv, l_w, l_u, l_t, l_x):
    rep, dat, mod = lax.axis_index("replica"), lax.axis_index("data"), lax.axis_index("model")
    core = lax.rem(mod, 2)
    chip = mod // 2
    sib = mod + 1 - 2 * core
    cnt = lax.rem(mod + 2, 4)
    crs = lax.rem(sib + 2, 4)
    p_sib, p_cnt, p_crs = (rep, dat, sib), (rep, dat, cnt), (rep, dat, crs)
    p_y, p_ys = (rep, 1 - dat, mod), (rep, 1 - dat, sib)
    rows_own = x_hbm.shape[0] // 2
    shared_at = rows_own - SHARED_ROWS
    row_base = core * rows_own

    def each_chunk(groups, first, at, body):
        for size, count in groups:
            def step(i, carry, size=size, first=first, at=at):
                body(first + i, at + i * size, size)
                return carry
            if count == 1:
                step(0, 0)
            else:
                lax.fori_loop(0, count, step, 0)
            first, at = first + count, at + size * count
    w_hbm = [w0_hbm, w1_hbm, w2_hbm]
    u_hbm = [u0_hbm, u1_hbm, u2_hbm]

    def remote(src, dst, ssem, rsem, peer):
        return pltpu.make_async_remote_copy(src_ref=src, dst_ref=dst, send_sem=ssem, recv_sem=rsem,
                                            device_id=peer, device_id_type=MESH)

    def arrived(ref, sem):
        pltpu.make_async_copy(ref, ref, sem).wait()

    def span(start, size):
        return pl.ds(pl.multiple_of(start, size), size)

    def tile(start, size):
        return pl.ds(pl.multiple_of(start, 128), size)

    def w_copy(layer, kind):
        ssem, rsem = w_send, w_recv.at[layer, (0, 1, 2, 0, 0)[kind]]
        if kind == 0:
            return remote(w_hbm[layer], wbuf.at[layer, span(128 * mod, 128)], ssem, rsem, p_sib)
        if kind == 1:
            return remote(w_hbm[layer].at[span(64 * dat, 64)], wbuf.at[layer, span(128 * mod + 64 * dat, 64)], ssem, rsem, p_cnt)
        half = 1 - dat if kind == 4 else dat
        ref = wbuf.at[layer, span(128 * cnt + 64 * half, 64)]
        return remote(ref, ref, ssem, rsem, p_y if kind == 2 else p_sib)

    def u_copy(kind):
        ref = ubuf.at[:, mod]
        return remote(ref, ref, u_send, u_recv, (p_sib, p_cnt, p_crs)[kind])

    def t_copy(kind, idx, at, size):
        other_core = core if kind == 0 else 1 - core
        return remote(t_hbm.at[tile(other_core * rows_own + at, size)], tbuf.at[mod, tile(at, size)],
                      t_send, t_recv.at[idx], p_cnt if kind == 0 else p_crs)

    def f_copy(kind):
        if kind == 0:
            src, dst, peer = x_hbm.at[tile(row_base + shared_at, SHARED_ROWS)], xfor, p_y
        else:
            other_core = core if kind == 1 else 1 - core
            src = t_hbm.at[tile(other_core * rows_own + shared_at, SHARED_ROWS)]
            dst, peer = tbuf.at[mod, tile(rows_own, SHARED_ROWS)], p_y if kind == 1 else p_ys
        return remote(src, dst, f_send, f_recv, peer)

    def h_copy(kind, idx, at, size):
        ref = tbuf.at[mod if kind == 0 else sib, tile(at, size)]
        return remote(ref, ref, h_send, h_recv.at[idx], p_cnt)

    barrier = pltpu.get_barrier_semaphore()
    peers = (p_sib, p_cnt, p_crs, p_y, p_ys)
    for peer in peers:
        pl.semaphore_signal(barrier, inc=1, device_id=peer, device_id_type=MESH)
    local_w = [pltpu.make_async_copy(w_hbm[k], wbuf.at[k, span(128 * mod, 128)], l_w.at[k]) for k in range(3)]
    local_u = [pltpu.make_async_copy(u_hbm[k], ubuf.at[k, mod], l_u.at[k]) for k in range(3)]
    own_rows = span(row_base, rows_own)
    local_x = pltpu.make_async_copy(x_hbm.at[own_rows], dx_out.at[own_rows], l_x)
    local_t = pltpu.make_async_copy(t_hbm.at[own_rows], tbuf.at[mod, pl.ds(0, rows_own)], l_t)
    for k in range(3):
        local_w[k].start()
        local_u[k].start()
    local_x.start()
    local_t.start()
    pl.semaphore_wait(barrier, len(peers))

    for k in range(3):
        w_copy(k, 1).start()
        w_copy(k, 0).start()

    for copy in local_u:
        copy.wait()
    for kind in range(3):
        u_copy(kind).start()

    def start_targets(idx, at, size):
        t_copy(0, idx, at, size).start()
        t_copy(1, idx, at, size).start()

    each_chunk(PLAIN + SHARED, 0, 0, start_targets)
    t_sib = remote(t_hbm.at[span((1 - core) * rows_own, rows_own)], tbuf.at[mod, pl.ds(0, rows_own)], s_send, s_recv, p_sib)
    t_sib.start()
    acc[...] = jnp.zeros_like(acc)
    facc[...] = jnp.zeros_like(facc)
    stat[...] = jnp.zeros_like(stat)
    fstat[...] = jnp.zeros_like(fstat)

    def relay_x(k):
        w_copy(k, 1).wait_recv()
        w_copy(k, 2).start()
        w_copy(k, 3).start()

    def relay_y(k):
        w_copy(k, 2).wait_recv()
        w_copy(k, 4).start()

    own_cols = span(256 * chip, 256)

    def fold(val):
        return jnp.sum(val.reshape(val.shape[0] // 8, 8, val.shape[1]), axis=0)

    def leaky(val):
        return jnp.maximum(val, 0.2 * val).astype(BF16)

    def add_grad(ref, e_val, x_val):
        part = dot_tn(e_val, x_val)
        ref[0] += part[:128]
        ref[1] += part[128:]

    def residual(y_val, slab, rows, sums, at):
        res = y_val - tbuf[slab, rows, :].astype(F32)
        grad = res * inv_batch
        if sums is not None:
            sums[0, :, at:at + 128] += fold(res * res)
            sums[1, :, at:at + 128] += fold(grad * y_val)
        e2[rows, span(128 * slab, 128)] = grad.astype(BF16)

    def last_layer(rows, sums):
        y_val = dot_nt(x2[rows, :], wbuf[2]) * inv_sigma[2]
        first = chip == 0
        own = jnp.where(first, y_val[:, :256], y_val[:, 256:])
        y2[rows, :] = jnp.where(first, y_val[:, 256:], y_val[:, :256])
        for j in range(2):
            residual(own[:, 128 * j:128 * j + 128], 2 * chip + j, rows, sums, 256 + 128 * j)

    inv_sigma = []
    for k in range(3):
        relay_x(k)
    for kind in range(3):
        f_copy(kind).start()
    relay_y(0)
    relay_y(1)
    for k in range(3):
        local_w[k].wait()
        if k == 0:
            arrived(ubuf.at[:, pl.ds(0, 3)], u_recv)
        arrived(wbuf.at[k, pl.ds(0, 256)], w_recv.at[k, 0])
        u_row = jnp.concatenate([ubuf[k, j] for j in range(4)], axis=1)
        p_vec = jnp.sum(dot_nn(split_rows(u_row), wbuf[k]), axis=0, keepdims=True)
        norm = jnp.sqrt(jnp.sum(p_vec * p_vec, axis=1, keepdims=True))
        v_vec = p_vec / jnp.maximum(norm, 1e-12)
        s_vec = jnp.sum(dot_nt(split_rows(v_vec), wbuf[k]), axis=0, keepdims=True)
        sigma = jnp.sqrt(jnp.sum(s_vec * s_vec, axis=1, keepdims=True))
        pack_out[k:k + 1, :] = v_vec
        srow[k] = jnp.broadcast_to(s_vec / sigma, srow.shape[1:])
        pack_out[3 + k:4 + k, 0:128] = srow[k, 0:1, span(128 * mod, 128)]
        pack_out[6 + k:7 + k, :] = jnp.broadcast_to(sigma, (1, pack_out.shape[1]))
        inv = 1.0 / sigma
        inv_sigma.append(inv)
        if k == 0:
            relay_y(2)
        if k == 0:
            local_x.wait()
        if k == 2:
            local_t.wait()
            t_sib.wait_recv()

        def forward(c, carry, k=k, inv=inv):
            rows = span(c * FWD_ROWS, FWD_ROWS)
            if k == 0:
                y_val = dot_nt(dx_out[span(row_base + c * FWD_ROWS, FWD_ROWS), :], wbuf[0]) * inv
                y0[rows, :] = y_val
                x1[rows, :] = leaky(y_val)
            elif k == 1:
                y_val = dot_nt(x1[rows, :], wbuf[1]) * inv
                y1[rows, :] = y_val
                x2[rows, :] = leaky(y_val)
            else:
                last_layer(rows, stat)
                add_grad(acc.at[2], e2[rows, own_cols], x2[rows, :])
            return carry

        lax.fori_loop(0, rows_own // FWD_ROWS, forward, 0)

    def d_copy(k):
        return remote(acc.at[k, 1 - core], rbuf.at[k], d_send, d_recv.at[k], p_sib)

    def fd_copy(k):
        return remote(fsend.at[k], frbuf.at[k], d_send, d_recv.at[4 + k], p_sib)

    def p_copy(k):
        part = pl.ds((256, 0, 128)[k], (8, 128, 128)[k])
        return remote(p_own.at[part], p_other.at[part], d_send, d_recv.at[8 + k], p_y)

    s_copy = remote(sstat, rstat, d_send, d_recv.at[3], p_sib)
    fs_copy = remote(fsstat, frstat, d_send, d_recv.at[6], p_sib)
    g_copy = remote(g_own, g_other, d_send, d_recv.at[7], p_y)

    def dx_copy(at, size):
        ref = dx_out.at[tile(row_base + at, size)]
        return remote(ref, ref, e_send, e_recv, p_sib)

    def backward(at, size, sums, grads, idx=None, mid=None):
        rows = tile(at, size)
        for j in range(2):
            residual(y2[rows, 128 * j:128 * j + 128], 2 - 2 * chip + j, rows, sums, 128 * j)
        back = (dot_nn(e2[rows, :], wbuf[2]) * inv_sigma[2]).astype(BF16).astype(F32)
        y_val = y1[rows, :]
        grad = back * jnp.where(y_val > 0, 1.0, 0.2)
        sums[2] += fold(grad * y_val)
        e1[:size] = grad.astype(BF16)
        add_grad(grads.at[1], e1[:size, own_cols], x1[rows, :])
        back = (dot_nn(e1[:size], wbuf[1]) * inv_sigma[1]).astype(BF16).astype(F32)
        y_val = y0[rows, :]
        grad = back * jnp.where(y_val > 0, 1.0, 0.2)
        sums[3] += fold(grad * y_val)
        e0[:size] = grad.astype(BF16)
        if mid is not None:
            mid(1)
        if idx is None:
            add_grad(grads.at[0], e0[:size, own_cols], xfor[tile(at - rows_own, size), :])
            if mid is not None:
                mid(0)
        else:
            x_rows = tile(row_base + at, size)
            add_grad(grads.at[0], e0[:size, own_cols], dx_out[x_rows, :])
            if mid is not None:
                mid(0)
            dx_out[x_rows, :] = (dot_nn(e0[:size], wbuf[0]) * inv_sigma[0]).astype(BF16)

    row = lax.broadcasted_iota(jnp.int32, sstat.shape, 0)

    def gather_sums(ref_sums):
        mine = jnp.zeros(sstat.shape, F32)
        for i in range(4):
            mine = jnp.where(row == i, jnp.sum(ref_sums(i), axis=0, keepdims=True), mine)
        return mine

    def own_chunk(idx, at, size, sums, grads, mid=None):
        arrived(tbuf.at[pl.ds(0, 2), tile(at, size)], t_recv.at[idx])
        backward(at, size, sums, grads, idx, mid)

    n_big = PLAIN[0][1]

    def plain_send(k):
        if k == 0:
            sstat[...] = gather_sums(lambda i: stat[i])
        d_copy(k).start()
        if k == 0:
            s_copy.start()

    def plain_chunk(idx, at, size):
        if size == BIG_ROWS:
            @pl.when(idx == 0)
            def _():
                d_copy(2).start()

            @pl.when(idx == 1)
            def _():
                d_copy(2).wait_recv()
                g_own[...] = acc[2, core] + rbuf[2]

            @pl.when(idx == 2)
            def _():
                g_copy.start()

            @pl.when(idx == n_big - 2)
            def _():
                arrived(x1.at[pl.ds(0, 3 * SHARED_ROWS // 2)], f_recv)

                def forward_on(j, h_at, h_size):
                    h_copy(0, j, h_at, h_size).start()
                    h_copy(1, j, h_at, h_size).start()

                each_chunk(SHARED, 0, rows_own, forward_on)

            @pl.when(idx == n_big - 1)
            def _():
                rows = pl.ds(rows_own, SHARED_ROWS)
                y_val = dot_nt(xfor[...], wbuf[0]) * inv_sigma[0]
                y0[rows, :] = y_val
                x1[rows, :] = leaky(y_val)
                y_val = dot_nt(x1[rows, :], wbuf[1]) * inv_sigma[1]
                y1[rows, :] = y_val
                x2[rows, :] = leaky(y_val)
                last_layer(rows, None)

        last = isinstance(at, int) and at + size == shared_at
        own_chunk(idx, at, size, stat, acc, plain_send if last else None)
        dx_copy(at, size).start()

    each_chunk(PLAIN, 0, 0, plain_chunk)

    d_copy(1).wait_recv()
    p_own[0:128, :] = acc[1, core] + rbuf[1]
    d_copy(0).wait_recv()
    p_copy(1).start()
    p_own[128:256, :] = acc[0, core] + rbuf[0]
    s_copy.wait_recv()
    p_copy(2).start()
    p_own[256:264, :] = sstat[...] + rstat[...]

    def shared_chunk(idx, at, size):
        own_chunk(idx, at, size, fstat.at[0], facc.at[0])
        dx_copy(at, size).start()

        @pl.when(idx == N_PLAIN)
        def _():
            p_copy(0).start()

    each_chunk(SHARED, N_PLAIN, shared_at, shared_chunk)

    def last_send(k):
        fsend[k] = facc[0, k, 1 - core] + facc[1, k, 1 - core]
        if k == 0:
            fd_copy(1).start()
            fsstat[...] = gather_sums(lambda i: fstat[0, i] + fstat[1, i])
            fd_copy(0).start()
            fs_copy.start()

    def foreign_chunk(idx, at, size):
        arrived(tbuf.at[pl.ds(0, 2), tile(at, size)], h_recv.at[idx])
        last = isinstance(at, int) and at + size == rows_own + SHARED_ROWS
        backward(at, size, fstat.at[1], facc.at[1], None, last_send if last else None)

    each_chunk(SHARED, 0, rows_own, foreign_chunk)

    g_copy.wait_recv()
    tot_out[256:384, :] = g_own[...] + g_other[...]
    for k in range(3):
        p_copy(k).wait_recv()
    for i, k in enumerate((1, 0)):
        part = slice(128 * i, 128 * i + 128)
        fd_copy(k).wait_recv()
        tot_out[part, :] = (p_own[part, :] + p_other[part, :]) + ((facc[0, k, core] + facc[1, k, core]) + frbuf[k])
    fs_copy.wait_recv()
    tot_out[384:392, :] = (p_own[256:264, :] + p_other[256:264, :]) + (fsstat[...] + frstat[...])

    arrived(x1.at[pl.ds(0, 3 * 384)], w_send)
    arrived(ubuf.at[:, pl.ds(0, 3)], u_send)
    arrived(t_hbm, t_send)
    arrived(tbuf.at[mod, pl.ds(0, rows_own)], s_send)
    arrived(x1.at[pl.ds(0, 3 * SHARED_ROWS // 2)], f_send)
    arrived(tbuf.at[pl.ds(0, 2), pl.ds(rows_own, SHARED_ROWS)], h_send)
    arrived(y0.at[pl.ds(0, 8 * 128 + 24)], d_send)
    arrived(dx_out.at[own_rows], e_send)
    arrived(dx_out.at[own_rows], e_recv)


def finish_kernel(loss_scale, dx_in, tot, pack, dx_ref, dw0, dw1, dw2, v0, v1, v2, n0, n1, n2, sig_out, loss_out,
                  grads, sig_row, loss_row, sems, out_sems):
    parts = sems.shape[0]
    rows = dx_in.shape[0] // parts
    copies = [pltpu.make_async_copy(dx_in.at[pl.ds(i * rows, rows)], dx_ref.at[pl.ds(i * rows, rows)], sems.at[i]) for i in range(parts)]
    for copy in copies:
        copy.start()

    def out_copy(src, dst):
        copy = pltpu.make_async_copy(src, dst, out_sems.at[len(copies) - parts])
        copy.start()
        copies.append(copy)

    for k, (v_out, n_out) in enumerate(((v0, n0), (v1, n1), (v2, n2))):
        out_copy(pack.at[k:k + 1, :], v_out)
        out_copy(pack.at[3 + k:4 + k, 0:128], n_out)
    lane = lax.broadcasted_iota(jnp.int32, (1, 128), 1)
    row = jnp.where(lane == 0, pack[6:7, 0:128], jnp.where(lane == 1, pack[7:8, 0:128], pack[8:9, 0:128]))
    sig_row[...] = row[:, :3]
    stats = jnp.sum(tot[384:392, :], axis=1, keepdims=True)
    loss_row[...] = loss_scale * stats[0:1]
    for k, at in enumerate((128, 0, 256)):
        inv = 1.0 / pack[6 + k:7 + k, 0:1]
        u_col = jnp.transpose(jnp.broadcast_to(pack[3 + k:4 + k, 0:128], (128, 128)))[:, 0:1]
        grads[k] = tot[at:at + 128, :] * inv - (stats[3 - k:4 - k] * inv) * (u_col * pack[k:k + 1, :])
    out_copy(sig_row, sig_out)
    out_copy(loss_row, loss_out)
    for k, out in enumerate((dw0, dw1, dw2)):
        out_copy(grads.at[k], out)
    for copy in copies:
        copy.wait()


def solution(mesh):
    data_size = mesh.shape["data"]
    row_spec = P(("replica", "model"), None)
    vec_spec = P(("replica", "model"))
    batch_spec = P(("replica", "data"), None)
    target_spec = P(("replica", "data"), "model")
    part_spec = P("replica")

    def local_step(x_in, w_in, w_mid, w_out, u_in, u_mid, u_out, target):
        rows, width = x_in.shape
        half = rows // 2
        ext = half + SHARED_ROWS
        batch_total = rows * data_size
        any_spec = pl.BlockSpec(memory_space=pl.ANY)
        vmem_spec = pl.BlockSpec(memory_space=pltpu.VMEM)
        dma = pltpu.SemaphoreType.DMA
        vm = pltpu.VMEM
        dx_all, tot, pack = pl.pallas_call(
            functools.partial(main_kernel, 1.0 / batch_total),
            out_shape=[vm((rows, width), BF16), vm((392, width), F32), vm((16, width), F32)],
            in_specs=[any_spec] * 8,
            out_specs=[vmem_spec] * 3,
            scratch_shapes=[
                vm((ext, width), BF16), vm((ext, width), BF16),
                vm((ext, width), F32), vm((ext, width), F32), vm((ext, 256), F32),
                vm((4, ext, 128), BF16),
                vm((3, width, width), BF16),
                vm((3, 4, 1, 128), F32),
                vm((ext, width), BF16), vm((BIG_ROWS, width), BF16), vm((BIG_ROWS, width), BF16),
                vm((SHARED_ROWS, width), BF16),
                vm((3, 2, 128, width), F32), vm((2, 2, 2, 128, width), F32),
                vm((3, 128, width), F32), vm((2, 128, width), F32), vm((2, 128, width), F32),
                vm((128, width), F32), vm((128, width), F32),
                vm((264, width), F32), vm((264, width), F32),
                vm((4, 8, width), F32), vm((2, 4, 8, width), F32),
                vm((8, width), F32), vm((8, width), F32), vm((8, width), F32), vm((8, width), F32),
                vm((3, 8, width), F32),
                dma(()), dma((3, 3)), dma(()), dma(()),
                dma(()), dma((N_PLAIN + N_SHARED,)), dma(()), dma(()), dma(()), dma(()), dma(()), dma((11,)),
                dma(()), dma(()), dma(()), dma((N_SHARED,)),
                dma((3,)), dma((3,)), dma(()), dma(()),
            ],
            compiler_params=pltpu.CompilerParams(
                collective_id=0, has_side_effects=True, vmem_limit_bytes=55 * 2**20),
            name="fused_step",
        )(x_in, w_in, w_mid, w_out, u_in.reshape(1, 128), u_mid.reshape(1, 128), u_out.reshape(1, 128), target)

        f32 = lambda *shape: jax.ShapeDtypeStruct(shape, F32)
        finals = pl.pallas_call(
            functools.partial(finish_kernel, 0.5 / batch_total),
            out_shape=[jax.ShapeDtypeStruct((rows, width), BF16)] + [f32(128, width)] * 3 + [f32(1, width)] * 3 + [
                f32(1, 128)] * 3 + [f32(1, 3), f32(1, 1)],
            in_specs=[vmem_spec] * 3,
            out_specs=[any_spec] * 12,
            scratch_shapes=[vm((3, 128, width), F32), vm((1, 3), F32), vm((1, 1), F32), dma((4,)), dma((11,))],
            compiler_params=pltpu.CompilerParams(vmem_limit_bytes=8 * 2**20),
            name="finish",
        )(dx_all, tot, pack)
        grad_x, dw0, dw1, dw2, v0, v1, v2, n0, n1, n2, sig, loss = finals
        return (loss.reshape(1), grad_x, dw0, dw1, dw2, n0.reshape(128), n1.reshape(128), n2.reshape(128),
                v0.reshape(width), v1.reshape(width), v2.reshape(width), sig.reshape(3))

    in_specs = (batch_spec, row_spec, row_spec, row_spec, vec_spec, vec_spec, vec_spec, target_spec)
    out_specs = (part_spec, batch_spec, row_spec, row_spec, row_spec, vec_spec, vec_spec, vec_spec, part_spec, part_spec, part_spec, part_spec)
    return jax.shard_map(local_step, mesh=mesh, in_specs=in_specs, out_specs=out_specs, check_vma=False)
```

```python
import functools

import jax
import jax.numpy as jnp
from jax import lax
from jax.experimental import pallas as pl
from jax.experimental.pallas import tpu as pltpu
from jax.sharding import PartitionSpec as P

MESH = pl.DeviceIdType.MESH
F32 = jnp.float32
BF16 = jnp.bfloat16
FWD_ROWS = 1024
BIG_ROWS = 512
PLAIN = ((512, 6), (256, 1), (192, 1))
SHARED = ((256, 1), (192, 1), (128, 1))
SHARED_ROWS = sum(size * count for size, count in SHARED)
N_PLAIN = sum(count for _, count in PLAIN)
LAST = PLAIN[-1][0]
N_SHARED = sum(count for _, count in SHARED)


def dot_nt(lhs, rhs):
    return lax.dot_general(lhs, rhs, (((1,), (1,)), ((), ())), preferred_element_type=F32)


def dot_nn(lhs, rhs):
    return lax.dot_general(lhs, rhs, (((1,), (0,)), ((), ())), preferred_element_type=F32)


def dot_tn(lhs, rhs):
    return lax.dot_general(lhs, rhs, (((0,), (0,)), ((), ())), preferred_element_type=F32)


def split_rows(vec):
    width = vec.shape[1]
    high = vec.astype(BF16).astype(F32)
    rest = vec - high
    mid = rest.astype(BF16).astype(F32)
    low = rest - mid
    row = lax.broadcasted_iota(jnp.int32, (16, width), 0)
    stacked = jnp.where(row == 0, high, jnp.where(row == 1, mid, jnp.where(row == 2, low, 0.0)))
    return stacked.astype(BF16)


def main_kernel(inv_batch, x_hbm, w0_hbm, w1_hbm, w2_hbm, u0_hbm, u1_hbm, u2_hbm, t_hbm,
                dx_out, tot_out, pack_out,
                x1, x2, y0, y1, y2, tbuf, wbuf, ubuf, e2, e1, e0, xfor, acc, facc, rbuf, frbuf, fsend,
                g_own, g_other, p_own, p_other, stat, fstat, sstat, rstat, fsstat, frstat, srow, sx, se, eq,
                w_send, w_recv, u_send, u_recv, t_send, t_recv, s_send, s_recv, e_send, e_recv, d_send, d_recv,
                f_send, f_recv, h_send, h_recv, q_send, q_recv, l_w, l_u, l_t, l_x, l_q):
    rep, dat, mod = lax.axis_index("replica"), lax.axis_index("data"), lax.axis_index("model")
    core = lax.rem(mod, 2)
    chip = mod // 2
    sib = mod + 1 - 2 * core
    cnt = lax.rem(mod + 2, 4)
    crs = lax.rem(sib + 2, 4)
    p_sib, p_cnt, p_crs = (rep, dat, sib), (rep, dat, cnt), (rep, dat, crs)
    p_y, p_ys = (rep, 1 - dat, mod), (rep, 1 - dat, sib)
    rows_own = x_hbm.shape[0] // 2
    shared_at = rows_own - SHARED_ROWS
    row_base = core * rows_own

    def each_chunk(groups, first, at, body):
        for size, count in groups:
            def step(i, carry, size=size, first=first, at=at):
                body(first + i, at + i * size, size)
                return carry
            if count == 1:
                step(0, 0)
            else:
                lax.fori_loop(0, count, step, 0)
            first, at = first + count, at + size * count
    w_hbm = [w0_hbm, w1_hbm, w2_hbm]
    u_hbm = [u0_hbm, u1_hbm, u2_hbm]

    def remote(src, dst, ssem, rsem, peer):
        return pltpu.make_async_remote_copy(src_ref=src, dst_ref=dst, send_sem=ssem, recv_sem=rsem,
                                            device_id=peer, device_id_type=MESH)

    def arrived(ref, sem):
        pltpu.make_async_copy(ref, ref, sem).wait()

    def span(start, size):
        return pl.ds(pl.multiple_of(start, size), size)

    def tile(start, size):
        return pl.ds(pl.multiple_of(start, 64), size)

    def w_copy(layer, kind):
        ssem, rsem = w_send, w_recv.at[layer, (0, 1, 2, 0, 0)[kind]]
        if kind == 0:
            return remote(w_hbm[layer], wbuf.at[layer, span(128 * mod, 128)], ssem, rsem, p_sib)
        if kind == 1:
            return remote(w_hbm[layer].at[span(64 * dat, 64)], wbuf.at[layer, span(128 * mod + 64 * dat, 64)], ssem, rsem, p_cnt)
        half = 1 - dat if kind == 4 else dat
        ref = wbuf.at[layer, span(128 * cnt + 64 * half, 64)]
        return remote(ref, ref, ssem, rsem, p_y if kind == 2 else p_sib)

    def u_copy(kind):
        ref = ubuf.at[:, mod]
        return remote(ref, ref, u_send, u_recv, (p_sib, p_cnt, p_crs)[kind])

    def t_copy(kind, idx, at, size):
        other_core = core if kind == 0 else 1 - core
        return remote(t_hbm.at[tile(other_core * rows_own + at, size)], tbuf.at[mod, tile(at, size)],
                      t_send, t_recv.at[idx], p_cnt if kind == 0 else p_crs)

    def f_copy(kind):
        if kind == 0:
            src, dst, peer = x_hbm.at[tile(row_base + shared_at, SHARED_ROWS)], xfor, p_y
        else:
            other_core = core if kind == 1 else 1 - core
            src = t_hbm.at[tile(other_core * rows_own + shared_at, SHARED_ROWS)]
            dst, peer = tbuf.at[mod, tile(rows_own, SHARED_ROWS)], p_y if kind == 1 else p_ys
        return remote(src, dst, f_send, f_recv, peer)

    def h_copy(kind, idx, at, size):
        ref = tbuf.at[mod if kind == 0 else sib, tile(at, size)]
        return remote(ref, ref, h_send, h_recv.at[idx], p_cnt)

    barrier = pltpu.get_barrier_semaphore()
    peers = (p_sib, p_cnt, p_crs, p_y, p_ys)
    for peer in peers:
        pl.semaphore_signal(barrier, inc=1, device_id=peer, device_id_type=MESH)
    local_w = [pltpu.make_async_copy(w_hbm[k], wbuf.at[k, span(128 * mod, 128)], l_w.at[k]) for k in range(3)]
    local_u = [pltpu.make_async_copy(u_hbm[k], ubuf.at[k, mod], l_u.at[k]) for k in range(3)]
    own_rows = span(row_base, rows_own)
    local_x = pltpu.make_async_copy(x_hbm.at[own_rows], dx_out.at[own_rows], l_x)
    local_t = pltpu.make_async_copy(t_hbm.at[own_rows], tbuf.at[mod, pl.ds(0, rows_own)], l_t)
    for k in range(3):
        local_w[k].start()
        local_u[k].start()
    local_x.start()
    local_t.start()
    last_at = shared_at - LAST
    local_q = pltpu.make_async_copy(x_hbm.at[tile((1 - core) * rows_own + last_at, LAST)], sx.at[0], l_q)
    local_q.start()
    pl.semaphore_wait(barrier, len(peers))

    for k in range(3):
        w_copy(k, 1).start()
        w_copy(k, 0).start()

    for copy in local_u:
        copy.wait()
    for kind in range(3):
        u_copy(kind).start()

    def start_targets(idx, at, size):
        t_copy(0, idx, at, size).start()
        t_copy(1, idx, at, size).start()

    each_chunk(PLAIN + SHARED, 0, 0, start_targets)
    t_sib = remote(t_hbm.at[span((1 - core) * rows_own, rows_own)], tbuf.at[mod, pl.ds(0, rows_own)], s_send, s_recv, p_sib)
    t_sib.start()
    acc[...] = jnp.zeros_like(acc)
    facc[...] = jnp.zeros_like(facc)
    stat[...] = jnp.zeros_like(stat)
    fstat[...] = jnp.zeros_like(fstat)

    def relay_x(k):
        w_copy(k, 1).wait_recv()
        w_copy(k, 2).start()
        w_copy(k, 3).start()

    def relay_y(k):
        w_copy(k, 2).wait_recv()
        w_copy(k, 4).start()

    own_cols = span(256 * chip, 256)
    my_cols = span(128 * mod, 128)

    def q_copy(kind):
        if kind == 2:
            src, dst = x1.at[pl.ds(last_at, LAST)], sx.at[1]
        else:
            src, dst = eq.at[kind, :, span(128 * sib, 128)], se.at[kind]
        return remote(src, dst, q_send, q_recv.at[kind], p_sib)

    def fold(val):
        return jnp.sum(val.reshape(val.shape[0] // 8, 8, val.shape[1]), axis=0)

    def leaky(val):
        return jnp.maximum(val, 0.2 * val).astype(BF16)

    def add_grad(ref, e_val, x_val):
        part = dot_tn(e_val, x_val)
        ref[0] += part[:128]
        ref[1] += part[128:]

    def residual(y_val, slab, rows, sums, at):
        res = y_val - tbuf[slab, rows, :].astype(F32)
        grad = res * inv_batch
        if sums is not None:
            sums[0, :, at:at + 128] += fold(res * res)
            sums[1, :, at:at + 128] += fold(grad * y_val)
        e2[rows, span(128 * slab, 128)] = grad.astype(BF16)

    def last_layer(rows, sums):
        y_val = dot_nt(x2[rows, :], wbuf[2]) * inv_sigma[2]
        first = chip == 0
        own = jnp.where(first, y_val[:, :256], y_val[:, 256:])
        y2[rows, :] = jnp.where(first, y_val[:, 256:], y_val[:, :256])
        for j in range(2):
            residual(own[:, 128 * j:128 * j + 128], 2 * chip + j, rows, sums, 256 + 128 * j)

    inv_sigma = []
    for k in range(3):
        relay_x(k)
    for kind in range(3):
        f_copy(kind).start()
    relay_y(0)
    relay_y(1)
    for k in range(3):
        local_w[k].wait()
        if k == 0:
            arrived(ubuf.at[:, pl.ds(0, 3)], u_recv)
        arrived(wbuf.at[k, pl.ds(0, 256)], w_recv.at[k, 0])
        u_row = jnp.concatenate([ubuf[k, j] for j in range(4)], axis=1)
        p_vec = jnp.sum(dot_nn(split_rows(u_row), wbuf[k]), axis=0, keepdims=True)
        norm = jnp.sqrt(jnp.sum(p_vec * p_vec, axis=1, keepdims=True))
        v_vec = p_vec / jnp.maximum(norm, 1e-12)
        s_vec = jnp.sum(dot_nt(split_rows(v_vec), wbuf[k]), axis=0, keepdims=True)
        sigma = jnp.sqrt(jnp.sum(s_vec * s_vec, axis=1, keepdims=True))
        pack_out[k:k + 1, :] = v_vec
        srow[k] = jnp.broadcast_to(s_vec / sigma, srow.shape[1:])
        pack_out[3 + k:4 + k, 0:128] = srow[k, 0:1, span(128 * mod, 128)]
        pack_out[6 + k:7 + k, :] = jnp.broadcast_to(sigma, (1, pack_out.shape[1]))
        inv = 1.0 / sigma
        inv_sigma.append(inv)
        if k == 0:
            relay_y(2)
        if k == 0:
            local_x.wait()
        if k == 2:
            local_t.wait()
            t_sib.wait_recv()

        def forward(c, carry, k=k, inv=inv):
            rows = span(c * FWD_ROWS, FWD_ROWS)
            if k == 0:
                y_val = dot_nt(dx_out[span(row_base + c * FWD_ROWS, FWD_ROWS), :], wbuf[0]) * inv
                y0[rows, :] = y_val
                x1[rows, :] = leaky(y_val)
            elif k == 1:
                y_val = dot_nt(x1[rows, :], wbuf[1]) * inv
                y1[rows, :] = y_val
                x2[rows, :] = leaky(y_val)
            else:
                last_layer(rows, stat)
                add_grad(acc.at[2], e2[rows, own_cols], x2[rows, :])
            return carry

        lax.fori_loop(0, rows_own // FWD_ROWS, forward, 0)

    def d_copy(k):
        return remote(acc.at[k, 1 - core], rbuf.at[k], d_send, d_recv.at[k], p_sib)

    def fd_copy(k):
        return remote(fsend.at[k], frbuf.at[k], d_send, d_recv.at[4 + k], p_sib)

    def p_copy(k):
        part = pl.ds((256, 0, 128)[k], (8, 128, 128)[k])
        return remote(p_own.at[part], p_other.at[part], d_send, d_recv.at[8 + k], p_y)

    s_copy = remote(sstat, rstat, d_send, d_recv.at[3], p_sib)
    fs_copy = remote(fsstat, frstat, d_send, d_recv.at[6], p_sib)
    g_copy = remote(g_own, g_other, d_send, d_recv.at[7], p_y)

    def dx_copy(at, size):
        ref = dx_out.at[tile(row_base + at, size)]
        return remote(ref, ref, e_send, e_recv, p_sib)

    def backward(at, size, sums, grads, idx=None, mid=None, split=False):
        rows = tile(at, size)
        b0, b1 = (eq.at[0], eq.at[1]) if split else (e0, e1)
        for j in range(2):
            residual(y2[rows, 128 * j:128 * j + 128], 2 - 2 * chip + j, rows, sums, 128 * j)
        back = (dot_nn(e2[rows, :], wbuf[2]) * inv_sigma[2]).astype(BF16).astype(F32)
        y_val = y1[rows, :]
        grad = back * jnp.where(y_val > 0, 1.0, 0.2)
        sums[2] += fold(grad * y_val)
        b1[:size] = grad.astype(BF16)
        if split:
            grads[1, core] += dot_tn(b1[:size, my_cols], x1[rows, :])
        else:
            add_grad(grads.at[1], b1[:size, own_cols], x1[rows, :])
        back = (dot_nn(b1[:size], wbuf[1]) * inv_sigma[1]).astype(BF16).astype(F32)
        if mid is not None:
            mid(1)
        y_val = y0[rows, :]
        grad = back * jnp.where(y_val > 0, 1.0, 0.2)
        sums[3] += fold(grad * y_val)
        b0[:size] = grad.astype(BF16)
        if idx is None:
            add_grad(grads.at[0], b0[:size, own_cols], xfor[tile(at - rows_own, size), :])
            if mid is not None:
                mid(0)
        else:
            x_rows = tile(row_base + at, size)
            if split:
                grads[0, core] += dot_tn(b0[:size, my_cols], dx_out[x_rows, :])
                mid(0)
            else:
                add_grad(grads.at[0], b0[:size, own_cols], dx_out[x_rows, :])
            dx_out[x_rows, :] = (dot_nn(b0[:size], wbuf[0]) * inv_sigma[0]).astype(BF16)

    row = lax.broadcasted_iota(jnp.int32, sstat.shape, 0)

    def gather_sums(ref_sums):
        mine = jnp.zeros(sstat.shape, F32)
        for i in range(4):
            mine = jnp.where(row == i, jnp.sum(ref_sums(i), axis=0, keepdims=True), mine)
        return mine

    def own_chunk(idx, at, size, sums, grads, mid=None, split=False):
        arrived(tbuf.at[pl.ds(0, 2), tile(at, size)], t_recv.at[idx])
        if isinstance(idx, int) and idx == N_PLAIN:
            p_copy(2).start()
        backward(at, size, sums, grads, idx, mid, split)

    n_big = PLAIN[0][1]

    def plain_send(k):
        q_copy(k).start()

    def plain_chunk(idx, at, size):
        if size == BIG_ROWS:
            @pl.when(idx == 0)
            def _():
                d_copy(2).start()
                q_copy(2).start()

            @pl.when(idx == 1)
            def _():
                d_copy(2).wait_recv()
                g_own[...] = acc[2, core] + rbuf[2]

            @pl.when(idx == 2)
            def _():
                g_copy.start()

            @pl.when(idx == n_big - 2)
            def _():
                arrived(x1.at[pl.ds(0, 3 * SHARED_ROWS // 2)], f_recv)

                def forward_on(j, h_at, h_size):
                    h_copy(0, j, h_at, h_size).start()
                    h_copy(1, j, h_at, h_size).start()

                each_chunk(SHARED, 0, rows_own, forward_on)

            @pl.when(idx == n_big - 1)
            def _():
                rows = pl.ds(rows_own, SHARED_ROWS)
                y_val = dot_nt(xfor[...], wbuf[0]) * inv_sigma[0]
                y0[rows, :] = y_val
                x1[rows, :] = leaky(y_val)
                y_val = dot_nt(x1[rows, :], wbuf[1]) * inv_sigma[1]
                y1[rows, :] = y_val
                x2[rows, :] = leaky(y_val)
                last_layer(rows, None)

        last = idx == N_PLAIN - 1 if isinstance(idx, int) else False
        own_chunk(idx, at, size, stat, acc, plain_send if last else None, last)
        dx_copy(at, size).start()
        if isinstance(idx, int) and idx == N_PLAIN - 2:
            d_copy(1).start()
            d_copy(0).start()

    each_chunk(PLAIN, 0, 0, plain_chunk)

    d_copy(1).wait_recv()
    q_copy(2).wait_recv()
    q_copy(1).wait_recv()
    p_own[0:128, :] = (acc[1, core] + rbuf[1]) + dot_tn(se[1], sx[1])
    sstat[...] = gather_sums(lambda i: stat[i])
    s_copy.start()
    p_copy(1).start()
    d_copy(0).wait_recv()
    local_q.wait()
    q_copy(0).wait_recv()
    p_own[128:256, :] = (acc[0, core] + rbuf[0]) + dot_tn(se[0], sx[0])

    def shared_chunk(idx, at, size):
        if idx == N_PLAIN + 1:
            p_copy(0).start()
        own_chunk(idx, at, size, fstat.at[0], facc.at[0])
        dx_copy(at, size).start()
        if idx == N_PLAIN:
            s_copy.wait_recv()
            p_own[256:264, :] = sstat[...] + rstat[...]

    each_chunk(SHARED, N_PLAIN, shared_at, shared_chunk)

    def last_send(k):
        fsend[k] = facc[0, k, 1 - core] + facc[1, k, 1 - core]
        if k == 1:
            fd_copy(1).start()
        if k == 0:
            fsstat[...] = gather_sums(lambda i: fstat[0, i] + fstat[1, i])
            fd_copy(0).start()
            fs_copy.start()

    def foreign_chunk(idx, at, size):
        arrived(tbuf.at[pl.ds(0, 2), tile(at, size)], h_recv.at[idx])
        last = isinstance(at, int) and at + size == rows_own + SHARED_ROWS
        backward(at, size, fstat.at[1], facc.at[1], None, last_send if last else None)

    each_chunk(SHARED, 0, rows_own, foreign_chunk)

    g_copy.wait_recv()
    tot_out[256:384, :] = g_own[...] + g_other[...]
    for k in range(3):
        p_copy(k).wait_recv()
    for i, k in enumerate((1, 0)):
        part = slice(128 * i, 128 * i + 128)
        fd_copy(k).wait_recv()
        tot_out[part, :] = (p_own[part, :] + p_other[part, :]) + ((facc[0, k, core] + facc[1, k, core]) + frbuf[k])
    fs_copy.wait_recv()
    tot_out[384:392, :] = (p_own[256:264, :] + p_other[256:264, :]) + (fsstat[...] + frstat[...])

    arrived(x1.at[pl.ds(0, 3 * 384)], w_send)
    arrived(ubuf.at[:, pl.ds(0, 3)], u_send)
    arrived(t_hbm, t_send)
    arrived(tbuf.at[mod, pl.ds(0, rows_own)], s_send)
    arrived(x1.at[pl.ds(0, 3 * SHARED_ROWS // 2)], f_send)
    arrived(tbuf.at[pl.ds(0, 2), pl.ds(rows_own, SHARED_ROWS)], h_send)
    arrived(y0.at[pl.ds(0, 8 * 128 + 24)], d_send)
    arrived(x1.at[pl.ds(0, 3 * LAST // 2)], q_send)
    arrived(dx_out.at[own_rows], e_send)
    arrived(dx_out.at[own_rows], e_recv)


def finish_kernel(loss_scale, dx_in, tot, pack, dx_ref, dw0, dw1, dw2, v0, v1, v2, n0, n1, n2, sig_out, loss_out,
                  grads, sig_row, loss_row, sems, out_sems):
    parts = sems.shape[0]
    rows = dx_in.shape[0] // parts
    copies = [pltpu.make_async_copy(dx_in.at[pl.ds(i * rows, rows)], dx_ref.at[pl.ds(i * rows, rows)], sems.at[i]) for i in range(parts)]
    for copy in copies:
        copy.start()

    def out_copy(src, dst):
        copy = pltpu.make_async_copy(src, dst, out_sems.at[len(copies) - parts])
        copy.start()
        copies.append(copy)

    for k, (v_out, n_out) in enumerate(((v0, n0), (v1, n1), (v2, n2))):
        out_copy(pack.at[k:k + 1, :], v_out)
        out_copy(pack.at[3 + k:4 + k, 0:128], n_out)
    lane = lax.broadcasted_iota(jnp.int32, (1, 128), 1)
    row = jnp.where(lane == 0, pack[6:7, 0:128], jnp.where(lane == 1, pack[7:8, 0:128], pack[8:9, 0:128]))
    sig_row[...] = row[:, :3]
    stats = jnp.sum(tot[384:392, :], axis=1, keepdims=True)
    loss_row[...] = loss_scale * stats[0:1]
    for k, at in enumerate((128, 0, 256)):
        inv = 1.0 / pack[6 + k:7 + k, 0:1]
        u_col = jnp.transpose(jnp.broadcast_to(pack[3 + k:4 + k, 0:128], (128, 128)))[:, 0:1]
        grads[k] = tot[at:at + 128, :] * inv - (stats[3 - k:4 - k] * inv) * (u_col * pack[k:k + 1, :])
    out_copy(sig_row, sig_out)
    out_copy(loss_row, loss_out)
    for k, out in enumerate((dw0, dw1, dw2)):
        out_copy(grads.at[k], out)
    for copy in copies:
        copy.wait()


def solution(mesh):
    data_size = mesh.shape["data"]
    row_spec = P(("replica", "model"), None)
    vec_spec = P(("replica", "model"))
    batch_spec = P(("replica", "data"), None)
    target_spec = P(("replica", "data"), "model")
    part_spec = P("replica")

    def local_step(x_in, w_in, w_mid, w_out, u_in, u_mid, u_out, target):
        rows, width = x_in.shape
        half = rows // 2
        ext = half + SHARED_ROWS
        batch_total = rows * data_size
        any_spec = pl.BlockSpec(memory_space=pl.ANY)
        vmem_spec = pl.BlockSpec(memory_space=pltpu.VMEM)
        dma = pltpu.SemaphoreType.DMA
        vm = pltpu.VMEM
        dx_all, tot, pack = pl.pallas_call(
            functools.partial(main_kernel, 1.0 / batch_total),
            out_shape=[vm((rows, width), BF16), vm((392, width), F32), vm((16, width), F32)],
            in_specs=[any_spec] * 8,
            out_specs=[vmem_spec] * 3,
            scratch_shapes=[
                vm((ext, width), BF16), vm((ext, width), BF16),
                vm((ext, width), F32), vm((ext, width), F32), vm((ext, 256), F32),
                vm((4, ext, 128), BF16),
                vm((3, width, width), BF16),
                vm((3, 4, 1, 128), F32),
                vm((ext, width), BF16), vm((BIG_ROWS, width), BF16), vm((BIG_ROWS, width), BF16),
                vm((SHARED_ROWS, width), BF16),
                vm((3, 2, 128, width), F32), vm((2, 2, 2, 128, width), F32),
                vm((3, 128, width), F32), vm((2, 128, width), F32), vm((2, 128, width), F32),
                vm((128, width), F32), vm((128, width), F32),
                vm((264, width), F32), vm((264, width), F32),
                vm((4, 8, width), F32), vm((2, 4, 8, width), F32),
                vm((8, width), F32), vm((8, width), F32), vm((8, width), F32), vm((8, width), F32),
                vm((3, 8, width), F32),
                vm((2, LAST, width), BF16), vm((2, LAST, 128), BF16), vm((2, LAST, width), BF16),
                dma(()), dma((3, 3)), dma(()), dma(()),
                dma(()), dma((N_PLAIN + N_SHARED,)), dma(()), dma(()), dma(()), dma(()), dma(()), dma((11,)),
                dma(()), dma(()), dma(()), dma((N_SHARED,)), dma(()), dma((3,)),
                dma((3,)), dma((3,)), dma(()), dma(()), dma(()),
            ],
            compiler_params=pltpu.CompilerParams(
                collective_id=0, has_side_effects=True, vmem_limit_bytes=55 * 2**20),
            name="fused_step",
        )(x_in, w_in, w_mid, w_out, u_in.reshape(1, 128), u_mid.reshape(1, 128), u_out.reshape(1, 128), target)

        f32 = lambda *shape: jax.ShapeDtypeStruct(shape, F32)
        finals = pl.pallas_call(
            functools.partial(finish_kernel, 0.5 / batch_total),
            out_shape=[jax.ShapeDtypeStruct((rows, width), BF16)] + [f32(128, width)] * 3 + [f32(1, width)] * 3 + [
                f32(1, 128)] * 3 + [f32(1, 3), f32(1, 1)],
            in_specs=[vmem_spec] * 3,
            out_specs=[any_spec] * 12,
            scratch_shapes=[vm((3, 128, width), F32), vm((1, 3), F32), vm((1, 1), F32), dma((4,)), dma((11,))],
            compiler_params=pltpu.CompilerParams(vmem_limit_bytes=8 * 2**20),
            name="finish",
        )(dx_all, tot, pack)
        grad_x, dw0, dw1, dw2, v0, v1, v2, n0, n1, n2, sig, loss = finals
        return (loss.reshape(1), grad_x, dw0, dw1, dw2, n0.reshape(128), n1.reshape(128), n2.reshape(128),
                v0.reshape(width), v1.reshape(width), v2.reshape(width), sig.reshape(3))

    in_specs = (batch_spec, row_spec, row_spec, row_spec, vec_spec, vec_spec, vec_spec, target_spec)
    out_specs = (part_spec, batch_spec, row_spec, row_spec, row_spec, vec_spec, vec_spec, vec_spec, part_spec, part_spec, part_spec, part_spec)
    return jax.shard_map(local_step, mesh=mesh, in_specs=in_specs, out_specs=out_specs, check_vma=False)
```

```python
import functools

import jax
import jax.numpy as jnp
from jax import lax
from jax.experimental import pallas as pl
from jax.experimental.pallas import tpu as pltpu
from jax.sharding import PartitionSpec as P

MESH = pl.DeviceIdType.MESH
F32 = jnp.float32
BF16 = jnp.bfloat16
LANE = 128
PAIR = 2 * LANE
FWD_ROWS = 1024
BIG_ROWS = 512
PLAIN = ((512, 6), (256, 1), (192, 1))
SHARED = ((256, 1), (192, 1), (128, 1))
SHARED_ROWS = sum(size * count for size, count in SHARED)
N_PLAIN = sum(count for _, count in PLAIN)
LAST = PLAIN[-1][0]
N_SHARED = sum(count for _, count in SHARED)


def dot_nt(lhs, rhs):
    return lax.dot_general(lhs, rhs, (((1,), (1,)), ((), ())), preferred_element_type=F32)


def dot_nn(lhs, rhs):
    return lax.dot_general(lhs, rhs, (((1,), (0,)), ((), ())), preferred_element_type=F32)


def dot_tn(lhs, rhs):
    return lax.dot_general(lhs, rhs, (((0,), (0,)), ((), ())), preferred_element_type=F32)


def split_rows(vec):
    width = vec.shape[1]
    high = vec.astype(BF16).astype(F32)
    rest = vec - high
    mid = rest.astype(BF16).astype(F32)
    low = rest - mid
    row = lax.broadcasted_iota(jnp.int32, (16, width), 0)
    stacked = jnp.where(row == 0, high, jnp.where(row == 1, mid, jnp.where(row == 2, low, 0.0)))
    return stacked.astype(BF16)


def main_kernel(inv_batch, x_hbm, w0_hbm, w1_hbm, w2_hbm, u0_hbm, u1_hbm, u2_hbm, t_hbm,
                dx_out, tot_out, pack_out,
                x1, x2, y0, y1, y2, tbuf, wbuf, ubuf, e2, e1, e0, xfor, acc, facc, rbuf, frbuf, fsend,
                g_own, g_other, p_own, p_other, stat, fstat, sstat, rstat, fsstat, frstat, srow, sx, se, eq,
                w_send, w_recv, u_send, u_recv, t_send, t_recv, s_send, s_recv, e_send, e_recv, d_send, d_recv,
                f_send, f_recv, h_send, h_recv, q_send, q_recv, l_w, l_u, l_t, l_x, l_q):
    rep, dat, mod = lax.axis_index("replica"), lax.axis_index("data"), lax.axis_index("model")
    core = lax.rem(mod, 2)
    chip = mod // 2
    sib = mod + 1 - 2 * core
    cnt = lax.rem(mod + 2, 4)
    crs = lax.rem(sib + 2, 4)
    p_sib, p_cnt, p_crs = (rep, dat, sib), (rep, dat, cnt), (rep, dat, crs)
    p_y, p_ys = (rep, 1 - dat, mod), (rep, 1 - dat, sib)
    rows_own = x_hbm.shape[0] // 2
    shared_at = rows_own - SHARED_ROWS
    row_base = core * rows_own

    def each_chunk(groups, first, at, body):
        for size, count in groups:
            def step(i, carry, size=size, first=first, at=at):
                body(first + i, at + i * size, size)
                return carry
            if count == 1:
                step(0, 0)
            else:
                lax.fori_loop(0, count, step, 0)
            first, at = first + count, at + size * count
    w_hbm = [w0_hbm, w1_hbm, w2_hbm]
    u_hbm = [u0_hbm, u1_hbm, u2_hbm]

    def remote(src, dst, ssem, rsem, peer):
        return pltpu.make_async_remote_copy(src_ref=src, dst_ref=dst, send_sem=ssem, recv_sem=rsem,
                                            device_id=peer, device_id_type=MESH)

    def arrived(ref, sem):
        pltpu.make_async_copy(ref, ref, sem).wait()

    def span(start, size):
        return pl.ds(pl.multiple_of(start, size), size)

    def tile(start, size):
        return pl.ds(pl.multiple_of(start, 64), size)

    def w_copy(layer, kind):
        ssem, rsem = w_send, w_recv.at[layer, (0, 1, 2, 0, 0)[kind]]
        if kind == 0:
            return remote(w_hbm[layer], wbuf.at[layer, span(LANE * mod, LANE)], ssem, rsem, p_sib)
        if kind == 1:
            return remote(w_hbm[layer].at[span(64 * dat, 64)], wbuf.at[layer, span(LANE * mod + 64 * dat, 64)], ssem, rsem, p_cnt)
        half = 1 - dat if kind == 4 else dat
        ref = wbuf.at[layer, span(LANE * cnt + 64 * half, 64)]
        return remote(ref, ref, ssem, rsem, p_y if kind == 2 else p_sib)

    def u_copy(kind):
        ref = ubuf.at[:, mod]
        return remote(ref, ref, u_send, u_recv, (p_sib, p_cnt, p_crs)[kind])

    def t_copy(kind, idx, at, size):
        other_core = core if kind == 0 else 1 - core
        return remote(t_hbm.at[tile(other_core * rows_own + at, size)], tbuf.at[mod, tile(at, size)],
                      t_send, t_recv.at[idx], p_cnt if kind == 0 else p_crs)

    def f_copy(kind):
        if kind == 0:
            src, dst, peer = x_hbm.at[tile(row_base + shared_at, SHARED_ROWS)], xfor, p_y
        else:
            other_core = core if kind == 1 else 1 - core
            src = t_hbm.at[tile(other_core * rows_own + shared_at, SHARED_ROWS)]
            dst, peer = tbuf.at[mod, tile(rows_own, SHARED_ROWS)], p_y if kind == 1 else p_ys
        return remote(src, dst, f_send, f_recv, peer)

    def h_copy(kind, idx, at, size):
        ref = tbuf.at[mod if kind == 0 else sib, tile(at, size)]
        return remote(ref, ref, h_send, h_recv.at[idx], p_cnt)

    barrier = pltpu.get_barrier_semaphore()
    peers = (p_sib, p_cnt, p_crs, p_y, p_ys)
    for peer in peers:
        pl.semaphore_signal(barrier, inc=1, device_id=peer, device_id_type=MESH)
    local_w = [pltpu.make_async_copy(w_hbm[k], wbuf.at[k, span(LANE * mod, LANE)], l_w.at[k]) for k in range(3)]
    local_u = [pltpu.make_async_copy(u_hbm[k], ubuf.at[k, mod], l_u.at[k]) for k in range(3)]
    own_rows = span(row_base, rows_own)
    local_x = pltpu.make_async_copy(x_hbm.at[own_rows], dx_out.at[own_rows], l_x)
    local_t = pltpu.make_async_copy(t_hbm.at[own_rows], tbuf.at[mod, pl.ds(0, rows_own)], l_t)
    for k in range(3):
        local_w[k].start()
        local_u[k].start()
    local_x.start()
    local_t.start()
    last_at = shared_at - LAST
    local_q = pltpu.make_async_copy(x_hbm.at[tile((1 - core) * rows_own + last_at, LAST)], sx.at[0], l_q)
    local_q.start()
    pl.semaphore_wait(barrier, len(peers))

    for k in range(3):
        w_copy(k, 1).start()
        w_copy(k, 0).start()

    for copy in local_u:
        copy.wait()
    for kind in range(3):
        u_copy(kind).start()

    def start_targets(idx, at, size):
        t_copy(0, idx, at, size).start()
        t_copy(1, idx, at, size).start()

    each_chunk(PLAIN + SHARED, 0, 0, start_targets)
    t_sib = remote(t_hbm.at[span((1 - core) * rows_own, rows_own)], tbuf.at[mod, pl.ds(0, rows_own)], s_send, s_recv, p_sib)
    t_sib.start()
    acc[...] = jnp.zeros_like(acc)
    facc[...] = jnp.zeros_like(facc)
    stat[...] = jnp.zeros_like(stat)
    fstat[...] = jnp.zeros_like(fstat)

    def relay_x(k):
        w_copy(k, 1).wait_recv()
        w_copy(k, 2).start()
        w_copy(k, 3).start()

    def relay_y(k):
        w_copy(k, 2).wait_recv()
        w_copy(k, 4).start()

    own_cols = span(PAIR * chip, PAIR)
    my_cols = span(LANE * mod, LANE)

    def q_copy(kind):
        if kind == 2:
            src, dst = x1.at[pl.ds(last_at, LAST)], sx.at[1]
        else:
            src, dst = eq.at[kind, :, span(LANE * sib, LANE)], se.at[kind]
        return remote(src, dst, q_send, q_recv.at[kind], p_sib)

    def fold(val):
        return jnp.sum(val.reshape(val.shape[0] // 8, 8, val.shape[1]), axis=0)

    def leaky(val):
        return jnp.maximum(val, 0.2 * val).astype(BF16)

    def add_grad(ref, e_val, x_val):
        part = dot_tn(e_val, x_val)
        ref[0] += part[:LANE]
        ref[1] += part[LANE:]

    def residual(y_val, slab, rows, sums, at):
        res = y_val - tbuf[slab, rows, :].astype(F32)
        grad = res * inv_batch
        if sums is not None:
            sums[0, :, at:at + LANE] += fold(res * res)
            sums[1, :, at:at + LANE] += fold(grad * y_val)
        e2[rows, span(LANE * slab, LANE)] = grad.astype(BF16)

    def last_layer(rows, sums):
        y_val = dot_nt(x2[rows, :], wbuf[2]) * inv_sigma[2]
        first = chip == 0
        own = jnp.where(first, y_val[:, :PAIR], y_val[:, PAIR:])
        y2[rows, :] = jnp.where(first, y_val[:, PAIR:], y_val[:, :PAIR])
        for j in range(2):
            residual(own[:, LANE * j:LANE * j + LANE], 2 * chip + j, rows, sums, PAIR + LANE * j)

    inv_sigma = []
    for k in range(3):
        relay_x(k)
    for kind in range(3):
        f_copy(kind).start()
    relay_y(0)
    relay_y(1)
    for k in range(3):
        local_w[k].wait()
        if k == 0:
            arrived(ubuf.at[:, pl.ds(0, 3)], u_recv)
        arrived(wbuf.at[k, pl.ds(0, PAIR)], w_recv.at[k, 0])
        u_row = jnp.concatenate([ubuf[k, j] for j in range(4)], axis=1)
        p_vec = jnp.sum(dot_nn(split_rows(u_row), wbuf[k]), axis=0, keepdims=True)
        norm = jnp.sqrt(jnp.sum(p_vec * p_vec, axis=1, keepdims=True))
        v_vec = p_vec / jnp.maximum(norm, 1e-12)
        s_vec = jnp.sum(dot_nt(split_rows(v_vec), wbuf[k]), axis=0, keepdims=True)
        sigma = jnp.sqrt(jnp.sum(s_vec * s_vec, axis=1, keepdims=True))
        pack_out[k:k + 1, :] = v_vec
        srow[k] = jnp.broadcast_to(s_vec / sigma, srow.shape[1:])
        pack_out[3 + k:4 + k, 0:LANE] = srow[k, 0:1, span(LANE * mod, LANE)]
        pack_out[6 + k:7 + k, :] = jnp.broadcast_to(sigma, (1, pack_out.shape[1]))
        inv = 1.0 / sigma
        inv_sigma.append(inv)
        if k == 0:
            relay_y(2)
        if k == 0:
            local_x.wait()
        if k == 2:
            local_t.wait()
            t_sib.wait_recv()

        def forward(c, carry, k=k, inv=inv):
            rows = span(c * FWD_ROWS, FWD_ROWS)
            if k == 0:
                y_val = dot_nt(dx_out[span(row_base + c * FWD_ROWS, FWD_ROWS), :], wbuf[0]) * inv
                y0[rows, :] = y_val
                x1[rows, :] = leaky(y_val)
            elif k == 1:
                y_val = dot_nt(x1[rows, :], wbuf[1]) * inv
                y1[rows, :] = y_val
                x2[rows, :] = leaky(y_val)
            else:
                last_layer(rows, stat)
                add_grad(acc.at[2], e2[rows, own_cols], x2[rows, :])
            return carry

        lax.fori_loop(0, rows_own // FWD_ROWS, forward, 0)

    def d_copy(k):
        return remote(acc.at[k, 1 - core], rbuf.at[k], d_send, d_recv.at[k], p_sib)

    def fd_copy(k):
        return remote(fsend.at[k], frbuf.at[k], d_send, d_recv.at[4 + k], p_sib)

    def p_copy(k):
        part = pl.ds((PAIR, 0, LANE)[k], (8, LANE, LANE)[k])
        return remote(p_own.at[part], p_other.at[part], d_send, d_recv.at[8 + k], p_y)

    s_copy = remote(sstat, rstat, d_send, d_recv.at[3], p_sib)
    fs_copy = remote(fsstat, frstat, d_send, d_recv.at[6], p_sib)
    g_copy = remote(g_own, g_other, d_send, d_recv.at[7], p_y)

    def dx_copy(at, size):
        ref = dx_out.at[tile(row_base + at, size)]
        return remote(ref, ref, e_send, e_recv, p_sib)

    def backward(at, size, sums, grads, idx=None, mid=None, split=False):
        rows = tile(at, size)
        b0, b1 = (eq.at[0], eq.at[1]) if split else (e0, e1)
        for j in range(2):
            residual(y2[rows, LANE * j:LANE * j + LANE], 2 - 2 * chip + j, rows, sums, LANE * j)
        back = (dot_nn(e2[rows, :], wbuf[2]) * inv_sigma[2]).astype(BF16).astype(F32)
        y_val = y1[rows, :]
        grad = back * jnp.where(y_val > 0, 1.0, 0.2)
        sums[2] += fold(grad * y_val)
        b1[:size] = grad.astype(BF16)
        if split:
            grads[1, core] += dot_tn(b1[:size, my_cols], x1[rows, :])
        else:
            add_grad(grads.at[1], b1[:size, own_cols], x1[rows, :])
        back = (dot_nn(b1[:size], wbuf[1]) * inv_sigma[1]).astype(BF16).astype(F32)
        if mid is not None:
            mid(1)
        y_val = y0[rows, :]
        grad = back * jnp.where(y_val > 0, 1.0, 0.2)
        sums[3] += fold(grad * y_val)
        b0[:size] = grad.astype(BF16)
        if idx is None:
            add_grad(grads.at[0], b0[:size, own_cols], xfor[tile(at - rows_own, size), :])
            if mid is not None:
                mid(0)
        else:
            x_rows = tile(row_base + at, size)
            if split:
                grads[0, core] += dot_tn(b0[:size, my_cols], dx_out[x_rows, :])
                mid(0)
            else:
                add_grad(grads.at[0], b0[:size, own_cols], dx_out[x_rows, :])
            dx_out[x_rows, :] = (dot_nn(b0[:size], wbuf[0]) * inv_sigma[0]).astype(BF16)

    row = lax.broadcasted_iota(jnp.int32, sstat.shape, 0)

    def gather_sums(ref_sums):
        mine = jnp.zeros(sstat.shape, F32)
        for i in range(4):
            mine = jnp.where(row == i, jnp.sum(ref_sums(i), axis=0, keepdims=True), mine)
        return mine

    def own_chunk(idx, at, size, sums, grads, mid=None, split=False):
        arrived(tbuf.at[pl.ds(0, 2), tile(at, size)], t_recv.at[idx])
        if isinstance(idx, int) and idx == N_PLAIN:
            p_copy(2).start()
        backward(at, size, sums, grads, idx, mid, split)

    n_big = PLAIN[0][1]

    def plain_send(k):
        q_copy(k).start()

    def plain_chunk(idx, at, size):
        if size == BIG_ROWS:
            @pl.when(idx == 0)
            def _():
                d_copy(2).start()
                q_copy(2).start()

            @pl.when(idx == 1)
            def _():
                d_copy(2).wait_recv()
                g_own[...] = acc[2, core] + rbuf[2]

            @pl.when(idx == 2)
            def _():
                g_copy.start()

            @pl.when(idx == n_big - 2)
            def _():
                arrived(x1.at[pl.ds(0, 3 * SHARED_ROWS // 2)], f_recv)

                def forward_on(j, h_at, h_size):
                    h_copy(0, j, h_at, h_size).start()
                    h_copy(1, j, h_at, h_size).start()

                each_chunk(SHARED, 0, rows_own, forward_on)

            @pl.when(idx == n_big - 1)
            def _():
                rows = pl.ds(rows_own, SHARED_ROWS)
                y_val = dot_nt(xfor[...], wbuf[0]) * inv_sigma[0]
                y0[rows, :] = y_val
                x1[rows, :] = leaky(y_val)
                y_val = dot_nt(x1[rows, :], wbuf[1]) * inv_sigma[1]
                y1[rows, :] = y_val
                x2[rows, :] = leaky(y_val)
                last_layer(rows, None)

        last = idx == N_PLAIN - 1 if isinstance(idx, int) else False
        own_chunk(idx, at, size, stat, acc, plain_send if last else None, last)
        if isinstance(idx, int) and idx == N_PLAIN - 2:
            d_copy(1).start()
            d_copy(0).start()
        dx_copy(at, size).start()

    each_chunk(PLAIN, 0, 0, plain_chunk)

    d_copy(1).wait_recv()
    q_copy(2).wait_recv()
    q_copy(1).wait_recv()
    p_own[0:LANE, :] = (acc[1, core] + rbuf[1]) + dot_tn(se[1], sx[1])
    sstat[...] = gather_sums(lambda i: stat[i])
    s_copy.start()
    p_copy(1).start()
    d_copy(0).wait_recv()
    local_q.wait()
    q_copy(0).wait_recv()
    p_own[LANE:PAIR, :] = (acc[0, core] + rbuf[0]) + dot_tn(se[0], sx[0])

    def shared_chunk(idx, at, size):
        if idx == N_PLAIN + 1:
            p_copy(0).start()
        own_chunk(idx, at, size, fstat.at[0], facc.at[0])
        dx_copy(at, size).start()
        if idx == N_PLAIN:
            s_copy.wait_recv()
            p_own[PAIR:264, :] = sstat[...] + rstat[...]

    each_chunk(SHARED, N_PLAIN, shared_at, shared_chunk)

    def last_send(k):
        fsend[k] = facc[0, k, 1 - core] + facc[1, k, 1 - core]
        if k == 1:
            fd_copy(1).start()
        if k == 0:
            fsstat[...] = gather_sums(lambda i: fstat[0, i] + fstat[1, i])
            fd_copy(0).start()
            fs_copy.start()

    def foreign_chunk(idx, at, size):
        arrived(tbuf.at[pl.ds(0, 2), tile(at, size)], h_recv.at[idx])
        last = isinstance(at, int) and at + size == rows_own + SHARED_ROWS
        backward(at, size, fstat.at[1], facc.at[1], None, last_send if last else None)

    each_chunk(SHARED, 0, rows_own, foreign_chunk)

    g_copy.wait_recv()
    tot_out[PAIR:384, :] = g_own[...] + g_other[...]
    for k in range(3):
        p_copy(k).wait_recv()
    for i, k in enumerate((1, 0)):
        part = slice(LANE * i, LANE * i + LANE)
        fd_copy(k).wait_recv()
        tot_out[part, :] = (p_own[part, :] + p_other[part, :]) + ((facc[0, k, core] + facc[1, k, core]) + frbuf[k])
    fs_copy.wait_recv()
    tot_out[384:392, :] = (p_own[PAIR:264, :] + p_other[PAIR:264, :]) + (fsstat[...] + frstat[...])

    arrived(x1.at[pl.ds(0, 3 * 384)], w_send)
    arrived(ubuf.at[:, pl.ds(0, 3)], u_send)
    arrived(t_hbm, t_send)
    arrived(tbuf.at[mod, pl.ds(0, rows_own)], s_send)
    arrived(x1.at[pl.ds(0, 3 * SHARED_ROWS // 2)], f_send)
    arrived(tbuf.at[pl.ds(0, 2), pl.ds(rows_own, SHARED_ROWS)], h_send)
    arrived(y0.at[pl.ds(0, 8 * LANE + 24)], d_send)
    arrived(x1.at[pl.ds(0, 3 * LAST // 2)], q_send)
    arrived(dx_out.at[own_rows], e_send)
    arrived(dx_out.at[own_rows], e_recv)


def finish_kernel(loss_scale, dx_in, tot, pack, dx_ref, dw0, dw1, dw2, v0, v1, v2, n0, n1, n2, sig_out, loss_out,
                  grads, sig_row, loss_row, sems, out_sems):
    parts = sems.shape[0]
    rows = dx_in.shape[0] // parts
    copies = [pltpu.make_async_copy(dx_in.at[pl.ds(i * rows, rows)], dx_ref.at[pl.ds(i * rows, rows)], sems.at[i]) for i in range(parts)]
    for copy in copies:
        copy.start()

    def out_copy(src, dst):
        copy = pltpu.make_async_copy(src, dst, out_sems.at[len(copies) - parts])
        copy.start()
        copies.append(copy)

    for k, (v_out, n_out) in enumerate(((v0, n0), (v1, n1), (v2, n2))):
        out_copy(pack.at[k:k + 1, :], v_out)
        out_copy(pack.at[3 + k:4 + k, 0:LANE], n_out)
    lane = lax.broadcasted_iota(jnp.int32, (1, LANE), 1)
    row = jnp.where(lane == 0, pack[6:7, 0:LANE], jnp.where(lane == 1, pack[7:8, 0:LANE], pack[8:9, 0:LANE]))
    sig_row[...] = row[:, :3]
    stats = jnp.sum(tot[384:392, :], axis=1, keepdims=True)
    loss_row[...] = loss_scale * stats[0:1]
    for k, at in enumerate((LANE, 0, PAIR)):
        inv = 1.0 / pack[6 + k:7 + k, 0:1]
        u_col = jnp.transpose(jnp.broadcast_to(pack[3 + k:4 + k, 0:LANE], (LANE, LANE)))[:, 0:1]
        grads[k] = tot[at:at + LANE, :] * inv - (stats[3 - k:4 - k] * inv) * (u_col * pack[k:k + 1, :])
    out_copy(sig_row, sig_out)
    out_copy(loss_row, loss_out)
    for k, out in enumerate((dw0, dw1, dw2)):
        out_copy(grads.at[k], out)
    for copy in copies:
        copy.wait()


def solution(mesh):
    data_size = mesh.shape["data"]
    row_spec = P(("replica", "model"), None)
    vec_spec = P(("replica", "model"))
    batch_spec = P(("replica", "data"), None)
    target_spec = P(("replica", "data"), "model")
    part_spec = P("replica")

    def local_step(x_in, w_in, w_mid, w_out, u_in, u_mid, u_out, target):
        rows, width = x_in.shape
        half = rows // 2
        ext = half + SHARED_ROWS
        batch_total = rows * data_size
        any_spec = pl.BlockSpec(memory_space=pl.ANY)
        vmem_spec = pl.BlockSpec(memory_space=pltpu.VMEM)
        dma = pltpu.SemaphoreType.DMA
        vm = pltpu.VMEM
        dx_all, tot, pack = pl.pallas_call(
            functools.partial(main_kernel, 1.0 / batch_total),
            out_shape=[vm((rows, width), BF16), vm((392, width), F32), vm((16, width), F32)],
            in_specs=[any_spec] * 8,
            out_specs=[vmem_spec] * 3,
            scratch_shapes=[
                vm((ext, width), BF16), vm((ext, width), BF16),
                vm((ext, width), F32), vm((ext, width), F32), vm((ext, PAIR), F32),
                vm((4, ext, LANE), BF16),
                vm((3, width, width), BF16),
                vm((3, 4, 1, LANE), F32),
                vm((ext, width), BF16), vm((BIG_ROWS, width), BF16), vm((BIG_ROWS, width), BF16),
                vm((SHARED_ROWS, width), BF16),
                vm((3, 2, LANE, width), F32), vm((2, 2, 2, LANE, width), F32),
                vm((3, LANE, width), F32), vm((2, LANE, width), F32), vm((2, LANE, width), F32),
                vm((LANE, width), F32), vm((LANE, width), F32),
                vm((264, width), F32), vm((264, width), F32),
                vm((4, 8, width), F32), vm((2, 4, 8, width), F32),
                vm((8, width), F32), vm((8, width), F32), vm((8, width), F32), vm((8, width), F32),
                vm((3, 8, width), F32),
                vm((2, LAST, width), BF16), vm((2, LAST, LANE), BF16), vm((2, LAST, width), BF16),
                dma(()), dma((3, 3)), dma(()), dma(()),
                dma(()), dma((N_PLAIN + N_SHARED,)), dma(()), dma(()), dma(()), dma(()), dma(()), dma((11,)),
                dma(()), dma(()), dma(()), dma((N_SHARED,)), dma(()), dma((3,)),
                dma((3,)), dma((3,)), dma(()), dma(()), dma(()),
            ],
            compiler_params=pltpu.CompilerParams(
                collective_id=0, has_side_effects=True, vmem_limit_bytes=55 * 2**20),
            name="fused_step",
        )(x_in, w_in, w_mid, w_out, u_in.reshape(1, LANE), u_mid.reshape(1, LANE), u_out.reshape(1, LANE), target)

        f32 = lambda *shape: jax.ShapeDtypeStruct(shape, F32)
        finals = pl.pallas_call(
            functools.partial(finish_kernel, 0.5 / batch_total),
            out_shape=[jax.ShapeDtypeStruct((rows, width), BF16)] + [f32(LANE, width)] * 3 + [f32(1, width)] * 3 + [
                f32(1, LANE)] * 3 + [f32(1, 3), f32(1, 1)],
            in_specs=[vmem_spec] * 3,
            out_specs=[any_spec] * 12,
            scratch_shapes=[vm((3, LANE, width), F32), vm((1, 3), F32), vm((1, 1), F32), dma((4,)), dma((11,))],
            compiler_params=pltpu.CompilerParams(vmem_limit_bytes=8 * 2**20),
            name="finish",
        )(dx_all, tot, pack)
        grad_x, dw0, dw1, dw2, v0, v1, v2, n0, n1, n2, sig, loss = finals
        return (loss.reshape(1), grad_x, dw0, dw1, dw2, n0.reshape(LANE), n1.reshape(LANE), n2.reshape(LANE),
                v0.reshape(width), v1.reshape(width), v2.reshape(width), sig.reshape(3))

    in_specs = (batch_spec, row_spec, row_spec, row_spec, vec_spec, vec_spec, vec_spec, target_spec)
    out_specs = (part_spec, batch_spec, row_spec, row_spec, row_spec, vec_spec, vec_spec, vec_spec, part_spec, part_spec, part_spec, part_spec)
    return jax.shard_map(local_step, mesh=mesh, in_specs=in_specs, out_specs=out_specs, check_vma=False)
```

```python
import functools

import jax
import jax.numpy as jnp
from jax import lax
from jax.experimental import pallas as pl
from jax.experimental.pallas import tpu as pltpu
from jax.sharding import PartitionSpec as P

MESH = pl.DeviceIdType.MESH
F32 = jnp.float32
BF16 = jnp.bfloat16
LANE = 128
PAIR = 2 * LANE
FWD_ROWS = 1024
BIG_ROWS = 512
PLAIN = ((512, 6), (256, 1), (192, 1))
SHARED = ((256, 1), (192, 1), (128, 1))
SHARED_ROWS = sum(size * count for size, count in SHARED)
N_PLAIN = sum(count for _, count in PLAIN)
LAST = PLAIN[-1][0]
N_SHARED = sum(count for _, count in SHARED)


def dot_nt(lhs, rhs):
    return lax.dot_general(lhs, rhs, (((1,), (1,)), ((), ())), preferred_element_type=F32)


def dot_nn(lhs, rhs):
    return lax.dot_general(lhs, rhs, (((1,), (0,)), ((), ())), preferred_element_type=F32)


def dot_tn(lhs, rhs):
    return lax.dot_general(lhs, rhs, (((0,), (0,)), ((), ())), preferred_element_type=F32)


def split_rows(vec):
    width = vec.shape[1]
    limit = float(jnp.finfo(BF16).max)
    high = jnp.clip(vec, -limit, limit).astype(BF16).astype(F32)
    rest = vec - high
    mid = rest.astype(BF16).astype(F32)
    low = rest - mid
    row = lax.broadcasted_iota(jnp.int32, (16, width), 0)
    stacked = jnp.where(row == 0, high, jnp.where(row == 1, mid, jnp.where(row == 2, low, 0.0)))
    return stacked.astype(BF16)


def main_kernel(inv_batch, x_hbm, w0_hbm, w1_hbm, w2_hbm, u0_hbm, u1_hbm, u2_hbm, t_hbm,
                dx_out, tot_out, pack_out,
                x1, x2, y0, y1, y2, tbuf, wbuf, ubuf, e2, e1, e0, xfor, acc, facc, rbuf, frbuf, fsend,
                g_own, g_other, p_own, p_other, stat, fstat, sstat, rstat, fsstat, frstat, srow, sx, se, eq, xstat, xb,
                w_send, w_recv, u_send, u_recv, t_send, t_recv, s_send, s_recv, e_send, e_recv, d_send, d_recv,
                f_send, f_recv, h_send, h_recv, q_send, q_recv, x_send, x_recv, l_w, l_u, l_t, l_x, l_q):
    rep, dat, mod = lax.axis_index("replica"), lax.axis_index("data"), lax.axis_index("model")
    core = lax.rem(mod, 2)
    chip = mod // 2
    sib = mod + 1 - 2 * core
    cnt = lax.rem(mod + 2, 4)
    crs = lax.rem(sib + 2, 4)
    p_sib, p_cnt, p_crs = (rep, dat, sib), (rep, dat, cnt), (rep, dat, crs)
    p_y, p_ys = (rep, 1 - dat, mod), (rep, 1 - dat, sib)
    rows_own = x_hbm.shape[0] // 2
    shared_at = rows_own - SHARED_ROWS
    row_base = core * rows_own

    def each_chunk(groups, first, at, body):
        for size, count in groups:
            def step(i, carry, size=size, first=first, at=at):
                body(first + i, at + i * size, size)
                return carry
            if count == 1:
                step(0, 0)
            else:
                lax.fori_loop(0, count, step, 0)
            first, at = first + count, at + size * count
    w_hbm = [w0_hbm, w1_hbm, w2_hbm]
    u_hbm = [u0_hbm, u1_hbm, u2_hbm]

    def remote(src, dst, ssem, rsem, peer):
        return pltpu.make_async_remote_copy(src_ref=src, dst_ref=dst, send_sem=ssem, recv_sem=rsem,
                                            device_id=peer, device_id_type=MESH)

    def arrived(ref, sem):
        pltpu.make_async_copy(ref, ref, sem).wait()

    def span(start, size):
        return pl.ds(pl.multiple_of(start, size), size)

    def tile(start, size):
        return pl.ds(pl.multiple_of(start, 64), size)

    def w_copy(layer, kind):
        ssem, rsem = w_send, w_recv.at[layer, (0, 1, 2, 0, 0)[kind]]
        if kind == 0:
            return remote(w_hbm[layer], wbuf.at[layer, span(LANE * mod, LANE)], ssem, rsem, p_sib)
        if kind == 1:
            return remote(w_hbm[layer].at[span(64 * dat, 64)], wbuf.at[layer, span(LANE * mod + 64 * dat, 64)], ssem, rsem, p_cnt)
        half = 1 - dat if kind == 4 else dat
        ref = wbuf.at[layer, span(LANE * cnt + 64 * half, 64)]
        return remote(ref, ref, ssem, rsem, p_y if kind == 2 else p_sib)

    def u_copy(kind):
        ref = ubuf.at[:, mod]
        return remote(ref, ref, u_send, u_recv, (p_sib, p_cnt, p_crs)[kind])

    def t_copy(kind, idx, at, size):
        other_core = core if kind == 0 else 1 - core
        return remote(t_hbm.at[tile(other_core * rows_own + at, size)], tbuf.at[mod, tile(at, size)],
                      t_send, t_recv.at[idx], p_cnt if kind == 0 else p_crs)

    def f_copy(kind):
        if kind == 0:
            src, dst, peer = x_hbm.at[tile(row_base + shared_at, SHARED_ROWS)], xfor, p_y
        else:
            other_core = core if kind == 1 else 1 - core
            src = t_hbm.at[tile(other_core * rows_own + shared_at, SHARED_ROWS)]
            dst, peer = tbuf.at[mod, tile(rows_own, SHARED_ROWS)], p_y if kind == 1 else p_ys
        return remote(src, dst, f_send, f_recv, peer)

    def h_copy(kind, idx, at, size):
        ref = tbuf.at[mod if kind == 0 else sib, tile(at, size)]
        return remote(ref, ref, h_send, h_recv.at[idx], p_cnt)

    barrier = pltpu.get_barrier_semaphore()
    peers = (p_sib, p_cnt, p_crs, p_y, p_ys)
    for peer in peers:
        pl.semaphore_signal(barrier, inc=1, device_id=peer, device_id_type=MESH)
    local_w = [pltpu.make_async_copy(w_hbm[k], wbuf.at[k, span(LANE * mod, LANE)], l_w.at[k]) for k in range(3)]
    local_u = [pltpu.make_async_copy(u_hbm[k], ubuf.at[k, mod], l_u.at[k]) for k in range(3)]
    own_rows = span(row_base, rows_own)
    local_x = pltpu.make_async_copy(x_hbm.at[own_rows], dx_out.at[own_rows], l_x)
    local_t = pltpu.make_async_copy(t_hbm.at[own_rows], tbuf.at[mod, pl.ds(0, rows_own)], l_t)
    for k in range(3):
        local_w[k].start()
        local_u[k].start()
    local_x.start()
    local_t.start()
    last_at = shared_at - LAST
    local_q = pltpu.make_async_copy(x_hbm.at[tile((1 - core) * rows_own + last_at, LAST)], sx.at[0], l_q)
    local_q.start()
    pl.semaphore_wait(barrier, len(peers))

    for k in range(3):
        w_copy(k, 1).start()
        w_copy(k, 0).start()

    for copy in local_u:
        copy.wait()
    for kind in range(3):
        u_copy(kind).start()

    def start_targets(idx, at, size):
        t_copy(0, idx, at, size).start()
        t_copy(1, idx, at, size).start()

    each_chunk(PLAIN + SHARED, 0, 0, start_targets)
    t_sib = remote(t_hbm.at[span((1 - core) * rows_own, rows_own)], tbuf.at[mod, pl.ds(0, rows_own)], s_send, s_recv, p_sib)
    t_sib.start()
    acc[...] = jnp.zeros_like(acc)
    facc[...] = jnp.zeros_like(facc)
    stat[...] = jnp.zeros_like(stat)
    xstat[...] = jnp.zeros_like(xstat)
    fstat[...] = jnp.zeros_like(fstat)

    def relay_x(k):
        w_copy(k, 1).wait_recv()
        w_copy(k, 2).start()
        w_copy(k, 3).start()

    def relay_y(k):
        w_copy(k, 2).wait_recv()
        w_copy(k, 4).start()

    own_cols = span(PAIR * chip, PAIR)
    my_cols = span(LANE * mod, LANE)

    def q_copy(kind):
        if kind == 2:
            src, dst = x1.at[pl.ds(last_at, LAST)], sx.at[1]
        else:
            src, dst = eq.at[kind, :, span(LANE * sib, LANE)], se.at[kind]
        return remote(src, dst, q_send, q_recv.at[kind], p_sib)

    def fold(val):
        return jnp.sum(val.reshape(val.shape[0] // 8, 8, val.shape[1]), axis=0)

    def leaky(val):
        return jnp.maximum(val, 0.2 * val).astype(BF16)

    def add_grad(ref, e_val, x_val):
        part = dot_tn(e_val, x_val)
        ref[0] += part[:LANE]
        ref[1] += part[LANE:]

    def residual(y_val, slab, rows, sums=None):
        res = y_val - tbuf[slab, rows, :].astype(F32)
        grad = res * inv_batch
        if sums is not None:
            sums[0] += fold(res * res)
            sums[1] += fold(grad * y_val)
        e2[rows, span(LANE * slab, LANE)] = grad.astype(BF16)

    def last_layer(rows, sums):
        y_val = dot_nt(x2[rows, :], wbuf[2]) * inv_sigma[2]
        first = chip == 0
        own = jnp.where(first, y_val[:, :PAIR], y_val[:, PAIR:])
        y2[rows, :] = jnp.where(first, y_val[:, PAIR:], y_val[:, :PAIR])
        for j in range(2):
            residual(own[:, LANE * j:LANE * j + LANE], 2 * chip + j, rows, sums)

    inv_sigma = []
    for k in range(3):
        relay_x(k)
    for kind in range(3):
        f_copy(kind).start()
    relay_y(0)
    relay_y(1)
    for k in range(3):
        local_w[k].wait()
        if k == 0:
            arrived(ubuf.at[:, pl.ds(0, 3)], u_recv)
        arrived(wbuf.at[k, pl.ds(0, PAIR)], w_recv.at[k, 0])
        u_row = jnp.concatenate([ubuf[k, j] for j in range(4)], axis=1)
        p_vec = jnp.sum(dot_nn(split_rows(u_row), wbuf[k]), axis=0, keepdims=True)
        norm = jnp.sqrt(jnp.sum(p_vec * p_vec, axis=1, keepdims=True))
        v_vec = p_vec / jnp.maximum(norm, 1e-12)
        s_vec = jnp.sum(dot_nt(split_rows(v_vec), wbuf[k]), axis=0, keepdims=True)
        sigma = jnp.sqrt(jnp.sum(s_vec * s_vec, axis=1, keepdims=True))
        pack_out[k:k + 1, :] = v_vec
        srow[k] = jnp.broadcast_to(s_vec / sigma, srow.shape[1:])
        pack_out[3 + k:4 + k, 0:LANE] = srow[k, 0:1, span(LANE * mod, LANE)]
        pack_out[6 + k:7 + k, :] = jnp.broadcast_to(sigma, (1, pack_out.shape[1]))
        inv = 1.0 / sigma
        inv_sigma.append(inv)
        if k == 0:
            relay_y(2)
        if k == 0:
            local_x.wait()
        if k == 2:
            local_t.wait()
            t_sib.wait_recv()

        def forward(c, carry, k=k, inv=inv):
            rows = span(c * FWD_ROWS, FWD_ROWS)
            if k == 0:
                y_val = dot_nt(dx_out[span(row_base + c * FWD_ROWS, FWD_ROWS), :], wbuf[0]) * inv
                y0[rows, :] = y_val
                x1[rows, :] = leaky(y_val)
            elif k == 1:
                y_val = dot_nt(x1[rows, :], wbuf[1]) * inv
                y1[rows, :] = y_val
                x2[rows, :] = leaky(y_val)
            else:
                last_layer(rows, xstat)
                add_grad(acc.at[2], e2[rows, own_cols], x2[rows, :])
            return carry

        lax.fori_loop(0, rows_own // FWD_ROWS, forward, 0)

    def d_copy(k):
        return remote(acc.at[k, 1 - core], rbuf.at[k], d_send, d_recv.at[k], p_sib)

    def fd_copy(k):
        return remote(fsend.at[k], frbuf.at[k], d_send, d_recv.at[4 + k], p_sib)

    def p_copy(k):
        part = pl.ds((PAIR, 0, LANE)[k], (8, LANE, LANE)[k])
        return remote(p_own.at[part], p_other.at[part], d_send, d_recv.at[8 + k], p_y)

    s_copy = remote(sstat, rstat, d_send, d_recv.at[3], p_sib)
    fs_copy = remote(fsstat, frstat, d_send, d_recv.at[6], p_sib)
    g_copy = remote(g_own, g_other, d_send, d_recv.at[7], p_y)

    def dx_copy(at, size):
        ref = dx_out.at[tile(row_base + at, size)]
        return remote(ref, ref, e_send, e_recv, p_sib)

    def backward(at, size, sums, grads, idx=None, mid=None, split=False):
        rows = tile(at, size)
        b0, b1 = (eq.at[0], eq.at[1]) if split else (e0, e1)
        for j in range(2):
            residual(y2[rows, LANE * j:LANE * j + LANE], 2 - 2 * chip + j, rows)
        back = (dot_nn(e2[rows, :], wbuf[2]) * inv_sigma[2]).astype(BF16).astype(F32)
        y_val = y1[rows, :]
        grad = back * jnp.where(y_val > 0, 1.0, 0.2)
        sums[0] += fold(grad * y_val)
        b1[:size] = grad.astype(BF16)
        if split:
            grads[1, core] += dot_tn(b1[:size, my_cols], x1[rows, :])
        else:
            add_grad(grads.at[1], b1[:size, own_cols], x1[rows, :])
        back = (dot_nn(b1[:size], wbuf[1]) * inv_sigma[1]).astype(BF16).astype(F32)
        if mid is not None:
            mid(1)
        y_val = y0[rows, :]
        grad = back * jnp.where(y_val > 0, 1.0, 0.2)
        sums[1] += fold(grad * y_val)
        b0[:size] = grad.astype(BF16)
        if idx is None:
            add_grad(grads.at[0], b0[:size, own_cols], xfor[tile(at - rows_own, size), :])
            if mid is not None:
                mid(0)
        else:
            x_rows = tile(row_base + at, size)
            if split:
                grads[0, core] += dot_tn(b0[:size, my_cols], dx_out[x_rows, :])
                mid(0)
            else:
                add_grad(grads.at[0], b0[:size, own_cols], dx_out[x_rows, :])
            dx_out[x_rows, :] = (dot_nn(b0[:size], wbuf[0]) * inv_sigma[0]).astype(BF16)

    row = lax.broadcasted_iota(jnp.int32, sstat.shape, 0)

    def gather_sums(ref_sums):
        mine = jnp.zeros(sstat.shape, F32)
        for i in range(2):
            mine = jnp.where(row == 2 + i, jnp.sum(ref_sums(i), axis=0, keepdims=True), mine)
        return mine

    first_sums = [jnp.sum(xstat[i], axis=0, keepdims=True) for i in range(2)]
    xb[0] = jnp.where(row[:, :LANE] == 0, first_sums[0], jnp.where(row[:, :LANE] == 1, first_sums[1], 0.0))

    def x_copy(k):
        return remote(xb.at[2 * k], xb.at[2 * k + 1], x_send, x_recv.at[k], (p_sib, p_y, p_cnt)[k])

    def own_chunk(idx, at, size, sums, grads, mid=None, split=False):
        arrived(tbuf.at[pl.ds(0, 2), tile(at, size)], t_recv.at[idx])
        if isinstance(idx, int) and idx == N_PLAIN:
            p_copy(2).start()
        backward(at, size, sums, grads, idx, mid, split)

    n_big = PLAIN[0][1]

    def plain_send(k):
        q_copy(k).start()

    def plain_chunk(idx, at, size):
        if size == BIG_ROWS:
            @pl.when(idx == 0)
            def _():
                d_copy(2).start()
                q_copy(2).start()
                x_copy(0).start()

            @pl.when(idx == 1)
            def _():
                d_copy(2).wait_recv()
                g_own[...] = acc[2, core] + rbuf[2]
                x_copy(0).wait_recv()
                xb[2] = xb[0] + xb[1]

            @pl.when(idx == 2)
            def _():
                g_copy.start()
                x_copy(1).start()

            @pl.when(idx == n_big - 3)
            def _():
                x_copy(1).wait_recv()
                xb[4] = xb[2] + xb[3]

            @pl.when(idx == n_big - 2)
            def _():
                x_copy(2).start()
                arrived(x1.at[pl.ds(0, 3 * SHARED_ROWS // 2)], f_recv)

                def forward_on(j, h_at, h_size):
                    h_copy(0, j, h_at, h_size).start()
                    h_copy(1, j, h_at, h_size).start()

                each_chunk(SHARED, 0, rows_own, forward_on)

            @pl.when(idx == n_big - 1)
            def _():
                rows = pl.ds(rows_own, SHARED_ROWS)
                y_val = dot_nt(xfor[...], wbuf[0]) * inv_sigma[0]
                y0[rows, :] = y_val
                x1[rows, :] = leaky(y_val)
                y_val = dot_nt(x1[rows, :], wbuf[1]) * inv_sigma[1]
                y1[rows, :] = y_val
                x2[rows, :] = leaky(y_val)
                last_layer(rows, None)

        last = idx == N_PLAIN - 1 if isinstance(idx, int) else False
        own_chunk(idx, at, size, stat, acc, plain_send if last else None, last)
        if isinstance(idx, int) and idx == N_PLAIN - 2:
            d_copy(1).start()
            d_copy(0).start()
        dx_copy(at, size).start()

    each_chunk(PLAIN, 0, 0, plain_chunk)

    d_copy(1).wait_recv()
    q_copy(2).wait_recv()
    q_copy(1).wait_recv()
    p_own[0:LANE, :] = (acc[1, core] + rbuf[1]) + dot_tn(se[1], sx[1])
    sstat[...] = gather_sums(lambda i: stat[i])
    s_copy.start()
    p_copy(1).start()
    d_copy(0).wait_recv()
    local_q.wait()
    q_copy(0).wait_recv()
    p_own[LANE:PAIR, :] = (acc[0, core] + rbuf[0]) + dot_tn(se[0], sx[0])

    def shared_chunk(idx, at, size):
        if idx == N_PLAIN + 1:
            p_copy(0).start()
        own_chunk(idx, at, size, fstat.at[0], facc.at[0])
        dx_copy(at, size).start()
        if idx == N_PLAIN:
            s_copy.wait_recv()
            p_own[PAIR:264, :] = sstat[...] + rstat[...]

    each_chunk(SHARED, N_PLAIN, shared_at, shared_chunk)

    def last_send(k):
        fsend[k] = facc[0, k, 1 - core] + facc[1, k, 1 - core]
        if k == 1:
            fd_copy(1).start()
        if k == 0:
            fsstat[...] = gather_sums(lambda i: fstat[0, i] + fstat[1, i])
            fd_copy(0).start()
            fs_copy.start()

    def foreign_chunk(idx, at, size):
        arrived(tbuf.at[pl.ds(0, 2), tile(at, size)], h_recv.at[idx])
        last = isinstance(at, int) and at + size == rows_own + SHARED_ROWS
        backward(at, size, fstat.at[1], facc.at[1], None, last_send if last else None)

    each_chunk(SHARED, 0, rows_own, foreign_chunk)

    g_copy.wait_recv()
    tot_out[PAIR:384, :] = g_own[...] + g_other[...]
    for k in range(3):
        p_copy(k).wait_recv()
    for i, k in enumerate((1, 0)):
        part = slice(LANE * i, LANE * i + LANE)
        fd_copy(k).wait_recv()
        tot_out[part, :] = (p_own[part, :] + p_other[part, :]) + ((facc[0, k, core] + facc[1, k, core]) + frbuf[k])
    fs_copy.wait_recv()
    tot_out[384:392, :] = (p_own[PAIR:264, :] + p_other[PAIR:264, :]) + (fsstat[...] + frstat[...])
    x_copy(2).wait_recv()
    tot_out[384:392, :LANE] += xb[4] + xb[5]

    arrived(x1.at[pl.ds(0, 3 * 384)], w_send)
    arrived(ubuf.at[:, pl.ds(0, 3)], u_send)
    arrived(t_hbm, t_send)
    arrived(tbuf.at[mod, pl.ds(0, rows_own)], s_send)
    arrived(x1.at[pl.ds(0, 3 * SHARED_ROWS // 2)], f_send)
    arrived(tbuf.at[pl.ds(0, 2), pl.ds(rows_own, SHARED_ROWS)], h_send)
    arrived(y0.at[pl.ds(0, 8 * LANE + 24)], d_send)
    arrived(xb.at[pl.ds(0, 3)], x_send)
    arrived(x1.at[pl.ds(0, 3 * LAST // 2)], q_send)
    arrived(dx_out.at[own_rows], e_send)
    arrived(dx_out.at[own_rows], e_recv)


def finish_kernel(loss_scale, dx_in, tot, pack, dx_ref, dw0, dw1, dw2, v0, v1, v2, n0, n1, n2, sig_out, loss_out,
                  grads, sig_row, loss_row, sems, out_sems):
    parts = sems.shape[0]
    rows = dx_in.shape[0] // parts
    copies = [pltpu.make_async_copy(dx_in.at[pl.ds(i * rows, rows)], dx_ref.at[pl.ds(i * rows, rows)], sems.at[i]) for i in range(parts)]
    for copy in copies:
        copy.start()

    def out_copy(src, dst):
        copy = pltpu.make_async_copy(src, dst, out_sems.at[len(copies) - parts])
        copy.start()
        copies.append(copy)

    for k, (v_out, n_out) in enumerate(((v0, n0), (v1, n1), (v2, n2))):
        out_copy(pack.at[k:k + 1, :], v_out)
        out_copy(pack.at[3 + k:4 + k, 0:LANE], n_out)
    lane = lax.broadcasted_iota(jnp.int32, (1, LANE), 1)
    row = jnp.where(lane == 0, pack[6:7, 0:LANE], jnp.where(lane == 1, pack[7:8, 0:LANE], pack[8:9, 0:LANE]))
    sig_row[...] = row[:, :3]
    stats = jnp.sum(tot[384:392, :], axis=1, keepdims=True)
    loss_row[...] = loss_scale * stats[0:1]
    for k, at in enumerate((LANE, 0, PAIR)):
        inv = 1.0 / pack[6 + k:7 + k, 0:1]
        u_col = jnp.transpose(jnp.broadcast_to(pack[3 + k:4 + k, 0:LANE], (LANE, LANE)))[:, 0:1]
        grads[k] = tot[at:at + LANE, :] * inv - (stats[3 - k:4 - k] * inv) * (u_col * pack[k:k + 1, :])
    out_copy(sig_row, sig_out)
    out_copy(loss_row, loss_out)
    for k, out in enumerate((dw0, dw1, dw2)):
        out_copy(grads.at[k], out)
    for copy in copies:
        copy.wait()


def solution(mesh):
    data_size = mesh.shape["data"]
    row_spec = P(("replica", "model"), None)
    vec_spec = P(("replica", "model"))
    batch_spec = P(("replica", "data"), None)
    target_spec = P(("replica", "data"), "model")
    part_spec = P("replica")

    def local_step(x_in, w_in, w_mid, w_out, u_in, u_mid, u_out, target):
        rows, width = x_in.shape
        half = rows // 2
        ext = half + SHARED_ROWS
        batch_total = rows * data_size
        any_spec = pl.BlockSpec(memory_space=pl.ANY)
        vmem_spec = pl.BlockSpec(memory_space=pltpu.VMEM)
        dma = pltpu.SemaphoreType.DMA
        vm = pltpu.VMEM
        dx_all, tot, pack = pl.pallas_call(
            functools.partial(main_kernel, 1.0 / batch_total),
            out_shape=[vm((rows, width), BF16), vm((392, width), F32), vm((16, width), F32)],
            in_specs=[any_spec] * 8,
            out_specs=[vmem_spec] * 3,
            scratch_shapes=[
                vm((ext, width), BF16), vm((ext, width), BF16),
                vm((ext, width), F32), vm((ext, width), F32), vm((ext, PAIR), F32),
                vm((4, ext, LANE), BF16),
                vm((3, width, width), BF16),
                vm((3, 4, 1, LANE), F32),
                vm((ext, width), BF16), vm((BIG_ROWS, width), BF16), vm((BIG_ROWS, width), BF16),
                vm((SHARED_ROWS, width), BF16),
                vm((3, 2, LANE, width), F32), vm((2, 2, 2, LANE, width), F32),
                vm((3, LANE, width), F32), vm((2, LANE, width), F32), vm((2, LANE, width), F32),
                vm((LANE, width), F32), vm((LANE, width), F32),
                vm((264, width), F32), vm((264, width), F32),
                vm((2, 8, width), F32), vm((2, 2, 8, width), F32),
                vm((8, width), F32), vm((8, width), F32), vm((8, width), F32), vm((8, width), F32),
                vm((3, 8, width), F32),
                vm((2, LAST, width), BF16), vm((2, LAST, LANE), BF16), vm((2, LAST, width), BF16),
                vm((2, 8, LANE), F32), vm((6, 8, LANE), F32),
                dma(()), dma((3, 3)), dma(()), dma(()),
                dma(()), dma((N_PLAIN + N_SHARED,)), dma(()), dma(()), dma(()), dma(()), dma(()), dma((11,)),
                dma(()), dma(()), dma(()), dma((N_SHARED,)), dma(()), dma((3,)), dma(()), dma((3,)),
                dma((3,)), dma((3,)), dma(()), dma(()), dma(()),
            ],
            compiler_params=pltpu.CompilerParams(
                collective_id=0, has_side_effects=True, vmem_limit_bytes=55 * 2**20),
            name="fused_step",
        )(x_in, w_in, w_mid, w_out, u_in.reshape(1, LANE), u_mid.reshape(1, LANE), u_out.reshape(1, LANE), target)

        f32 = lambda *shape: jax.ShapeDtypeStruct(shape, F32)
        finals = pl.pallas_call(
            functools.partial(finish_kernel, 0.5 / batch_total),
            out_shape=[jax.ShapeDtypeStruct((rows, width), BF16)] + [f32(LANE, width)] * 3 + [f32(1, width)] * 3 + [
                f32(1, LANE)] * 3 + [f32(1, 3), f32(1, 1)],
            in_specs=[vmem_spec] * 3,
            out_specs=[any_spec] * 12,
            scratch_shapes=[vm((3, LANE, width), F32), vm((1, 3), F32), vm((1, 1), F32), dma((4,)), dma((11,))],
            compiler_params=pltpu.CompilerParams(vmem_limit_bytes=8 * 2**20),
            name="finish",
        )(dx_all, tot, pack)
        grad_x, dw0, dw1, dw2, v0, v1, v2, n0, n1, n2, sig, loss = finals
        return (loss.reshape(1), grad_x, dw0, dw1, dw2, n0.reshape(LANE), n1.reshape(LANE), n2.reshape(LANE),
                v0.reshape(width), v1.reshape(width), v2.reshape(width), sig.reshape(3))

    in_specs = (batch_spec, row_spec, row_spec, row_spec, vec_spec, vec_spec, vec_spec, target_spec)
    out_specs = (part_spec, batch_spec, row_spec, row_spec, row_spec, vec_spec, vec_spec, vec_spec, part_spec, part_spec, part_spec, part_spec)
    return jax.shard_map(local_step, mesh=mesh, in_specs=in_specs, out_specs=out_specs, check_vma=False)
```

```python
import functools

import jax
import jax.numpy as jnp
from jax import lax
from jax.experimental import pallas as pl
from jax.experimental.pallas import tpu as pltpu
from jax.sharding import PartitionSpec as P

MESH = pl.DeviceIdType.MESH
F32 = jnp.float32
BF16 = jnp.bfloat16
LANE = 128
PAIR = 2 * LANE
FWD_ROWS = 1024
BIG_ROWS = 512
PLAIN = ((512, 6), (256, 1), (192, 1))
SHARED = ((256, 1), (192, 1), (128, 1))
SHARED_ROWS = sum(size * count for size, count in SHARED)
N_PLAIN = sum(count for _, count in PLAIN)
LAST = PLAIN[-1][0]
N_SHARED = sum(count for _, count in SHARED)


def dot_nt(lhs, rhs):
    return lax.dot_general(lhs, rhs, (((1,), (1,)), ((), ())), preferred_element_type=F32)


def dot_nn(lhs, rhs):
    return lax.dot_general(lhs, rhs, (((1,), (0,)), ((), ())), preferred_element_type=F32)


def dot_tn(lhs, rhs):
    return lax.dot_general(lhs, rhs, (((0,), (0,)), ((), ())), preferred_element_type=F32)


def split_rows(vec):
    width = vec.shape[1]
    limit = float(jnp.finfo(BF16).max)
    high = jnp.clip(vec, -limit, limit).astype(BF16).astype(F32)
    rest = vec - high
    mid = rest.astype(BF16).astype(F32)
    low = rest - mid
    row = lax.broadcasted_iota(jnp.int32, (16, width), 0)
    stacked = jnp.where(row == 0, high, jnp.where(row == 1, mid, jnp.where(row == 2, low, 0.0)))
    return stacked.astype(BF16)


def main_kernel(inv_batch, x_hbm, w0_hbm, w1_hbm, w2_hbm, u0_hbm, u1_hbm, u2_hbm, t_hbm,
                dx_out, tot_out, pack_out,
                x1, x2, y0, y1, y2, tbuf, wbuf, ubuf, e2, e1, e0, xfor, acc, facc, rbuf, frbuf, fsend,
                g_own, g_other, p_own, p_other, stat, fstat, sstat, rstat, fsstat, frstat, srow, sx, se, eq, xstat, xb,
                w_send, w_recv, u_send, u_recv, t_send, t_recv, s_send, s_recv, e_send, e_recv, d_send, d_recv,
                f_send, f_recv, h_send, h_recv, q_send, q_recv, x_send, x_recv, l_w, l_u, l_t, l_x, l_q):
    rep, dat, mod = lax.axis_index("replica"), lax.axis_index("data"), lax.axis_index("model")
    core = lax.rem(mod, 2)
    chip = mod // 2
    sib = mod + 1 - 2 * core
    cnt = lax.rem(mod + 2, 4)
    crs = lax.rem(sib + 2, 4)
    p_sib, p_cnt, p_crs = (rep, dat, sib), (rep, dat, cnt), (rep, dat, crs)
    p_y, p_ys = (rep, 1 - dat, mod), (rep, 1 - dat, sib)
    rows_own = x_hbm.shape[0] // 2
    shared_at = rows_own - SHARED_ROWS
    row_base = core * rows_own

    def each_chunk(groups, first, at, body):
        for size, count in groups:
            def step(i, carry, size=size, first=first, at=at):
                body(first + i, at + i * size, size)
                return carry
            if count == 1:
                step(0, 0)
            else:
                lax.fori_loop(0, count, step, 0)
            first, at = first + count, at + size * count
    w_hbm = [w0_hbm, w1_hbm, w2_hbm]
    u_hbm = [u0_hbm, u1_hbm, u2_hbm]

    def remote(src, dst, ssem, rsem, peer):
        return pltpu.make_async_remote_copy(src_ref=src, dst_ref=dst, send_sem=ssem, recv_sem=rsem,
                                            device_id=peer, device_id_type=MESH)

    def arrived(ref, sem):
        pltpu.make_async_copy(ref, ref, sem).wait()

    def span(start, size):
        return pl.ds(pl.multiple_of(start, size), size)

    def tile(start, size):
        return pl.ds(pl.multiple_of(start, 64), size)

    def w_copy(layer, kind):
        ssem, rsem = w_send, w_recv.at[layer, (0, 1, 2, 0, 0)[kind]]
        if kind == 0:
            return remote(w_hbm[layer], wbuf.at[layer, span(LANE * mod, LANE)], ssem, rsem, p_sib)
        if kind == 1:
            return remote(w_hbm[layer].at[span(64 * dat, 64)], wbuf.at[layer, span(LANE * mod + 64 * dat, 64)], ssem, rsem, p_cnt)
        half = 1 - dat if kind == 4 else dat
        ref = wbuf.at[layer, span(LANE * cnt + 64 * half, 64)]
        return remote(ref, ref, ssem, rsem, p_y if kind == 2 else p_sib)

    def u_copy(kind):
        ref = ubuf.at[:, mod]
        return remote(ref, ref, u_send, u_recv, (p_sib, p_cnt, p_crs)[kind])

    def t_copy(kind, idx, at, size):
        other_core = core if kind == 0 else 1 - core
        return remote(t_hbm.at[tile(other_core * rows_own + at, size)], tbuf.at[mod, tile(at, size)],
                      t_send, t_recv.at[idx], p_cnt if kind == 0 else p_crs)

    def f_copy(kind):
        if kind == 0:
            src, dst, peer = x_hbm.at[tile(row_base + shared_at, SHARED_ROWS)], xfor, p_y
        else:
            other_core = core if kind == 1 else 1 - core
            src = t_hbm.at[tile(other_core * rows_own + shared_at, SHARED_ROWS)]
            dst, peer = tbuf.at[mod, tile(rows_own, SHARED_ROWS)], p_y if kind == 1 else p_ys
        return remote(src, dst, f_send, f_recv, peer)

    def h_copy(kind, idx, at, size):
        ref = tbuf.at[mod if kind == 0 else sib, tile(at, size)]
        return remote(ref, ref, h_send, h_recv.at[idx], p_cnt)

    barrier = pltpu.get_barrier_semaphore()
    peers = (p_sib, p_cnt, p_crs, p_y, p_ys)
    for peer in peers:
        pl.semaphore_signal(barrier, inc=1, device_id=peer, device_id_type=MESH)
    local_w = [pltpu.make_async_copy(w_hbm[k], wbuf.at[k, span(LANE * mod, LANE)], l_w.at[k]) for k in range(3)]
    local_u = [pltpu.make_async_copy(u_hbm[k], ubuf.at[k, mod], l_u.at[k]) for k in range(3)]
    own_rows = span(row_base, rows_own)
    local_x = pltpu.make_async_copy(x_hbm.at[own_rows], dx_out.at[own_rows], l_x)
    local_t = pltpu.make_async_copy(t_hbm.at[own_rows], tbuf.at[mod, pl.ds(0, rows_own)], l_t)
    for k in range(3):
        local_w[k].start()
        local_u[k].start()
    local_x.start()
    local_t.start()
    last_at = shared_at - LAST
    local_q = pltpu.make_async_copy(x_hbm.at[tile((1 - core) * rows_own + last_at, LAST)], sx.at[0], l_q)
    local_q.start()
    pl.semaphore_wait(barrier, len(peers))

    for k in range(3):
        w_copy(k, 1).start()
        w_copy(k, 0).start()

    for copy in local_u:
        copy.wait()
    for kind in range(3):
        u_copy(kind).start()

    def start_targets(idx, at, size):
        t_copy(0, idx, at, size).start()
        t_copy(1, idx, at, size).start()

    each_chunk(PLAIN + SHARED, 0, 0, start_targets)
    t_sib = remote(t_hbm.at[span((1 - core) * rows_own, rows_own)], tbuf.at[mod, pl.ds(0, rows_own)], s_send, s_recv, p_sib)
    t_sib.start()
    acc[...] = jnp.zeros_like(acc)
    facc[...] = jnp.zeros_like(facc)
    stat[...] = jnp.zeros_like(stat)
    xstat[...] = jnp.zeros_like(xstat)
    fstat[...] = jnp.zeros_like(fstat)

    def relay_x(k):
        w_copy(k, 1).wait_recv()
        w_copy(k, 2).start()
        w_copy(k, 3).start()

    def relay_y(k):
        w_copy(k, 2).wait_recv()
        w_copy(k, 4).start()

    own_cols = span(PAIR * chip, PAIR)
    my_cols = span(LANE * mod, LANE)

    def q_copy(kind):
        if kind == 2:
            src, dst = x1.at[pl.ds(last_at, LAST)], sx.at[1]
        else:
            src, dst = eq.at[kind, :, span(LANE * sib, LANE)], se.at[kind]
        return remote(src, dst, q_send, q_recv.at[kind], p_sib)

    def fold(val):
        return jnp.sum(val.reshape(val.shape[0] // 8, 8, val.shape[1]), axis=0)

    def leaky(val):
        return jnp.maximum(val, 0.2 * val).astype(BF16)

    def add_grad(ref, e_val, x_val):
        part = dot_tn(e_val, x_val)
        ref[0] += part[:LANE]
        ref[1] += part[LANE:]

    def residual(y_val, slab, rows, sums=None):
        res = y_val - tbuf[slab, rows, :].astype(F32)
        grad = res * inv_batch
        if sums is not None:
            sums[0] += fold(res * res)
            sums[1] += fold(grad * y_val)
        e2[rows, span(LANE * slab, LANE)] = grad.astype(BF16)

    def last_layer(rows, sums):
        y_val = dot_nt(x2[rows, :], wbuf[2]) * inv_sigma[2]
        first = chip == 0
        own = jnp.where(first, y_val[:, :PAIR], y_val[:, PAIR:])
        y2[rows, :] = jnp.where(first, y_val[:, PAIR:], y_val[:, :PAIR])
        for j in range(2):
            residual(own[:, LANE * j:LANE * j + LANE], 2 * chip + j, rows, sums)

    inv_sigma = []
    for k in range(3):
        relay_x(k)
    for kind in range(3):
        f_copy(kind).start()
    relay_y(0)
    relay_y(1)
    for k in range(3):
        local_w[k].wait()
        if k == 0:
            arrived(ubuf.at[:, pl.ds(0, 3)], u_recv)
        arrived(wbuf.at[k, pl.ds(0, PAIR)], w_recv.at[k, 0])
        u_row = jnp.concatenate([ubuf[k, j] for j in range(4)], axis=1)
        p_vec = jnp.sum(dot_nn(split_rows(u_row), wbuf[k]), axis=0, keepdims=True)
        norm = jnp.sqrt(jnp.sum(p_vec * p_vec, axis=1, keepdims=True))
        v_vec = p_vec / jnp.maximum(norm, 1e-12)
        s_vec = jnp.sum(dot_nt(split_rows(v_vec), wbuf[k]), axis=0, keepdims=True)
        sigma = jnp.sqrt(jnp.sum(s_vec * s_vec, axis=1, keepdims=True))
        pack_out[k:k + 1, :] = v_vec
        srow[k] = jnp.broadcast_to(s_vec / sigma, srow.shape[1:])
        pack_out[3 + k:4 + k, 0:LANE] = srow[k, 0:1, span(LANE * mod, LANE)]
        pack_out[6 + k:7 + k, :] = jnp.broadcast_to(sigma, (1, pack_out.shape[1]))
        inv = 1.0 / sigma
        inv_sigma.append(inv)
        if k == 0:
            relay_y(2)
        if k == 0:
            local_x.wait()
        if k == 2:
            local_t.wait()
            t_sib.wait_recv()

        def forward(c, carry, k=k, inv=inv):
            rows = span(c * FWD_ROWS, FWD_ROWS)
            if k == 0:
                y_val = dot_nt(dx_out[span(row_base + c * FWD_ROWS, FWD_ROWS), :], wbuf[0]) * inv
                y0[rows, :] = y_val
                x1[rows, :] = leaky(y_val)
            elif k == 1:
                y_val = dot_nt(x1[rows, :], wbuf[1]) * inv
                y1[rows, :] = y_val
                x2[rows, :] = leaky(y_val)
            else:
                last_layer(rows, xstat)
                add_grad(acc.at[2], e2[rows, own_cols], x2[rows, :])
            return carry

        lax.fori_loop(0, rows_own // FWD_ROWS, forward, 0)

    def d_copy(k):
        return remote(acc.at[k, 1 - core], rbuf.at[k], d_send, d_recv.at[k], p_sib)

    def fd_copy(k):
        return remote(fsend.at[k], frbuf.at[k], d_send, d_recv.at[4 + k], p_sib)

    def p_copy(k):
        part = pl.ds((PAIR, 0, LANE)[k], (8, LANE, LANE)[k])
        return remote(p_own.at[part], p_other.at[part], d_send, d_recv.at[8 + k], p_y)

    s_copy = remote(sstat, rstat, d_send, d_recv.at[3], p_sib)
    fs_copy = remote(fsstat, frstat, d_send, d_recv.at[6], p_sib)
    g_copy = remote(g_own, g_other, d_send, d_recv.at[7], p_y)

    def dx_copy(at, size):
        ref = dx_out.at[tile(row_base + at, size)]
        return remote(ref, ref, e_send, e_recv, p_sib)

    def backward(at, size, sums, grads, idx=None, mid=None, split=False):
        rows = tile(at, size)
        b0, b1 = (eq.at[0], eq.at[1]) if split else (e0, e1)
        for j in range(2):
            residual(y2[rows, LANE * j:LANE * j + LANE], 2 - 2 * chip + j, rows)
        back = (dot_nn(e2[rows, :], wbuf[2]) * inv_sigma[2]).astype(BF16).astype(F32)
        y_val = y1[rows, :]
        grad = back * jnp.where(y_val > 0, 1.0, 0.2)
        sums[0] += fold(grad * y_val)
        b1[:size] = grad.astype(BF16)
        if split:
            grads[1, core] += dot_tn(b1[:size, my_cols], x1[rows, :])
        else:
            add_grad(grads.at[1], b1[:size, own_cols], x1[rows, :])
        back = (dot_nn(b1[:size], wbuf[1]) * inv_sigma[1]).astype(BF16).astype(F32)
        if mid is not None:
            mid(1)
        y_val = y0[rows, :]
        grad = back * jnp.where(y_val > 0, 1.0, 0.2)
        sums[1] += fold(grad * y_val)
        b0[:size] = grad.astype(BF16)
        if idx is None:
            add_grad(grads.at[0], b0[:size, own_cols], xfor[tile(at - rows_own, size), :])
            if mid is not None:
                mid(0)
        else:
            x_rows = tile(row_base + at, size)
            if split:
                grads[0, core] += dot_tn(b0[:size, my_cols], dx_out[x_rows, :])
                mid(0)
            else:
                add_grad(grads.at[0], b0[:size, own_cols], dx_out[x_rows, :])
            dx_out[x_rows, :] = (dot_nn(b0[:size], wbuf[0]) * inv_sigma[0]).astype(BF16)

    row = lax.broadcasted_iota(jnp.int32, sstat.shape, 0)

    def gather_sums(ref_sums):
        mine = jnp.zeros(sstat.shape, F32)
        for i in range(2):
            mine = jnp.where(row == 2 + i, jnp.sum(ref_sums(i), axis=0, keepdims=True), mine)
        return mine

    first_sums = [jnp.sum(xstat[i], axis=0, keepdims=True) for i in range(2)]
    xb[0] = jnp.where(row[:, :LANE] == 0, first_sums[0], jnp.where(row[:, :LANE] == 1, first_sums[1], 0.0))

    def x_copy(k):
        return remote(xb.at[2 * k], xb.at[2 * k + 1], x_send, x_recv.at[k], (p_sib, p_y, p_cnt)[k])

    def own_chunk(idx, at, size, sums, grads, mid=None, split=False):
        arrived(tbuf.at[pl.ds(0, 2), tile(at, size)], t_recv.at[idx])
        if isinstance(idx, int) and idx == N_PLAIN:
            p_copy(2).start()
        backward(at, size, sums, grads, idx, mid, split)

    n_big = PLAIN[0][1]

    def plain_send(k):
        q_copy(k).start()

    def plain_chunk(idx, at, size):
        if size == BIG_ROWS:
            @pl.when(idx == 0)
            def _():
                d_copy(2).start()
                q_copy(2).start()
                x_copy(0).start()

            @pl.when(idx == 1)
            def _():
                d_copy(2).wait_recv()
                g_own[...] = acc[2, core] + rbuf[2]
                x_copy(0).wait_recv()
                xb[2] = xb[0] + xb[1]

            @pl.when(idx == 2)
            def _():
                g_copy.start()
                x_copy(1).start()

            @pl.when(idx == n_big - 2)
            def _():
                arrived(x1.at[pl.ds(0, 3 * SHARED_ROWS // 2)], f_recv)

                def forward_on(j, h_at, h_size):
                    h_copy(0, j, h_at, h_size).start()
                    h_copy(1, j, h_at, h_size).start()

                each_chunk(SHARED, 0, rows_own, forward_on)

            @pl.when(idx == n_big - 1)
            def _():
                rows = pl.ds(rows_own, SHARED_ROWS)
                y_val = dot_nt(xfor[...], wbuf[0]) * inv_sigma[0]
                y0[rows, :] = y_val
                x1[rows, :] = leaky(y_val)
                y_val = dot_nt(x1[rows, :], wbuf[1]) * inv_sigma[1]
                y1[rows, :] = y_val
                x2[rows, :] = leaky(y_val)
                last_layer(rows, None)

        if isinstance(idx, int) and idx == n_big:
            x_copy(1).wait_recv()
            xb[4] = xb[2] + xb[3]
        last = idx == N_PLAIN - 1 if isinstance(idx, int) else False
        own_chunk(idx, at, size, stat, acc, plain_send if last else None, last)
        if isinstance(idx, int) and idx == N_PLAIN - 2:
            d_copy(1).start()
            d_copy(0).start()
            x_copy(2).start()
        dx_copy(at, size).start()

    each_chunk(PLAIN, 0, 0, plain_chunk)

    d_copy(1).wait_recv()
    q_copy(2).wait_recv()
    q_copy(1).wait_recv()
    p_own[0:LANE, :] = (acc[1, core] + rbuf[1]) + dot_tn(se[1], sx[1])
    sstat[...] = gather_sums(lambda i: stat[i])
    s_copy.start()
    p_copy(1).start()
    d_copy(0).wait_recv()
    local_q.wait()
    q_copy(0).wait_recv()
    p_own[LANE:PAIR, :] = (acc[0, core] + rbuf[0]) + dot_tn(se[0], sx[0])

    def shared_chunk(idx, at, size):
        if idx == N_PLAIN + 1:
            p_copy(0).start()
        own_chunk(idx, at, size, fstat.at[0], facc.at[0])
        dx_copy(at, size).start()
        if idx == N_PLAIN:
            s_copy.wait_recv()
            p_own[PAIR:264, :] = sstat[...] + rstat[...]

    each_chunk(SHARED, N_PLAIN, shared_at, shared_chunk)

    def last_send(k):
        fsend[k] = facc[0, k, 1 - core] + facc[1, k, 1 - core]
        if k == 1:
            fd_copy(1).start()
        if k == 0:
            fsstat[...] = gather_sums(lambda i: fstat[0, i] + fstat[1, i])
            fd_copy(0).start()
            fs_copy.start()

    def foreign_chunk(idx, at, size):
        arrived(tbuf.at[pl.ds(0, 2), tile(at, size)], h_recv.at[idx])
        last = isinstance(at, int) and at + size == rows_own + SHARED_ROWS
        backward(at, size, fstat.at[1], facc.at[1], None, last_send if last else None)

    each_chunk(SHARED, 0, rows_own, foreign_chunk)

    g_copy.wait_recv()
    tot_out[PAIR:384, :] = g_own[...] + g_other[...]
    for k in range(3):
        p_copy(k).wait_recv()
    for i, k in enumerate((1, 0)):
        part = slice(LANE * i, LANE * i + LANE)
        fd_copy(k).wait_recv()
        tot_out[part, :] = (p_own[part, :] + p_other[part, :]) + ((facc[0, k, core] + facc[1, k, core]) + frbuf[k])
    fs_copy.wait_recv()
    tot_out[384:392, :] = (p_own[PAIR:264, :] + p_other[PAIR:264, :]) + (fsstat[...] + frstat[...])
    x_copy(2).wait_recv()
    tot_out[384:392, :LANE] += xb[4] + xb[5]

    arrived(x1.at[pl.ds(0, 3 * 384)], w_send)
    arrived(ubuf.at[:, pl.ds(0, 3)], u_send)
    arrived(t_hbm, t_send)
    arrived(tbuf.at[mod, pl.ds(0, rows_own)], s_send)
    arrived(x1.at[pl.ds(0, 3 * SHARED_ROWS // 2)], f_send)
    arrived(tbuf.at[pl.ds(0, 2), pl.ds(rows_own, SHARED_ROWS)], h_send)
    arrived(y0.at[pl.ds(0, 8 * LANE + 24)], d_send)
    arrived(xb.at[pl.ds(0, 3)], x_send)
    arrived(x1.at[pl.ds(0, 3 * LAST // 2)], q_send)
    arrived(dx_out.at[own_rows], e_send)
    arrived(dx_out.at[own_rows], e_recv)


def finish_kernel(loss_scale, dx_in, tot, pack, dx_ref, dw0, dw1, dw2, v0, v1, v2, n0, n1, n2, sig_out, loss_out,
                  grads, sig_row, loss_row, sems, out_sems):
    parts = sems.shape[0]
    rows = dx_in.shape[0] // parts
    copies = [pltpu.make_async_copy(dx_in.at[pl.ds(i * rows, rows)], dx_ref.at[pl.ds(i * rows, rows)], sems.at[i]) for i in range(parts)]
    for copy in copies:
        copy.start()

    def out_copy(src, dst):
        copy = pltpu.make_async_copy(src, dst, out_sems.at[len(copies) - parts])
        copy.start()
        copies.append(copy)

    for k, (v_out, n_out) in enumerate(((v0, n0), (v1, n1), (v2, n2))):
        out_copy(pack.at[k:k + 1, :], v_out)
        out_copy(pack.at[3 + k:4 + k, 0:LANE], n_out)
    lane = lax.broadcasted_iota(jnp.int32, (1, LANE), 1)
    row = jnp.where(lane == 0, pack[6:7, 0:LANE], jnp.where(lane == 1, pack[7:8, 0:LANE], pack[8:9, 0:LANE]))
    sig_row[...] = row[:, :3]
    stats = jnp.sum(tot[384:392, :], axis=1, keepdims=True)
    loss_row[...] = loss_scale * stats[0:1]
    for k, at in enumerate((LANE, 0, PAIR)):
        inv = 1.0 / pack[6 + k:7 + k, 0:1]
        u_col = jnp.transpose(jnp.broadcast_to(pack[3 + k:4 + k, 0:LANE], (LANE, LANE)))[:, 0:1]
        grads[k] = tot[at:at + LANE, :] * inv - (stats[3 - k:4 - k] * inv) * (u_col * pack[k:k + 1, :])
    out_copy(sig_row, sig_out)
    out_copy(loss_row, loss_out)
    for k, out in enumerate((dw0, dw1, dw2)):
        out_copy(grads.at[k], out)
    for copy in copies:
        copy.wait()


def solution(mesh):
    data_size = mesh.shape["data"]
    row_spec = P(("replica", "model"), None)
    vec_spec = P(("replica", "model"))
    batch_spec = P(("replica", "data"), None)
    target_spec = P(("replica", "data"), "model")
    part_spec = P("replica")

    def local_step(x_in, w_in, w_mid, w_out, u_in, u_mid, u_out, target):
        rows, width = x_in.shape
        half = rows // 2
        ext = half + SHARED_ROWS
        batch_total = rows * data_size
        any_spec = pl.BlockSpec(memory_space=pl.ANY)
        vmem_spec = pl.BlockSpec(memory_space=pltpu.VMEM)
        dma = pltpu.SemaphoreType.DMA
        vm = pltpu.VMEM
        dx_all, tot, pack = pl.pallas_call(
            functools.partial(main_kernel, 1.0 / batch_total),
            out_shape=[vm((rows, width), BF16), vm((392, width), F32), vm((16, width), F32)],
            in_specs=[any_spec] * 8,
            out_specs=[vmem_spec] * 3,
            scratch_shapes=[
                vm((ext, width), BF16), vm((ext, width), BF16),
                vm((ext, width), F32), vm((ext, width), F32), vm((ext, PAIR), F32),
                vm((4, ext, LANE), BF16),
                vm((3, width, width), BF16),
                vm((3, 4, 1, LANE), F32),
                vm((ext, width), BF16), vm((BIG_ROWS, width), BF16), vm((BIG_ROWS, width), BF16),
                vm((SHARED_ROWS, width), BF16),
                vm((3, 2, LANE, width), F32), vm((2, 2, 2, LANE, width), F32),
                vm((3, LANE, width), F32), vm((2, LANE, width), F32), vm((2, LANE, width), F32),
                vm((LANE, width), F32), vm((LANE, width), F32),
                vm((264, width), F32), vm((264, width), F32),
                vm((2, 8, width), F32), vm((2, 2, 8, width), F32),
                vm((8, width), F32), vm((8, width), F32), vm((8, width), F32), vm((8, width), F32),
                vm((3, 8, width), F32),
                vm((2, LAST, width), BF16), vm((2, LAST, LANE), BF16), vm((2, LAST, width), BF16),
                vm((2, 8, LANE), F32), vm((6, 8, LANE), F32),
                dma(()), dma((3, 3)), dma(()), dma(()),
                dma(()), dma((N_PLAIN + N_SHARED,)), dma(()), dma(()), dma(()), dma(()), dma(()), dma((11,)),
                dma(()), dma(()), dma(()), dma((N_SHARED,)), dma(()), dma((3,)), dma(()), dma((3,)),
                dma((3,)), dma((3,)), dma(()), dma(()), dma(()),
            ],
            compiler_params=pltpu.CompilerParams(
                collective_id=0, has_side_effects=True, vmem_limit_bytes=55 * 2**20),
            name="fused_step",
        )(x_in, w_in, w_mid, w_out, u_in.reshape(1, LANE), u_mid.reshape(1, LANE), u_out.reshape(1, LANE), target)

        f32 = lambda *shape: jax.ShapeDtypeStruct(shape, F32)
        finals = pl.pallas_call(
            functools.partial(finish_kernel, 0.5 / batch_total),
            out_shape=[jax.ShapeDtypeStruct((rows, width), BF16)] + [f32(LANE, width)] * 3 + [f32(1, width)] * 3 + [
                f32(1, LANE)] * 3 + [f32(1, 3), f32(1, 1)],
            in_specs=[vmem_spec] * 3,
            out_specs=[any_spec] * 12,
            scratch_shapes=[vm((3, LANE, width), F32), vm((1, 3), F32), vm((1, 1), F32), dma((4,)), dma((11,))],
            compiler_params=pltpu.CompilerParams(vmem_limit_bytes=8 * 2**20),
            name="finish",
        )(dx_all, tot, pack)
        grad_x, dw0, dw1, dw2, v0, v1, v2, n0, n1, n2, sig, loss = finals
        return (loss.reshape(1), grad_x, dw0, dw1, dw2, n0.reshape(LANE), n1.reshape(LANE), n2.reshape(LANE),
                v0.reshape(width), v1.reshape(width), v2.reshape(width), sig.reshape(3))

    in_specs = (batch_spec, row_spec, row_spec, row_spec, vec_spec, vec_spec, vec_spec, target_spec)
    out_specs = (part_spec, batch_spec, row_spec, row_spec, row_spec, vec_spec, vec_spec, vec_spec, part_spec, part_spec, part_spec, part_spec)
    return jax.shard_map(local_step, mesh=mesh, in_specs=in_specs, out_specs=out_specs, check_vma=False)
```

```python
import functools

import jax
import jax.numpy as jnp
from jax import lax
from jax.experimental import pallas as pl
from jax.experimental.pallas import tpu as pltpu
from jax.sharding import PartitionSpec as P

MESH = pl.DeviceIdType.MESH
F32 = jnp.float32
BF16 = jnp.bfloat16
LANE = 128
PAIR = 2 * LANE
FWD_ROWS = 1024
BIG_ROWS = 512
PLAIN = ((512, 6), (256, 1), (192, 1))
SHARED = ((256, 1), (192, 1), (128, 1))
SHARED_ROWS = sum(size * count for size, count in SHARED)
N_PLAIN = sum(count for _, count in PLAIN)
LAST = PLAIN[-1][0]
N_SHARED = sum(count for _, count in SHARED)


def dot_nt(lhs, rhs):
    return lax.dot_general(lhs, rhs, (((1,), (1,)), ((), ())), preferred_element_type=F32)


def dot_nn(lhs, rhs):
    return lax.dot_general(lhs, rhs, (((1,), (0,)), ((), ())), preferred_element_type=F32)


def dot_tn(lhs, rhs):
    return lax.dot_general(lhs, rhs, (((0,), (0,)), ((), ())), preferred_element_type=F32)


def split_rows(vec):
    width = vec.shape[1]
    limit = float(jnp.finfo(BF16).max)
    high = jnp.clip(vec, -limit, limit).astype(BF16).astype(F32)
    rest = vec - high
    mid = rest.astype(BF16).astype(F32)
    low = rest - mid
    row = lax.broadcasted_iota(jnp.int32, (16, width), 0)
    stacked = jnp.where(row == 0, high, jnp.where(row == 1, mid, jnp.where(row == 2, low, 0.0)))
    return stacked.astype(BF16)


def main_kernel(inv_batch, x_hbm, w0_hbm, w1_hbm, w2_hbm, u0_hbm, u1_hbm, u2_hbm, t_hbm,
                dx_out, tot_out, pack_out,
                x1, x2, y0, y1, y2, tbuf, wbuf, ubuf, e2, e1, e0, xfor, acc, facc, rbuf, frbuf, fsend,
                g_own, g_other, p_own, p_other, stat, fstat, sstat, rstat, fsstat, frstat, srow, sx, se, eq, xstat, xb,
                w_send, w_recv, u_send, u_recv, t_send, t_recv, s_send, s_recv, e_send, e_recv, d_send, d_recv,
                f_send, f_recv, h_send, h_recv, q_send, q_recv, x_send, x_recv, l_w, l_u, l_t, l_x, l_q):
    rep, dat, mod = lax.axis_index("replica"), lax.axis_index("data"), lax.axis_index("model")
    core = lax.rem(mod, 2)
    chip = mod // 2
    sib = mod + 1 - 2 * core
    cnt = lax.rem(mod + 2, 4)
    crs = lax.rem(sib + 2, 4)
    p_sib, p_cnt, p_crs = (rep, dat, sib), (rep, dat, cnt), (rep, dat, crs)
    p_y, p_ys = (rep, 1 - dat, mod), (rep, 1 - dat, sib)
    rows_own = x_hbm.shape[0] // 2
    shared_at = rows_own - SHARED_ROWS
    row_base = core * rows_own

    def each_chunk(groups, first, at, body):
        for size, count in groups:
            def step(i, carry, size=size, first=first, at=at):
                body(first + i, at + i * size, size)
                return carry
            if count == 1:
                step(0, 0)
            else:
                lax.fori_loop(0, count, step, 0)
            first, at = first + count, at + size * count
    w_hbm = [w0_hbm, w1_hbm, w2_hbm]
    u_hbm = [u0_hbm, u1_hbm, u2_hbm]

    def remote(src, dst, ssem, rsem, peer):
        return pltpu.make_async_remote_copy(src_ref=src, dst_ref=dst, send_sem=ssem, recv_sem=rsem,
                                            device_id=peer, device_id_type=MESH)

    def arrived(ref, sem):
        pltpu.make_async_copy(ref, ref, sem).wait()

    def span(start, size):
        return pl.ds(pl.multiple_of(start, size), size)

    def tile(start, size):
        return pl.ds(pl.multiple_of(start, 64), size)

    def w_copy(layer, kind):
        ssem, rsem = w_send, w_recv.at[layer, (0, 1, 2, 0, 0)[kind]]
        if kind == 0:
            return remote(w_hbm[layer], wbuf.at[layer, span(LANE * mod, LANE)], ssem, rsem, p_sib)
        if kind == 1:
            return remote(w_hbm[layer].at[span(64 * dat, 64)], wbuf.at[layer, span(LANE * mod + 64 * dat, 64)], ssem, rsem, p_cnt)
        half = 1 - dat if kind == 4 else dat
        ref = wbuf.at[layer, span(LANE * cnt + 64 * half, 64)]
        return remote(ref, ref, ssem, rsem, p_y if kind == 2 else p_sib)

    def u_copy(kind):
        ref = ubuf.at[:, mod]
        return remote(ref, ref, u_send, u_recv, (p_sib, p_cnt, p_crs)[kind])

    def t_copy(kind, idx, at, size):
        other_core = core if kind == 0 else 1 - core
        return remote(t_hbm.at[tile(other_core * rows_own + at, size)], tbuf.at[mod, tile(at, size)],
                      t_send, t_recv.at[idx], p_cnt if kind == 0 else p_crs)

    def f_copy(kind):
        if kind == 0:
            src, dst, peer = x_hbm.at[tile(row_base + shared_at, SHARED_ROWS)], xfor, p_y
        else:
            other_core = core if kind == 1 else 1 - core
            src = t_hbm.at[tile(other_core * rows_own + shared_at, SHARED_ROWS)]
            dst, peer = tbuf.at[mod, tile(rows_own, SHARED_ROWS)], p_y if kind == 1 else p_ys
        return remote(src, dst, f_send, f_recv, peer)

    def h_copy(kind, idx, at, size):
        ref = tbuf.at[mod if kind == 0 else sib, tile(at, size)]
        return remote(ref, ref, h_send, h_recv.at[idx], p_cnt)

    barrier = pltpu.get_barrier_semaphore()
    peers = (p_sib, p_cnt, p_crs, p_y, p_ys)
    for peer in peers:
        pl.semaphore_signal(barrier, inc=1, device_id=peer, device_id_type=MESH)
    local_w = [pltpu.make_async_copy(w_hbm[k], wbuf.at[k, span(LANE * mod, LANE)], l_w) for k in range(3)]
    local_u = [pltpu.make_async_copy(u_hbm[k], ubuf.at[k, mod], l_u) for k in range(3)]
    own_rows = span(row_base, rows_own)
    local_x = pltpu.make_async_copy(x_hbm.at[own_rows], dx_out.at[own_rows], l_x)
    local_t = pltpu.make_async_copy(t_hbm.at[own_rows], tbuf.at[mod, pl.ds(0, rows_own)], l_t)
    for k in range(3):
        local_w[k].start()
        local_u[k].start()
    local_x.start()
    local_t.start()
    last_at = shared_at - LAST
    local_q = pltpu.make_async_copy(x_hbm.at[tile((1 - core) * rows_own + last_at, LAST)], sx.at[0], l_q)
    local_q.start()
    pl.semaphore_wait(barrier, len(peers))

    for k in range(3):
        w_copy(k, 1).start()
        w_copy(k, 0).start()

    arrived(ubuf.at[:, mod], l_u)
    for kind in range(3):
        u_copy(kind).start()

    def start_targets(idx, at, size):
        t_copy(0, idx, at, size).start()
        t_copy(1, idx, at, size).start()

    each_chunk(PLAIN + SHARED, 0, 0, start_targets)
    t_sib = remote(t_hbm.at[span((1 - core) * rows_own, rows_own)], tbuf.at[mod, pl.ds(0, rows_own)], s_send, s_recv, p_sib)
    t_sib.start()
    acc[...] = jnp.zeros_like(acc)
    facc[...] = jnp.zeros_like(facc)
    stat[...] = jnp.zeros_like(stat)
    xstat[...] = jnp.zeros_like(xstat)
    fstat[...] = jnp.zeros_like(fstat)

    def relay_x(k):
        w_copy(k, 1).wait_recv()
        w_copy(k, 2).start()
        w_copy(k, 3).start()

    def relay_y(k):
        w_copy(k, 2).wait_recv()
        w_copy(k, 4).start()

    own_cols = span(PAIR * chip, PAIR)
    my_cols = span(LANE * mod, LANE)

    def q_copy(kind):
        if kind == 2:
            src, dst = x1.at[pl.ds(last_at, LAST)], sx.at[1]
        else:
            src, dst = eq.at[kind, :, span(LANE * sib, LANE)], se.at[kind]
        return remote(src, dst, q_send, q_recv.at[kind], p_sib)

    def fold(val):
        return jnp.sum(val.reshape(val.shape[0] // 8, 8, val.shape[1]), axis=0)

    def leaky(val):
        return jnp.maximum(val, 0.2 * val).astype(BF16)

    def add_grad(ref, e_val, x_val):
        part = dot_tn(e_val, x_val)
        ref[0] += part[:LANE]
        ref[1] += part[LANE:]

    def residual(y_val, slab, rows, sums=None):
        res = y_val - tbuf[slab, rows, :].astype(F32)
        grad = res * inv_batch
        if sums is not None:
            sums[0] += fold(res * res)
            sums[1] += fold(grad * y_val)
        e2[rows, span(LANE * slab, LANE)] = grad.astype(BF16)

    def last_layer(rows, sums):
        y_val = dot_nt(x2[rows, :], wbuf[2]) * inv_sigma[2]
        first = chip == 0
        own = jnp.where(first, y_val[:, :PAIR], y_val[:, PAIR:])
        y2[rows, :] = jnp.where(first, y_val[:, PAIR:], y_val[:, :PAIR])
        for j in range(2):
            residual(own[:, LANE * j:LANE * j + LANE], 2 * chip + j, rows, sums)

    inv_sigma = []
    for k in range(3):
        relay_x(k)
    for kind in range(3):
        f_copy(kind).start()
    relay_y(0)
    relay_y(1)
    for k in range(3):
        if k == 0:
            arrived(wbuf.at[:, span(LANE * mod, LANE)], l_w)
            arrived(ubuf.at[:, pl.ds(0, 3)], u_recv)
        arrived(wbuf.at[k, pl.ds(0, PAIR)], w_recv.at[k, 0])
        u_row = jnp.concatenate([ubuf[k, j] for j in range(4)], axis=1)
        p_vec = jnp.sum(dot_nn(split_rows(u_row), wbuf[k]), axis=0, keepdims=True)
        norm = jnp.sqrt(jnp.sum(p_vec * p_vec, axis=1, keepdims=True))
        v_vec = p_vec / jnp.maximum(norm, 1e-12)
        s_vec = jnp.sum(dot_nt(split_rows(v_vec), wbuf[k]), axis=0, keepdims=True)
        sigma = jnp.sqrt(jnp.sum(s_vec * s_vec, axis=1, keepdims=True))
        pack_out[k:k + 1, :] = v_vec
        srow[k] = jnp.broadcast_to(s_vec / sigma, srow.shape[1:])
        pack_out[3 + k:4 + k, 0:LANE] = srow[k, 0:1, span(LANE * mod, LANE)]
        pack_out[6 + k:7 + k, :] = jnp.broadcast_to(sigma, (1, pack_out.shape[1]))
        inv = 1.0 / sigma
        inv_sigma.append(inv)
        if k == 0:
            relay_y(2)
        if k == 0:
            local_x.wait()
        if k == 2:
            local_t.wait()
            t_sib.wait_recv()

        def forward(c, carry, k=k, inv=inv):
            rows = span(c * FWD_ROWS, FWD_ROWS)
            if k == 0:
                y_val = dot_nt(dx_out[span(row_base + c * FWD_ROWS, FWD_ROWS), :], wbuf[0]) * inv
                y0[rows, :] = y_val
                x1[rows, :] = leaky(y_val)
            elif k == 1:
                y_val = dot_nt(x1[rows, :], wbuf[1]) * inv
                y1[rows, :] = y_val
                x2[rows, :] = leaky(y_val)
            else:
                last_layer(rows, xstat)
                add_grad(acc.at[2], e2[rows, own_cols], x2[rows, :])
            return carry

        lax.fori_loop(0, rows_own // FWD_ROWS, forward, 0)

    def d_copy(k):
        return remote(acc.at[k, 1 - core], rbuf.at[k], d_send, d_recv.at[k], p_sib)

    def fd_copy(k):
        return remote(fsend.at[k], frbuf.at[k], d_send, d_recv.at[4], p_sib)

    def p_copy(k):
        part = pl.ds((PAIR, 0, LANE)[k], (8, LANE, LANE)[k])
        return remote(p_own.at[part], p_other.at[part], d_send, d_recv.at[5], p_y)

    s_copy = remote(sstat, rstat, d_send, d_recv.at[3], p_sib)
    fs_copy = remote(fsstat, frstat, d_send, d_recv.at[6], p_sib)
    g_copy = remote(g_own, g_other, d_send, d_recv.at[7], p_y)

    def dx_copy(at, size):
        ref = dx_out.at[tile(row_base + at, size)]
        return remote(ref, ref, e_send, e_recv, p_sib)

    def backward(at, size, sums, grads, idx=None, mid=None, split=False):
        rows = tile(at, size)
        b0, b1 = (eq.at[0], eq.at[1]) if split else (e0, e1)
        for j in range(2):
            residual(y2[rows, LANE * j:LANE * j + LANE], 2 - 2 * chip + j, rows)
        back = (dot_nn(e2[rows, :], wbuf[2]) * inv_sigma[2]).astype(BF16).astype(F32)
        y_val = y1[rows, :]
        grad = back * jnp.where(y_val > 0, 1.0, 0.2)
        sums[0] += fold(grad * y_val)
        b1[:size] = grad.astype(BF16)
        if split:
            grads[1, core] += dot_tn(b1[:size, my_cols], x1[rows, :])
        else:
            add_grad(grads.at[1], b1[:size, own_cols], x1[rows, :])
        back = (dot_nn(b1[:size], wbuf[1]) * inv_sigma[1]).astype(BF16).astype(F32)
        if mid is not None:
            mid(1)
        y_val = y0[rows, :]
        grad = back * jnp.where(y_val > 0, 1.0, 0.2)
        sums[1] += fold(grad * y_val)
        b0[:size] = grad.astype(BF16)
        if idx is None:
            add_grad(grads.at[0], b0[:size, own_cols], xfor[tile(at - rows_own, size), :])
            if mid is not None:
                mid(0)
        else:
            x_rows = tile(row_base + at, size)
            if split:
                grads[0, core] += dot_tn(b0[:size, my_cols], dx_out[x_rows, :])
                mid(0)
            else:
                add_grad(grads.at[0], b0[:size, own_cols], dx_out[x_rows, :])
            dx_out[x_rows, :] = (dot_nn(b0[:size], wbuf[0]) * inv_sigma[0]).astype(BF16)

    row = lax.broadcasted_iota(jnp.int32, sstat.shape, 0)

    def gather_sums(ref_sums):
        mine = jnp.zeros(sstat.shape, F32)
        for i in range(2):
            mine = jnp.where(row == 2 + i, jnp.sum(ref_sums(i), axis=0, keepdims=True), mine)
        return mine

    first_sums = [jnp.sum(xstat[i], axis=0, keepdims=True) for i in range(2)]
    xb[0] = jnp.where(row[:, :LANE] == 0, first_sums[0], jnp.where(row[:, :LANE] == 1, first_sums[1], 0.0))

    def x_copy(k):
        return remote(xb.at[2 * k], xb.at[2 * k + 1], x_send, x_recv.at[k], (p_sib, p_y, p_cnt)[k])

    def own_chunk(idx, at, size, sums, grads, mid=None, split=False):
        arrived(tbuf.at[pl.ds(0, 2), tile(at, size)], t_recv.at[idx])
        if isinstance(idx, int) and idx == N_PLAIN:
            p_copy(2).start()
        backward(at, size, sums, grads, idx, mid, split)

    n_big = PLAIN[0][1]

    def plain_send(k):
        q_copy(k).start()

    def plain_chunk(idx, at, size):
        if size == BIG_ROWS:
            @pl.when(idx == 0)
            def _():
                d_copy(2).start()
                q_copy(2).start()
                x_copy(0).start()

            @pl.when(idx == 1)
            def _():
                d_copy(2).wait_recv()
                g_own[...] = acc[2, core] + rbuf[2]
                x_copy(0).wait_recv()
                xb[2] = xb[0] + xb[1]

            @pl.when(idx == 2)
            def _():
                g_copy.start()
                x_copy(1).start()

            @pl.when(idx == n_big - 2)
            def _():
                arrived(x1.at[pl.ds(0, 3 * SHARED_ROWS // 2)], f_recv)

                def forward_on(j, h_at, h_size):
                    h_copy(0, j, h_at, h_size).start()
                    h_copy(1, j, h_at, h_size).start()

                each_chunk(SHARED, 0, rows_own, forward_on)

            @pl.when(idx == n_big - 1)
            def _():
                rows = pl.ds(rows_own, SHARED_ROWS)
                y_val = dot_nt(xfor[...], wbuf[0]) * inv_sigma[0]
                y0[rows, :] = y_val
                x1[rows, :] = leaky(y_val)
                y_val = dot_nt(x1[rows, :], wbuf[1]) * inv_sigma[1]
                y1[rows, :] = y_val
                x2[rows, :] = leaky(y_val)
                last_layer(rows, None)

        if isinstance(idx, int) and idx == n_big:
            x_copy(1).wait_recv()
            xb[4] = xb[2] + xb[3]
        last = idx == N_PLAIN - 1 if isinstance(idx, int) else False
        own_chunk(idx, at, size, stat, acc, plain_send if last else None, last)
        if isinstance(idx, int) and idx == N_PLAIN - 2:
            d_copy(1).start()
            d_copy(0).start()
            x_copy(2).start()
        dx_copy(at, size).start()

    each_chunk(PLAIN, 0, 0, plain_chunk)

    d_copy(1).wait_recv()
    q_copy(2).wait_recv()
    q_copy(1).wait_recv()
    p_own[0:LANE, :] = (acc[1, core] + rbuf[1]) + dot_tn(se[1], sx[1])
    sstat[...] = gather_sums(lambda i: stat[i])
    s_copy.start()
    p_copy(1).start()
    d_copy(0).wait_recv()
    local_q.wait()
    q_copy(0).wait_recv()
    p_own[LANE:PAIR, :] = (acc[0, core] + rbuf[0]) + dot_tn(se[0], sx[0])

    def shared_chunk(idx, at, size):
        if idx == N_PLAIN + 1:
            p_copy(0).start()
        own_chunk(idx, at, size, fstat.at[0], facc.at[0])
        dx_copy(at, size).start()
        if idx == N_PLAIN:
            s_copy.wait_recv()
            p_own[PAIR:264, :] = sstat[...] + rstat[...]

    each_chunk(SHARED, N_PLAIN, shared_at, shared_chunk)

    def last_send(k):
        fsend[k] = facc[0, k, 1 - core] + facc[1, k, 1 - core]
        if k == 1:
            fd_copy(1).start()
        if k == 0:
            fsstat[...] = gather_sums(lambda i: fstat[0, i] + fstat[1, i])
            fd_copy(0).start()
            fs_copy.start()

    def foreign_chunk(idx, at, size):
        arrived(tbuf.at[pl.ds(0, 2), tile(at, size)], h_recv.at[idx])
        last = isinstance(at, int) and at + size == rows_own + SHARED_ROWS
        backward(at, size, fstat.at[1], facc.at[1], None, last_send if last else None)

    each_chunk(SHARED, 0, rows_own, foreign_chunk)

    g_copy.wait_recv()
    tot_out[PAIR:384, :] = g_own[...] + g_other[...]
    arrived(p_other, d_recv.at[5])
    arrived(frbuf, d_recv.at[4])
    for i, k in enumerate((1, 0)):
        part = slice(LANE * i, LANE * i + LANE)
        tot_out[part, :] = (p_own[part, :] + p_other[part, :]) + ((facc[0, k, core] + facc[1, k, core]) + frbuf[k])
    fs_copy.wait_recv()
    tot_out[384:392, :] = (p_own[PAIR:264, :] + p_other[PAIR:264, :]) + (fsstat[...] + frstat[...])
    x_copy(2).wait_recv()
    tot_out[384:392, :LANE] += xb[4] + xb[5]

    arrived(x1.at[pl.ds(0, 3 * 384)], w_send)
    arrived(ubuf.at[:, pl.ds(0, 3)], u_send)
    arrived(t_hbm, t_send)
    arrived(tbuf.at[mod, pl.ds(0, rows_own)], s_send)
    arrived(x1.at[pl.ds(0, 3 * SHARED_ROWS // 2)], f_send)
    arrived(tbuf.at[pl.ds(0, 2), pl.ds(rows_own, SHARED_ROWS)], h_send)
    arrived(y0.at[pl.ds(0, 8 * LANE + 24)], d_send)
    arrived(xb.at[pl.ds(0, 3)], x_send)
    arrived(x1.at[pl.ds(0, 3 * LAST // 2)], q_send)
    arrived(dx_out.at[own_rows], e_send)
    arrived(dx_out.at[own_rows], e_recv)


def finish_kernel(loss_scale, dx_in, tot, pack, dx_ref, dw0, dw1, dw2, v0, v1, v2, n0, n1, n2, sig_out, loss_out,
                  grads, sig_row, loss_row, sems, out_sems):
    parts = sems.shape[0]
    rows = dx_in.shape[0] // parts
    copies = [pltpu.make_async_copy(dx_in.at[pl.ds(i * rows, rows)], dx_ref.at[pl.ds(i * rows, rows)], sems.at[i]) for i in range(parts)]
    for copy in copies:
        copy.start()

    def out_copy(src, dst):
        copy = pltpu.make_async_copy(src, dst, out_sems.at[len(copies) - parts])
        copy.start()
        copies.append(copy)

    for k, (v_out, n_out) in enumerate(((v0, n0), (v1, n1), (v2, n2))):
        out_copy(pack.at[k:k + 1, :], v_out)
        out_copy(pack.at[3 + k:4 + k, 0:LANE], n_out)
    lane = lax.broadcasted_iota(jnp.int32, (1, LANE), 1)
    row = jnp.where(lane == 0, pack[6:7, 0:LANE], jnp.where(lane == 1, pack[7:8, 0:LANE], pack[8:9, 0:LANE]))
    sig_row[...] = row[:, :3]
    stats = jnp.sum(tot[384:392, :], axis=1, keepdims=True)
    loss_row[...] = loss_scale * stats[0:1]
    for k, at in enumerate((LANE, 0, PAIR)):
        inv = 1.0 / pack[6 + k:7 + k, 0:1]
        u_col = jnp.transpose(jnp.broadcast_to(pack[3 + k:4 + k, 0:LANE], (LANE, LANE)))[:, 0:1]
        grads[k] = tot[at:at + LANE, :] * inv - (stats[3 - k:4 - k] * inv) * (u_col * pack[k:k + 1, :])
    out_copy(sig_row, sig_out)
    out_copy(loss_row, loss_out)
    for k, out in enumerate((dw0, dw1, dw2)):
        out_copy(grads.at[k], out)
    for copy in copies:
        copy.wait()


def solution(mesh):
    data_size = mesh.shape["data"]
    row_spec = P(("replica", "model"), None)
    vec_spec = P(("replica", "model"))
    batch_spec = P(("replica", "data"), None)
    target_spec = P(("replica", "data"), "model")
    part_spec = P("replica")

    def local_step(x_in, w_in, w_mid, w_out, u_in, u_mid, u_out, target):
        rows, width = x_in.shape
        half = rows // 2
        ext = half + SHARED_ROWS
        batch_total = rows * data_size
        any_spec = pl.BlockSpec(memory_space=pl.ANY)
        vmem_spec = pl.BlockSpec(memory_space=pltpu.VMEM)
        dma = pltpu.SemaphoreType.DMA
        vm = pltpu.VMEM
        dx_all, tot, pack = pl.pallas_call(
            functools.partial(main_kernel, 1.0 / batch_total),
            out_shape=[vm((rows, width), BF16), vm((392, width), F32), vm((16, width), F32)],
            in_specs=[any_spec] * 8,
            out_specs=[vmem_spec] * 3,
            scratch_shapes=[
                vm((ext, width), BF16), vm((ext, width), BF16),
                vm((ext, width), F32), vm((ext, width), F32), vm((ext, PAIR), F32),
                vm((4, ext, LANE), BF16),
                vm((3, width, width), BF16),
                vm((3, 4, 1, LANE), F32),
                vm((ext, width), BF16), vm((BIG_ROWS, width), BF16), vm((BIG_ROWS, width), BF16),
                vm((SHARED_ROWS, width), BF16),
                vm((3, 2, LANE, width), F32), vm((2, 2, 2, LANE, width), F32),
                vm((3, LANE, width), F32), vm((2, LANE, width), F32), vm((2, LANE, width), F32),
                vm((LANE, width), F32), vm((LANE, width), F32),
                vm((264, width), F32), vm((264, width), F32),
                vm((2, 8, width), F32), vm((2, 2, 8, width), F32),
                vm((8, width), F32), vm((8, width), F32), vm((8, width), F32), vm((8, width), F32),
                vm((3, 8, width), F32),
                vm((2, LAST, width), BF16), vm((2, LAST, LANE), BF16), vm((2, LAST, width), BF16),
                vm((2, 8, LANE), F32), vm((6, 8, LANE), F32),
                dma(()), dma((3, 3)), dma(()), dma(()),
                dma(()), dma((N_PLAIN + N_SHARED,)), dma(()), dma(()), dma(()), dma(()), dma(()), dma((8,)),
                dma(()), dma(()), dma(()), dma((N_SHARED,)), dma(()), dma((3,)), dma(()), dma((3,)),
                dma(()), dma(()), dma(()), dma(()), dma(()),
            ],
            compiler_params=pltpu.CompilerParams(
                collective_id=0, has_side_effects=True, vmem_limit_bytes=55 * 2**20),
            name="fused_step",
        )(x_in, w_in, w_mid, w_out, u_in.reshape(1, LANE), u_mid.reshape(1, LANE), u_out.reshape(1, LANE), target)

        f32 = lambda *shape: jax.ShapeDtypeStruct(shape, F32)
        finals = pl.pallas_call(
            functools.partial(finish_kernel, 0.5 / batch_total),
            out_shape=[jax.ShapeDtypeStruct((rows, width), BF16)] + [f32(LANE, width)] * 3 + [f32(1, width)] * 3 + [
                f32(1, LANE)] * 3 + [f32(1, 3), f32(1, 1)],
            in_specs=[vmem_spec] * 3,
            out_specs=[any_spec] * 12,
            scratch_shapes=[vm((3, LANE, width), F32), vm((1, 3), F32), vm((1, 1), F32), dma((4,)), dma((11,))],
            compiler_params=pltpu.CompilerParams(vmem_limit_bytes=8 * 2**20),
            name="finish",
        )(dx_all, tot, pack)
        grad_x, dw0, dw1, dw2, v0, v1, v2, n0, n1, n2, sig, loss = finals
        return (loss.reshape(1), grad_x, dw0, dw1, dw2, n0.reshape(LANE), n1.reshape(LANE), n2.reshape(LANE),
                v0.reshape(width), v1.reshape(width), v2.reshape(width), sig.reshape(3))

    in_specs = (batch_spec, row_spec, row_spec, row_spec, vec_spec, vec_spec, vec_spec, target_spec)
    out_specs = (part_spec, batch_spec, row_spec, row_spec, row_spec, vec_spec, vec_spec, vec_spec, part_spec, part_spec, part_spec, part_spec)
    return jax.shard_map(local_step, mesh=mesh, in_specs=in_specs, out_specs=out_specs, check_vma=False)
```

```python
import functools

import jax
import jax.numpy as jnp
from jax import lax
from jax.experimental import pallas as pl
from jax.experimental.pallas import tpu as pltpu
from jax.sharding import PartitionSpec as P

MESH = pl.DeviceIdType.MESH
F32 = jnp.float32
BF16 = jnp.bfloat16
LANE = 128
PAIR = 2 * LANE
FWD_ROWS = 1024
BIG_ROWS = 512
PLAIN = ((512, 6), (256, 1), (192, 1))
SHARED = ((256, 1), (192, 1), (128, 1))
SHARED_ROWS = sum(size * count for size, count in SHARED)
N_PLAIN = sum(count for _, count in PLAIN)
LAST = PLAIN[-1][0]
N_SHARED = sum(count for _, count in SHARED)


def dot_nt(lhs, rhs):
    return lax.dot_general(lhs, rhs, (((1,), (1,)), ((), ())), preferred_element_type=F32)


def dot_nn(lhs, rhs):
    return lax.dot_general(lhs, rhs, (((1,), (0,)), ((), ())), preferred_element_type=F32)


def dot_tn(lhs, rhs):
    return lax.dot_general(lhs, rhs, (((0,), (0,)), ((), ())), preferred_element_type=F32)


def split_rows(vec):
    width = vec.shape[1]
    limit = float(jnp.finfo(BF16).max)
    high = jnp.clip(vec, -limit, limit).astype(BF16).astype(F32)
    rest = vec - high
    mid = rest.astype(BF16).astype(F32)
    low = rest - mid
    row = lax.broadcasted_iota(jnp.int32, (16, width), 0)
    stacked = jnp.where(row == 0, high, jnp.where(row == 1, mid, jnp.where(row == 2, low, 0.0)))
    return stacked.astype(BF16)


def main_kernel(inv_batch, x_hbm, w0_hbm, w1_hbm, w2_hbm, u0_hbm, u1_hbm, u2_hbm, t_hbm,
                dx_out, tot_out, pack_out,
                x1, x2, y0, y1, y2, tbuf, wbuf, ubuf, e2, e1, e0, xfor, acc, facc, rbuf, frbuf, fsend,
                g_own, g_other, p_own, p_other, stat, fstat, sstat, rstat, fsstat, frstat, srow, sx, se, eq, xstat, xb,
                w_send, w_recv, u_send, u_recv, t_recv, s_recv, e_recv, d_send, d_recv,
                f_recv, h_recv, q_recv, x_send, x_recv, l_w, l_u, l_x, l_q):
    rep, dat, mod = lax.axis_index("replica"), lax.axis_index("data"), lax.axis_index("model")
    core = lax.rem(mod, 2)
    chip = mod // 2
    sib = mod + 1 - 2 * core
    cnt = lax.rem(mod + 2, 4)
    crs = lax.rem(sib + 2, 4)
    p_sib, p_cnt, p_crs = (rep, dat, sib), (rep, dat, cnt), (rep, dat, crs)
    p_y, p_ys = (rep, 1 - dat, mod), (rep, 1 - dat, sib)
    rows_own = x_hbm.shape[0] // 2
    shared_at = rows_own - SHARED_ROWS
    row_base = core * rows_own

    def each_chunk(groups, first, at, body):
        for size, count in groups:
            def step(i, carry, size=size, first=first, at=at):
                body(first + i, at + i * size, size)
                return carry
            if count == 1:
                step(0, 0)
            else:
                lax.fori_loop(0, count, step, 0)
            first, at = first + count, at + size * count
    w_hbm = [w0_hbm, w1_hbm, w2_hbm]
    u_hbm = [u0_hbm, u1_hbm, u2_hbm]

    def remote(src, dst, ssem, rsem, peer):
        return pltpu.make_async_remote_copy(src_ref=src, dst_ref=dst, send_sem=ssem, recv_sem=rsem,
                                            device_id=peer, device_id_type=MESH)

    def arrived(ref, sem):
        pltpu.make_async_copy(ref, ref, sem).wait()

    def span(start, size):
        return pl.ds(pl.multiple_of(start, size), size)

    def tile(start, size):
        return pl.ds(pl.multiple_of(start, 64), size)

    def w_copy(layer, kind):
        ssem, rsem = w_send, w_recv.at[layer, (0, 1, 2, 0, 0)[kind]]
        if kind == 0:
            return remote(w_hbm[layer], wbuf.at[layer, span(LANE * mod, LANE)], ssem, rsem, p_sib)
        if kind == 1:
            return remote(w_hbm[layer].at[span(64 * dat, 64)], wbuf.at[layer, span(LANE * mod + 64 * dat, 64)], ssem, rsem, p_cnt)
        half = 1 - dat if kind == 4 else dat
        ref = wbuf.at[layer, span(LANE * cnt + 64 * half, 64)]
        return remote(ref, ref, ssem, rsem, p_y if kind == 2 else p_sib)

    def u_copy(kind):
        ref = ubuf.at[:, mod]
        return remote(ref, ref, u_send, u_recv, (p_sib, p_cnt, p_crs)[kind])

    def t_copy(kind, idx, at, size):
        other_core = core if kind == 0 else 1 - core
        return remote(t_hbm.at[tile(other_core * rows_own + at, size)], tbuf.at[mod, tile(at, size)],
                      w_send, t_recv.at[idx], p_cnt if kind == 0 else p_crs)

    def f_copy(kind):
        if kind == 0:
            src, dst, peer = x_hbm.at[tile(row_base + shared_at, SHARED_ROWS)], xfor, p_y
        else:
            other_core = core if kind == 1 else 1 - core
            src = t_hbm.at[tile(other_core * rows_own + shared_at, SHARED_ROWS)]
            dst, peer = tbuf.at[mod, tile(rows_own, SHARED_ROWS)], p_y if kind == 1 else p_ys
        return remote(src, dst, w_send, f_recv, peer)

    def h_copy(kind, idx, at, size):
        ref = tbuf.at[mod if kind == 0 else sib, tile(at, size)]
        return remote(ref, ref, w_send, h_recv.at[idx], p_cnt)

    barrier = pltpu.get_barrier_semaphore()
    peers = (p_sib, p_cnt, p_crs, p_y, p_ys)
    for peer in peers:
        pl.semaphore_signal(barrier, inc=1, device_id=peer, device_id_type=MESH)
    local_w = [pltpu.make_async_copy(w_hbm[k], wbuf.at[k, span(LANE * mod, LANE)], l_w) for k in range(3)]
    local_u = [pltpu.make_async_copy(u_hbm[k], ubuf.at[k, mod], l_u) for k in range(3)]
    own_rows = span(row_base, rows_own)
    local_x = pltpu.make_async_copy(x_hbm.at[own_rows], dx_out.at[own_rows], l_x)
    local_t = pltpu.make_async_copy(t_hbm.at[own_rows], tbuf.at[mod, pl.ds(0, rows_own)], s_recv)
    for k in range(3):
        local_w[k].start()
        local_u[k].start()
    local_x.start()
    local_t.start()
    last_at = shared_at - LAST
    local_q = pltpu.make_async_copy(x_hbm.at[tile((1 - core) * rows_own + last_at, LAST)], sx.at[0], l_q)
    local_q.start()
    pl.semaphore_wait(barrier, len(peers))

    for k in range(3):
        w_copy(k, 1).start()
        w_copy(k, 0).start()

    arrived(ubuf.at[:, mod], l_u)
    for kind in range(3):
        u_copy(kind).start()

    def start_targets(idx, at, size):
        t_copy(0, idx, at, size).start()
        t_copy(1, idx, at, size).start()

    each_chunk(PLAIN + SHARED, 0, 0, start_targets)
    t_sib = remote(t_hbm.at[span((1 - core) * rows_own, rows_own)], tbuf.at[mod, pl.ds(0, rows_own)], w_send, s_recv, p_sib)
    t_sib.start()
    acc[...] = jnp.zeros_like(acc)
    facc[...] = jnp.zeros_like(facc)
    stat[...] = jnp.zeros_like(stat)
    xstat[...] = jnp.zeros_like(xstat)
    fstat[...] = jnp.zeros_like(fstat)

    def relay_x(k):
        w_copy(k, 1).wait_recv()
        w_copy(k, 2).start()
        w_copy(k, 3).start()

    def relay_y(k):
        w_copy(k, 2).wait_recv()
        w_copy(k, 4).start()

    own_cols = span(PAIR * chip, PAIR)
    my_cols = span(LANE * mod, LANE)

    def q_copy(kind):
        if kind == 2:
            src, dst = x1.at[pl.ds(last_at, LAST)], sx.at[1]
        else:
            src, dst = eq.at[kind, :, span(LANE * sib, LANE)], se.at[kind]
        return remote(src, dst, w_send, q_recv.at[kind], p_sib)

    def fold(val):
        return jnp.sum(val.reshape(val.shape[0] // 8, 8, val.shape[1]), axis=0)

    def leaky(val):
        return jnp.maximum(val, 0.2 * val).astype(BF16)

    def add_grad(ref, e_val, x_val):
        part = dot_tn(e_val, x_val)
        ref[0] += part[:LANE]
        ref[1] += part[LANE:]

    def residual(y_val, slab, rows, sums=None):
        res = y_val - tbuf[slab, rows, :].astype(F32)
        grad = res * inv_batch
        if sums is not None:
            sums[0] += fold(res * res)
            sums[1] += fold(grad * y_val)
        e2[rows, span(LANE * slab, LANE)] = grad.astype(BF16)

    def last_layer(rows, sums):
        y_val = dot_nt(x2[rows, :], wbuf[2]) * inv_sigma[2]
        first = chip == 0
        own = jnp.where(first, y_val[:, :PAIR], y_val[:, PAIR:])
        y2[rows, :] = jnp.where(first, y_val[:, PAIR:], y_val[:, :PAIR])
        for j in range(2):
            residual(own[:, LANE * j:LANE * j + LANE], 2 * chip + j, rows, sums)

    inv_sigma = []
    for k in range(3):
        relay_x(k)
    for kind in range(3):
        f_copy(kind).start()
    relay_y(0)
    relay_y(1)
    for k in range(3):
        if k == 0:
            arrived(wbuf.at[:, span(LANE * mod, LANE)], l_w)
            arrived(ubuf.at[:, pl.ds(0, 3)], u_recv)
        arrived(wbuf.at[k, pl.ds(0, PAIR)], w_recv.at[k, 0])
        u_row = jnp.concatenate([ubuf[k, j] for j in range(4)], axis=1)
        p_vec = jnp.sum(dot_nn(split_rows(u_row), wbuf[k]), axis=0, keepdims=True)
        norm = jnp.sqrt(jnp.sum(p_vec * p_vec, axis=1, keepdims=True))
        v_vec = p_vec / jnp.maximum(norm, 1e-12)
        s_vec = jnp.sum(dot_nt(split_rows(v_vec), wbuf[k]), axis=0, keepdims=True)
        sigma = jnp.sqrt(jnp.sum(s_vec * s_vec, axis=1, keepdims=True))
        pack_out[k:k + 1, :] = v_vec
        srow[k] = jnp.broadcast_to(s_vec / sigma, srow.shape[1:])
        pack_out[3 + k:4 + k, 0:LANE] = srow[k, 0:1, span(LANE * mod, LANE)]
        pack_out[6 + k:7 + k, :] = jnp.broadcast_to(sigma, (1, pack_out.shape[1]))
        inv = 1.0 / sigma
        inv_sigma.append(inv)
        if k == 0:
            relay_y(2)
        if k == 0:
            local_x.wait()
        if k == 2:
            arrived(tbuf.at[pl.ds(0, 2), pl.ds(0, rows_own)], s_recv)

        def forward(c, carry, k=k, inv=inv):
            rows = span(c * FWD_ROWS, FWD_ROWS)
            if k == 0:
                y_val = dot_nt(dx_out[span(row_base + c * FWD_ROWS, FWD_ROWS), :], wbuf[0]) * inv
                y0[rows, :] = y_val
                x1[rows, :] = leaky(y_val)
            elif k == 1:
                y_val = dot_nt(x1[rows, :], wbuf[1]) * inv
                y1[rows, :] = y_val
                x2[rows, :] = leaky(y_val)
            else:
                last_layer(rows, xstat)
                add_grad(acc.at[2], e2[rows, own_cols], x2[rows, :])
            return carry

        lax.fori_loop(0, rows_own // FWD_ROWS, forward, 0)

    def d_copy(k):
        return remote(acc.at[k, 1 - core], rbuf.at[k], d_send, d_recv.at[k], p_sib)

    def fd_copy(k):
        return remote(fsend.at[k], frbuf.at[k], d_send, d_recv.at[4], p_sib)

    def p_copy(k):
        part = pl.ds((PAIR, 0, LANE)[k], (8, LANE, LANE)[k])
        return remote(p_own.at[part], p_other.at[part], d_send, d_recv.at[5], p_y)

    s_copy = remote(sstat, rstat, d_send, d_recv.at[3], p_sib)
    fs_copy = remote(fsstat, frstat, d_send, d_recv.at[6], p_sib)
    g_copy = remote(g_own, g_other, d_send, d_recv.at[7], p_y)

    def dx_copy(at, size):
        ref = dx_out.at[tile(row_base + at, size)]
        return remote(ref, ref, d_send, e_recv, p_sib)

    def backward(at, size, sums, grads, idx=None, mid=None, split=False):
        rows = tile(at, size)
        b0, b1 = (eq.at[0], eq.at[1]) if split else (e0, e1)
        for j in range(2):
            residual(y2[rows, LANE * j:LANE * j + LANE], 2 - 2 * chip + j, rows)
        back = (dot_nn(e2[rows, :], wbuf[2]) * inv_sigma[2]).astype(BF16).astype(F32)
        y_val = y1[rows, :]
        grad = back * jnp.where(y_val > 0, 1.0, 0.2)
        sums[0] += fold(grad * y_val)
        b1[:size] = grad.astype(BF16)
        if split:
            grads[1, core] += dot_tn(b1[:size, my_cols], x1[rows, :])
        else:
            add_grad(grads.at[1], b1[:size, own_cols], x1[rows, :])
        back = (dot_nn(b1[:size], wbuf[1]) * inv_sigma[1]).astype(BF16).astype(F32)
        if mid is not None:
            mid(1)
        y_val = y0[rows, :]
        grad = back * jnp.where(y_val > 0, 1.0, 0.2)
        sums[1] += fold(grad * y_val)
        b0[:size] = grad.astype(BF16)
        if idx is None:
            add_grad(grads.at[0], b0[:size, own_cols], xfor[tile(at - rows_own, size), :])
            if mid is not None:
                mid(0)
        else:
            x_rows = tile(row_base + at, size)
            if split:
                grads[0, core] += dot_tn(b0[:size, my_cols], dx_out[x_rows, :])
                mid(0)
            else:
                add_grad(grads.at[0], b0[:size, own_cols], dx_out[x_rows, :])
            dx_out[x_rows, :] = (dot_nn(b0[:size], wbuf[0]) * inv_sigma[0]).astype(BF16)

    row = lax.broadcasted_iota(jnp.int32, sstat.shape, 0)

    def gather_sums(ref_sums):
        mine = jnp.zeros(sstat.shape, F32)
        for i in range(2):
            mine = jnp.where(row == 2 + i, jnp.sum(ref_sums(i), axis=0, keepdims=True), mine)
        return mine

    first_sums = [jnp.sum(xstat[i], axis=0, keepdims=True) for i in range(2)]
    xb[0] = jnp.where(row[:, :LANE] == 0, first_sums[0], jnp.where(row[:, :LANE] == 1, first_sums[1], 0.0))

    def x_copy(k):
        return remote(xb.at[2 * k], xb.at[2 * k + 1], x_send, x_recv.at[k], (p_sib, p_y, p_cnt)[k])

    def own_chunk(idx, at, size, sums, grads, mid=None, split=False):
        arrived(tbuf.at[pl.ds(0, 2), tile(at, size)], t_recv.at[idx])
        if isinstance(idx, int) and idx == N_PLAIN:
            p_copy(2).start()
        backward(at, size, sums, grads, idx, mid, split)

    n_big = PLAIN[0][1]

    def plain_send(k):
        q_copy(k).start()

    def plain_chunk(idx, at, size):
        if size == BIG_ROWS:
            @pl.when(idx == 0)
            def _():
                d_copy(2).start()
                q_copy(2).start()
                x_copy(0).start()

            @pl.when(idx == 1)
            def _():
                d_copy(2).wait_recv()
                g_own[...] = acc[2, core] + rbuf[2]
                x_copy(0).wait_recv()
                xb[2] = xb[0] + xb[1]

            @pl.when(idx == 2)
            def _():
                g_copy.start()
                x_copy(1).start()

            @pl.when(idx == n_big - 2)
            def _():
                arrived(x1.at[pl.ds(0, 3 * SHARED_ROWS // 2)], f_recv)

                def forward_on(j, h_at, h_size):
                    h_copy(0, j, h_at, h_size).start()
                    h_copy(1, j, h_at, h_size).start()

                each_chunk(SHARED, 0, rows_own, forward_on)

            @pl.when(idx == n_big - 1)
            def _():
                rows = pl.ds(rows_own, SHARED_ROWS)
                y_val = dot_nt(xfor[...], wbuf[0]) * inv_sigma[0]
                y0[rows, :] = y_val
                x1[rows, :] = leaky(y_val)
                y_val = dot_nt(x1[rows, :], wbuf[1]) * inv_sigma[1]
                y1[rows, :] = y_val
                x2[rows, :] = leaky(y_val)
                last_layer(rows, None)

        if isinstance(idx, int) and idx == n_big:
            x_copy(1).wait_recv()
            xb[4] = xb[2] + xb[3]
        last = idx == N_PLAIN - 1 if isinstance(idx, int) else False
        own_chunk(idx, at, size, stat, acc, plain_send if last else None, last)
        if isinstance(idx, int) and idx == N_PLAIN - 2:
            d_copy(1).start()
            d_copy(0).start()
            x_copy(2).start()
        dx_copy(at, size).start()

    each_chunk(PLAIN, 0, 0, plain_chunk)

    d_copy(1).wait_recv()
    q_copy(2).wait_recv()
    q_copy(1).wait_recv()
    p_own[0:LANE, :] = (acc[1, core] + rbuf[1]) + dot_tn(se[1], sx[1])
    sstat[...] = gather_sums(lambda i: stat[i])
    s_copy.start()
    p_copy(1).start()
    d_copy(0).wait_recv()
    local_q.wait()
    q_copy(0).wait_recv()
    p_own[LANE:PAIR, :] = (acc[0, core] + rbuf[0]) + dot_tn(se[0], sx[0])

    def shared_chunk(idx, at, size):
        if idx == N_PLAIN + 1:
            p_copy(0).start()
        own_chunk(idx, at, size, fstat.at[0], facc.at[0])
        dx_copy(at, size).start()
        if idx == N_PLAIN:
            s_copy.wait_recv()
            p_own[PAIR:264, :] = sstat[...] + rstat[...]

    each_chunk(SHARED, N_PLAIN, shared_at, shared_chunk)

    def last_send(k):
        fsend[k] = facc[0, k, 1 - core] + facc[1, k, 1 - core]
        if k == 1:
            fd_copy(1).start()
        if k == 0:
            fsstat[...] = gather_sums(lambda i: fstat[0, i] + fstat[1, i])
            fd_copy(0).start()
            fs_copy.start()

    def foreign_chunk(idx, at, size):
        arrived(tbuf.at[pl.ds(0, 2), tile(at, size)], h_recv.at[idx])
        last = isinstance(at, int) and at + size == rows_own + SHARED_ROWS
        backward(at, size, fstat.at[1], facc.at[1], None, last_send if last else None)

    each_chunk(SHARED, 0, rows_own, foreign_chunk)

    g_copy.wait_recv()
    tot_out[PAIR:384, :] = g_own[...] + g_other[...]
    arrived(p_other, d_recv.at[5])
    arrived(frbuf, d_recv.at[4])
    for i, k in enumerate((1, 0)):
        part = slice(LANE * i, LANE * i + LANE)
        tot_out[part, :] = (p_own[part, :] + p_other[part, :]) + ((facc[0, k, core] + facc[1, k, core]) + frbuf[k])
    fs_copy.wait_recv()
    tot_out[384:392, :] = (p_own[PAIR:264, :] + p_other[PAIR:264, :]) + (fsstat[...] + frstat[...])
    x_copy(2).wait_recv()
    tot_out[384:392, :LANE] += xb[4] + xb[5]

    sent_rows = 3 * 384 + 2 * SHARED_ROWS + 3 * LAST // 2 + 3 * rows_own // 4
    arrived(dx_out.at[pl.ds(0, sent_rows)], w_send)
    arrived(ubuf.at[:, pl.ds(0, 3)], u_send)
    arrived(dx_out.at[pl.ds(0, rows_own + 2 * (8 * LANE + 24))], d_send)
    arrived(xb.at[pl.ds(0, 3)], x_send)
    arrived(dx_out.at[own_rows], e_recv)


def finish_kernel(loss_scale, dx_in, tot, pack, dx_ref, dw0, dw1, dw2, v0, v1, v2, n0, n1, n2, sig_out, loss_out,
                  grads, sig_row, loss_row, sems, out_sems):
    parts = sems.shape[0]
    rows = dx_in.shape[0] // parts
    copies = [pltpu.make_async_copy(dx_in.at[pl.ds(i * rows, rows)], dx_ref.at[pl.ds(i * rows, rows)], sems.at[i]) for i in range(parts)]
    for copy in copies:
        copy.start()

    def out_copy(src, dst):
        copy = pltpu.make_async_copy(src, dst, out_sems.at[len(copies) - parts])
        copy.start()
        copies.append(copy)

    for k, (v_out, n_out) in enumerate(((v0, n0), (v1, n1), (v2, n2))):
        out_copy(pack.at[k:k + 1, :], v_out)
        out_copy(pack.at[3 + k:4 + k, 0:LANE], n_out)
    lane = lax.broadcasted_iota(jnp.int32, (1, LANE), 1)
    row = jnp.where(lane == 0, pack[6:7, 0:LANE], jnp.where(lane == 1, pack[7:8, 0:LANE], pack[8:9, 0:LANE]))
    sig_row[...] = row[:, :3]
    stats = jnp.sum(tot[384:392, :], axis=1, keepdims=True)
    loss_row[...] = loss_scale * stats[0:1]
    for k, at in enumerate((LANE, 0, PAIR)):
        inv = 1.0 / pack[6 + k:7 + k, 0:1]
        u_col = jnp.transpose(jnp.broadcast_to(pack[3 + k:4 + k, 0:LANE], (LANE, LANE)))[:, 0:1]
        grads[k] = tot[at:at + LANE, :] * inv - (stats[3 - k:4 - k] * inv) * (u_col * pack[k:k + 1, :])
    out_copy(sig_row, sig_out)
    out_copy(loss_row, loss_out)
    for k, out in enumerate((dw0, dw1, dw2)):
        out_copy(grads.at[k], out)
    for copy in copies:
        copy.wait()


def solution(mesh):
    data_size = mesh.shape["data"]
    row_spec = P(("replica", "model"), None)
    vec_spec = P(("replica", "model"))
    batch_spec = P(("replica", "data"), None)
    target_spec = P(("replica", "data"), "model")
    part_spec = P("replica")

    def local_step(x_in, w_in, w_mid, w_out, u_in, u_mid, u_out, target):
        rows, width = x_in.shape
        half = rows // 2
        ext = half + SHARED_ROWS
        batch_total = rows * data_size
        any_spec = pl.BlockSpec(memory_space=pl.ANY)
        vmem_spec = pl.BlockSpec(memory_space=pltpu.VMEM)
        dma = pltpu.SemaphoreType.DMA
        vm = pltpu.VMEM
        dx_all, tot, pack = pl.pallas_call(
            functools.partial(main_kernel, 1.0 / batch_total),
            out_shape=[vm((rows, width), BF16), vm((392, width), F32), vm((16, width), F32)],
            in_specs=[any_spec] * 8,
            out_specs=[vmem_spec] * 3,
            scratch_shapes=[
                vm((ext, width), BF16), vm((ext, width), BF16),
                vm((ext, width), F32), vm((ext, width), F32), vm((ext, PAIR), F32),
                vm((4, ext, LANE), BF16),
                vm((3, width, width), BF16),
                vm((3, 4, 1, LANE), F32),
                vm((ext, width), BF16), vm((BIG_ROWS, width), BF16), vm((BIG_ROWS, width), BF16),
                vm((SHARED_ROWS, width), BF16),
                vm((3, 2, LANE, width), F32), vm((2, 2, 2, LANE, width), F32),
                vm((3, LANE, width), F32), vm((2, LANE, width), F32), vm((2, LANE, width), F32),
                vm((LANE, width), F32), vm((LANE, width), F32),
                vm((264, width), F32), vm((264, width), F32),
                vm((2, 8, width), F32), vm((2, 2, 8, width), F32),
                vm((8, width), F32), vm((8, width), F32), vm((8, width), F32), vm((8, width), F32),
                vm((3, 8, width), F32),
                vm((2, LAST, width), BF16), vm((2, LAST, LANE), BF16), vm((2, LAST, width), BF16),
                vm((2, 8, LANE), F32), vm((6, 8, LANE), F32),
                dma(()), dma((3, 3)), dma(()), dma(()),
                dma((N_PLAIN + N_SHARED,)), dma(()), dma(()), dma(()), dma((8,)),
                dma(()), dma((N_SHARED,)), dma((3,)), dma(()), dma((3,)),
                dma(()), dma(()), dma(()), dma(()),
            ],
            compiler_params=pltpu.CompilerParams(
                collective_id=0, has_side_effects=True, vmem_limit_bytes=55 * 2**20),
            name="fused_step",
        )(x_in, w_in, w_mid, w_out, u_in.reshape(1, LANE), u_mid.reshape(1, LANE), u_out.reshape(1, LANE), target)

        f32 = lambda *shape: jax.ShapeDtypeStruct(shape, F32)
        finals = pl.pallas_call(
            functools.partial(finish_kernel, 0.5 / batch_total),
            out_shape=[jax.ShapeDtypeStruct((rows, width), BF16)] + [f32(LANE, width)] * 3 + [f32(1, width)] * 3 + [
                f32(1, LANE)] * 3 + [f32(1, 3), f32(1, 1)],
            in_specs=[vmem_spec] * 3,
            out_specs=[any_spec] * 12,
            scratch_shapes=[vm((3, LANE, width), F32), vm((1, 3), F32), vm((1, 1), F32), dma((4,)), dma((11,))],
            compiler_params=pltpu.CompilerParams(vmem_limit_bytes=8 * 2**20),
            name="finish",
        )(dx_all, tot, pack)
        grad_x, dw0, dw1, dw2, v0, v1, v2, n0, n1, n2, sig, loss = finals
        return (loss.reshape(1), grad_x, dw0, dw1, dw2, n0.reshape(LANE), n1.reshape(LANE), n2.reshape(LANE),
                v0.reshape(width), v1.reshape(width), v2.reshape(width), sig.reshape(3))

    in_specs = (batch_spec, row_spec, row_spec, row_spec, vec_spec, vec_spec, vec_spec, target_spec)
    out_specs = (part_spec, batch_spec, row_spec, row_spec, row_spec, vec_spec, vec_spec, vec_spec, part_spec, part_spec, part_spec, part_spec)
    return jax.shard_map(local_step, mesh=mesh, in_specs=in_specs, out_specs=out_specs, check_vma=False)
```

```python
import functools

import jax
import jax.numpy as jnp
from jax import lax
from jax.experimental import pallas as pl
from jax.experimental.pallas import tpu as pltpu
from jax.sharding import PartitionSpec as P

MESH = pl.DeviceIdType.MESH
F32 = jnp.float32
BF16 = jnp.bfloat16
LANE = 128
PAIR = 2 * LANE
FWD_ROWS = 1024
BIG_ROWS = 512
PLAIN = ((512, 6), (256, 1), (192, 1))
SHARED = ((256, 1), (192, 1), (128, 1))
SHARED_ROWS = sum(size * count for size, count in SHARED)
N_PLAIN = sum(count for _, count in PLAIN)
LAST = PLAIN[-1][0]
N_SHARED = sum(count for _, count in SHARED)


def dot_nt(lhs, rhs):
    return lax.dot_general(lhs, rhs, (((1,), (1,)), ((), ())), preferred_element_type=F32)


def dot_nn(lhs, rhs):
    return lax.dot_general(lhs, rhs, (((1,), (0,)), ((), ())), preferred_element_type=F32)


def dot_tn(lhs, rhs):
    return lax.dot_general(lhs, rhs, (((0,), (0,)), ((), ())), preferred_element_type=F32)


def split_rows(vec):
    width = vec.shape[1]
    limit = float(jnp.finfo(BF16).max)
    high = jnp.clip(vec, -limit, limit).astype(BF16).astype(F32)
    rest = vec - high
    mid = rest.astype(BF16).astype(F32)
    low = rest - mid
    row = lax.broadcasted_iota(jnp.int32, (16, width), 0)
    stacked = jnp.where(row == 0, high, jnp.where(row == 1, mid, jnp.where(row == 2, low, 0.0)))
    return stacked.astype(BF16)


def main_kernel(inv_batch, x_hbm, w0_hbm, w1_hbm, w2_hbm, u0_hbm, u1_hbm, u2_hbm, t_hbm,
                dx_out, tot_out, pack_out,
                x1, x2, y0, y1, y2, tbuf, wbuf, ubuf, e2, e1, e0, xfor, acc, facc, rbuf, frbuf, fsend,
                g_own, g_other, p_own, p_other, stat, fstat, sstat, rstat, fsstat, frstat, srow, sx, se, eq, xstat, xb,
                w_send, w_recv, u_send, u_recv, t_recv, s_recv, e_recv, d_send, d_recv,
                f_recv, h_recv, q_recv, x_send, x_recv, l_w, l_u, l_x, l_q):
    rep, dat, mod = lax.axis_index("replica"), lax.axis_index("data"), lax.axis_index("model")
    core = lax.rem(mod, 2)
    chip = mod // 2
    sib = mod + 1 - 2 * core
    cnt = lax.rem(mod + 2, 4)
    crs = lax.rem(sib + 2, 4)
    p_sib, p_cnt, p_crs = (rep, dat, sib), (rep, dat, cnt), (rep, dat, crs)
    p_y, p_ys = (rep, 1 - dat, mod), (rep, 1 - dat, sib)
    rows_own = x_hbm.shape[0] // 2
    shared_at = rows_own - SHARED_ROWS
    row_base = core * rows_own

    def each_chunk(groups, first, at, body):
        for size, count in groups:
            def step(i, carry, size=size, first=first, at=at):
                body(first + i, at + i * size, size)
                return carry
            if count == 1:
                step(0, 0)
            else:
                lax.fori_loop(0, count, step, 0)
            first, at = first + count, at + size * count
    w_hbm = [w0_hbm, w1_hbm, w2_hbm]
    u_hbm = [u0_hbm, u1_hbm, u2_hbm]

    def remote(src, dst, ssem, rsem, peer):
        return pltpu.make_async_remote_copy(src_ref=src, dst_ref=dst, send_sem=ssem, recv_sem=rsem,
                                            device_id=peer, device_id_type=MESH)

    def arrived(ref, sem):
        pltpu.make_async_copy(ref, ref, sem).wait()

    def span(start, size):
        return pl.ds(pl.multiple_of(start, size), size)

    def tile(start, size):
        return pl.ds(pl.multiple_of(start, 64), size)

    def w_copy(layer, kind):
        ssem, rsem = w_send, w_recv.at[layer, (0, 1, 2, 0, 0)[kind]]
        if kind == 0:
            return remote(w_hbm[layer], wbuf.at[layer, span(LANE * mod, LANE)], ssem, rsem, p_sib)
        if kind == 1:
            return remote(w_hbm[layer].at[span(64 * dat, 64)], wbuf.at[layer, span(LANE * mod + 64 * dat, 64)], ssem, rsem, p_cnt)
        half = 1 - dat if kind == 4 else dat
        ref = wbuf.at[layer, span(LANE * cnt + 64 * half, 64)]
        return remote(ref, ref, ssem, rsem, p_y if kind == 2 else p_sib)

    def u_copy(kind):
        ref = ubuf.at[:, mod]
        return remote(ref, ref, u_send, u_recv, (p_sib, p_cnt, p_crs)[kind])

    def t_copy(kind, idx, at, size):
        other_core = core if kind == 0 else 1 - core
        return remote(t_hbm.at[tile(other_core * rows_own + at, size)], tbuf.at[mod, tile(at, size)],
                      w_send, t_recv.at[idx], p_cnt if kind == 0 else p_crs)

    def f_copy(kind):
        if kind == 0:
            src, dst, peer = x_hbm.at[tile(row_base + shared_at, SHARED_ROWS)], xfor, p_y
        else:
            other_core = core if kind == 1 else 1 - core
            src = t_hbm.at[tile(other_core * rows_own + shared_at, SHARED_ROWS)]
            dst, peer = tbuf.at[mod, tile(rows_own, SHARED_ROWS)], p_y if kind == 1 else p_ys
        return remote(src, dst, w_send, f_recv, peer)

    def h_copy(kind, idx, at, size):
        ref = tbuf.at[mod if kind == 0 else sib, tile(at, size)]
        return remote(ref, ref, w_send, h_recv.at[idx], p_cnt)

    barrier = pltpu.get_barrier_semaphore()
    peers = (p_sib, p_cnt, p_crs, p_y, p_ys)
    for peer in peers:
        pl.semaphore_signal(barrier, inc=1, device_id=peer, device_id_type=MESH)
    local_w = [pltpu.make_async_copy(w_hbm[k], wbuf.at[k, span(LANE * mod, LANE)], l_w) for k in range(3)]
    local_u = [pltpu.make_async_copy(u_hbm[k], ubuf.at[k, mod], l_u) for k in range(3)]
    own_rows = span(row_base, rows_own)
    local_x = pltpu.make_async_copy(x_hbm.at[own_rows], dx_out.at[own_rows], l_x)
    local_t = pltpu.make_async_copy(t_hbm.at[own_rows], tbuf.at[mod, pl.ds(0, rows_own)], s_recv)
    for k in range(3):
        local_w[k].start()
        local_u[k].start()
    local_x.start()
    local_t.start()
    last_at = shared_at - LAST
    local_q = pltpu.make_async_copy(x_hbm.at[tile((1 - core) * rows_own + last_at, LAST)], sx.at[0], l_q)
    local_q.start()
    pl.semaphore_wait(barrier, len(peers))

    for k in range(3):
        w_copy(k, 1).start()
        w_copy(k, 0).start()

    arrived(ubuf.at[:, mod], l_u)
    for kind in range(3):
        u_copy(kind).start()

    def start_targets(idx, at, size):
        t_copy(0, idx, at, size).start()
        t_copy(1, idx, at, size).start()

    each_chunk(PLAIN + SHARED, 0, 0, start_targets)
    t_sib = remote(t_hbm.at[span((1 - core) * rows_own, rows_own)], tbuf.at[mod, pl.ds(0, rows_own)], w_send, s_recv, p_sib)
    t_sib.start()
    acc[...] = jnp.zeros_like(acc)
    facc[...] = jnp.zeros_like(facc)
    stat[...] = jnp.zeros_like(stat)
    xstat[...] = jnp.zeros_like(xstat)
    fstat[...] = jnp.zeros_like(fstat)

    def relay_x(k):
        w_copy(k, 1).wait_recv()
        w_copy(k, 2).start()
        w_copy(k, 3).start()

    def relay_y(k):
        w_copy(k, 2).wait_recv()
        w_copy(k, 4).start()

    own_cols = span(PAIR * chip, PAIR)
    my_cols = span(LANE * mod, LANE)

    def q_copy(kind):
        if kind == 2:
            src, dst = x1.at[pl.ds(last_at, LAST)], sx.at[1]
        else:
            src, dst = eq.at[kind, :, span(LANE * sib, LANE)], se.at[kind]
        return remote(src, dst, w_send, q_recv.at[kind], p_sib)

    def fold(val):
        return jnp.sum(val.reshape(val.shape[0] // 8, 8, val.shape[1]), axis=0)

    def leaky(val):
        return jnp.maximum(val, 0.2 * val).astype(BF16)

    def add_grad(ref, e_val, x_val):
        part = dot_tn(e_val, x_val)
        ref[0] += part[:LANE]
        ref[1] += part[LANE:]

    def residual(y_val, slab, rows, sums=None):
        res = y_val - tbuf[slab, rows, :].astype(F32)
        grad = res * inv_batch
        if sums is not None:
            sums[0] += fold(res * res)
            sums[1] += fold(grad * y_val)
        e2[rows, span(LANE * slab, LANE)] = grad.astype(BF16)

    def last_layer(rows, sums):
        y_val = dot_nt(x2[rows, :], wbuf[2]) * inv_sigma[2]
        first = chip == 0
        own = jnp.where(first, y_val[:, :PAIR], y_val[:, PAIR:])
        y2[rows, :] = jnp.where(first, y_val[:, PAIR:], y_val[:, :PAIR])
        for j in range(2):
            residual(own[:, LANE * j:LANE * j + LANE], 2 * chip + j, rows, sums)

    inv_sigma = []
    for k in range(3):
        relay_x(k)
    for kind in range(3):
        f_copy(kind).start()
    relay_y(0)
    relay_y(1)
    for k in range(3):
        if k == 0:
            arrived(wbuf.at[:, span(LANE * mod, LANE)], l_w)
            arrived(ubuf.at[:, pl.ds(0, 3)], u_recv)
        arrived(wbuf.at[k, pl.ds(0, PAIR)], w_recv.at[k, 0])
        u_row = jnp.concatenate([ubuf[k, j] for j in range(4)], axis=1)
        p_vec = jnp.sum(dot_nn(split_rows(u_row), wbuf[k]), axis=0, keepdims=True)
        norm = jnp.sqrt(jnp.sum(p_vec * p_vec, axis=1, keepdims=True))
        v_vec = p_vec / jnp.maximum(norm, 1e-12)
        s_vec = jnp.sum(dot_nt(split_rows(v_vec), wbuf[k]), axis=0, keepdims=True)
        sigma = jnp.sqrt(jnp.sum(s_vec * s_vec, axis=1, keepdims=True))
        pack_out[k:k + 1, :] = v_vec
        srow[k] = jnp.broadcast_to(s_vec / sigma, srow.shape[1:])
        pack_out[3 + k:4 + k, 0:LANE] = srow[k, 0:1, span(LANE * mod, LANE)]
        pack_out[6 + k:7 + k, :] = jnp.broadcast_to(sigma, (1, pack_out.shape[1]))
        inv = 1.0 / sigma
        inv_sigma.append(inv)
        if k == 0:
            relay_y(2)
        if k == 0:
            local_x.wait()
        if k == 2:
            arrived(tbuf.at[pl.ds(0, 2), pl.ds(0, rows_own)], s_recv)

        def forward(c, carry, k=k, inv=inv):
            rows = span(c * FWD_ROWS, FWD_ROWS)
            if k == 0:
                y_val = dot_nt(dx_out[span(row_base + c * FWD_ROWS, FWD_ROWS), :], wbuf[0]) * inv
                y0[rows, :] = y_val
                x1[rows, :] = leaky(y_val)
            elif k == 1:
                y_val = dot_nt(x1[rows, :], wbuf[1]) * inv
                y1[rows, :] = y_val
                x2[rows, :] = leaky(y_val)
            else:
                last_layer(rows, xstat)
                add_grad(acc.at[2], e2[rows, own_cols], x2[rows, :])
            return carry

        lax.fori_loop(0, rows_own // FWD_ROWS, forward, 0)

    def d_copy(k):
        return remote(acc.at[k, 1 - core], rbuf.at[k], d_send, d_recv.at[k], p_sib)

    def fd_copy(k):
        return remote(fsend.at[k], frbuf.at[k], d_send, d_recv.at[4], p_sib)

    def p_copy(k):
        part = pl.ds((PAIR, 0, LANE)[k], (8, LANE, LANE)[k])
        return remote(p_own.at[part], p_other.at[part], d_send, d_recv.at[5], p_y)

    s_copy = remote(sstat, rstat, d_send, d_recv.at[3], p_sib)
    fs_copy = remote(fsstat, frstat, d_send, d_recv.at[4], p_sib)
    g_copy = remote(g_own, g_other, d_send, d_recv.at[5], p_y)

    def dx_copy(at, size):
        ref = dx_out.at[tile(row_base + at, size)]
        return remote(ref, ref, d_send, e_recv, p_sib)

    def backward(at, size, sums, grads, idx=None, mid=None, split=False):
        rows = tile(at, size)
        b0, b1 = (eq.at[0], eq.at[1]) if split else (e0, e1)
        for j in range(2):
            residual(y2[rows, LANE * j:LANE * j + LANE], 2 - 2 * chip + j, rows)
        back = (dot_nn(e2[rows, :], wbuf[2]) * inv_sigma[2]).astype(BF16).astype(F32)
        y_val = y1[rows, :]
        grad = back * jnp.where(y_val > 0, 1.0, 0.2)
        sums[0] += fold(grad * y_val)
        b1[:size] = grad.astype(BF16)
        if split:
            grads[1, core] += dot_tn(b1[:size, my_cols], x1[rows, :])
        else:
            add_grad(grads.at[1], b1[:size, own_cols], x1[rows, :])
        back = (dot_nn(b1[:size], wbuf[1]) * inv_sigma[1]).astype(BF16).astype(F32)
        if mid is not None:
            mid(1)
        y_val = y0[rows, :]
        grad = back * jnp.where(y_val > 0, 1.0, 0.2)
        sums[1] += fold(grad * y_val)
        b0[:size] = grad.astype(BF16)
        if idx is None:
            add_grad(grads.at[0], b0[:size, own_cols], xfor[tile(at - rows_own, size), :])
            if mid is not None:
                mid(0)
        else:
            x_rows = tile(row_base + at, size)
            if split:
                grads[0, core] += dot_tn(b0[:size, my_cols], dx_out[x_rows, :])
                mid(0)
            else:
                add_grad(grads.at[0], b0[:size, own_cols], dx_out[x_rows, :])
            dx_out[x_rows, :] = (dot_nn(b0[:size], wbuf[0]) * inv_sigma[0]).astype(BF16)

    row = lax.broadcasted_iota(jnp.int32, sstat.shape, 0)

    def gather_sums(ref_sums):
        mine = jnp.zeros(sstat.shape, F32)
        for i in range(2):
            mine = jnp.where(row == 2 + i, jnp.sum(ref_sums(i), axis=0, keepdims=True), mine)
        return mine

    first_sums = [jnp.sum(xstat[i], axis=0, keepdims=True) for i in range(2)]
    xb[0] = jnp.where(row[:, :LANE] == 0, first_sums[0], jnp.where(row[:, :LANE] == 1, first_sums[1], 0.0))

    def x_copy(k):
        return remote(xb.at[2 * k], xb.at[2 * k + 1], x_send, x_recv.at[k], (p_sib, p_y, p_cnt)[k])

    def own_chunk(idx, at, size, sums, grads, mid=None, split=False):
        arrived(tbuf.at[pl.ds(0, 2), tile(at, size)], t_recv.at[idx])
        if isinstance(idx, int) and idx == N_PLAIN:
            p_copy(2).start()
        backward(at, size, sums, grads, idx, mid, split)

    n_big = PLAIN[0][1]

    def plain_send(k):
        q_copy(k).start()

    def plain_chunk(idx, at, size):
        if size == BIG_ROWS:
            @pl.when(idx == 0)
            def _():
                d_copy(2).start()
                q_copy(2).start()
                x_copy(0).start()

            @pl.when(idx == 1)
            def _():
                d_copy(2).wait_recv()
                g_own[...] = acc[2, core] + rbuf[2]
                x_copy(0).wait_recv()
                xb[2] = xb[0] + xb[1]

            @pl.when(idx == 2)
            def _():
                g_copy.start()
                x_copy(1).start()

            @pl.when(idx == n_big - 2)
            def _():
                arrived(x1.at[pl.ds(0, 3 * SHARED_ROWS // 2)], f_recv)

                def forward_on(j, h_at, h_size):
                    h_copy(0, j, h_at, h_size).start()
                    h_copy(1, j, h_at, h_size).start()

                each_chunk(SHARED, 0, rows_own, forward_on)

            @pl.when(idx == n_big - 1)
            def _():
                rows = pl.ds(rows_own, SHARED_ROWS)
                y_val = dot_nt(xfor[...], wbuf[0]) * inv_sigma[0]
                y0[rows, :] = y_val
                x1[rows, :] = leaky(y_val)
                y_val = dot_nt(x1[rows, :], wbuf[1]) * inv_sigma[1]
                y1[rows, :] = y_val
                x2[rows, :] = leaky(y_val)
                last_layer(rows, None)

        if isinstance(idx, int) and idx == n_big:
            x_copy(1).wait_recv()
            xb[4] = xb[2] + xb[3]
        last = idx == N_PLAIN - 1 if isinstance(idx, int) else False
        own_chunk(idx, at, size, stat, acc, plain_send if last else None, last)
        if isinstance(idx, int) and idx == N_PLAIN - 2:
            d_copy(1).start()
            d_copy(0).start()
            x_copy(2).start()
        dx_copy(at, size).start()

    each_chunk(PLAIN, 0, 0, plain_chunk)

    d_copy(1).wait_recv()
    q_copy(2).wait_recv()
    q_copy(1).wait_recv()
    p_own[0:LANE, :] = (acc[1, core] + rbuf[1]) + dot_tn(se[1], sx[1])
    sstat[...] = gather_sums(lambda i: stat[i])
    s_copy.start()
    p_copy(1).start()
    d_copy(0).wait_recv()
    local_q.wait()
    q_copy(0).wait_recv()
    p_own[LANE:PAIR, :] = (acc[0, core] + rbuf[0]) + dot_tn(se[0], sx[0])

    def shared_chunk(idx, at, size):
        if idx == N_PLAIN + 1:
            p_copy(0).start()
        own_chunk(idx, at, size, fstat.at[0], facc.at[0])
        dx_copy(at, size).start()
        if idx == N_PLAIN:
            s_copy.wait_recv()
            p_own[PAIR:264, :] = sstat[...] + rstat[...]

    each_chunk(SHARED, N_PLAIN, shared_at, shared_chunk)

    def last_send(k):
        fsend[k] = facc[0, k, 1 - core] + facc[1, k, 1 - core]
        if k == 1:
            fd_copy(1).start()
        if k == 0:
            fsstat[...] = gather_sums(lambda i: fstat[0, i] + fstat[1, i])
            fd_copy(0).start()
            fs_copy.start()

    def foreign_chunk(idx, at, size):
        arrived(tbuf.at[pl.ds(0, 2), tile(at, size)], h_recv.at[idx])
        last = isinstance(at, int) and at + size == rows_own + SHARED_ROWS
        backward(at, size, fstat.at[1], facc.at[1], None, last_send if last else None)

    each_chunk(SHARED, 0, rows_own, foreign_chunk)

    arrived(y0.at[pl.ds(0, 392)], d_recv.at[5])
    tot_out[PAIR:384, :] = g_own[...] + g_other[...]
    arrived(y0.at[pl.ds(0, 264)], d_recv.at[4])
    for i, k in enumerate((1, 0)):
        part = slice(LANE * i, LANE * i + LANE)
        tot_out[part, :] = (p_own[part, :] + p_other[part, :]) + ((facc[0, k, core] + facc[1, k, core]) + frbuf[k])
    tot_out[384:392, :] = (p_own[PAIR:264, :] + p_other[PAIR:264, :]) + (fsstat[...] + frstat[...])
    x_copy(2).wait_recv()
    tot_out[384:392, :LANE] += xb[4] + xb[5]

    sent_rows = 3 * 384 + 2 * SHARED_ROWS + 3 * LAST // 2 + 3 * rows_own // 4
    arrived(dx_out.at[pl.ds(0, sent_rows)], w_send)
    arrived(ubuf.at[:, pl.ds(0, 3)], u_send)
    arrived(dx_out.at[pl.ds(0, rows_own + 2 * (8 * LANE + 24))], d_send)
    arrived(xb.at[pl.ds(0, 3)], x_send)
    arrived(dx_out.at[own_rows], e_recv)


def finish_kernel(loss_scale, dx_in, tot, pack, dx_ref, dw0, dw1, dw2, v0, v1, v2, n0, n1, n2, sig_out, loss_out,
                  grads, sig_row, loss_row, sems, out_sems):
    parts = sems.shape[0]
    rows = dx_in.shape[0] // parts
    copies = [pltpu.make_async_copy(dx_in.at[pl.ds(i * rows, rows)], dx_ref.at[pl.ds(i * rows, rows)], sems.at[i]) for i in range(parts)]
    for copy in copies:
        copy.start()

    def out_copy(src, dst):
        copy = pltpu.make_async_copy(src, dst, out_sems.at[len(copies) - parts])
        copy.start()
        copies.append(copy)

    for k, (v_out, n_out) in enumerate(((v0, n0), (v1, n1), (v2, n2))):
        out_copy(pack.at[k:k + 1, :], v_out)
        out_copy(pack.at[3 + k:4 + k, 0:LANE], n_out)
    lane = lax.broadcasted_iota(jnp.int32, (1, LANE), 1)
    row = jnp.where(lane == 0, pack[6:7, 0:LANE], jnp.where(lane == 1, pack[7:8, 0:LANE], pack[8:9, 0:LANE]))
    sig_row[...] = row[:, :3]
    stats = jnp.sum(tot[384:392, :], axis=1, keepdims=True)
    loss_row[...] = loss_scale * stats[0:1]
    for k, at in enumerate((LANE, 0, PAIR)):
        inv = 1.0 / pack[6 + k:7 + k, 0:1]
        u_col = jnp.transpose(jnp.broadcast_to(pack[3 + k:4 + k, 0:LANE], (LANE, LANE)))[:, 0:1]
        grads[k] = tot[at:at + LANE, :] * inv - (stats[3 - k:4 - k] * inv) * (u_col * pack[k:k + 1, :])
    out_copy(sig_row, sig_out)
    out_copy(loss_row, loss_out)
    for k, out in enumerate((dw0, dw1, dw2)):
        out_copy(grads.at[k], out)
    for copy in copies:
        copy.wait()


def solution(mesh):
    data_size = mesh.shape["data"]
    row_spec = P(("replica", "model"), None)
    vec_spec = P(("replica", "model"))
    batch_spec = P(("replica", "data"), None)
    target_spec = P(("replica", "data"), "model")
    part_spec = P("replica")

    def local_step(x_in, w_in, w_mid, w_out, u_in, u_mid, u_out, target):
        rows, width = x_in.shape
        half = rows // 2
        ext = half + SHARED_ROWS
        batch_total = rows * data_size
        any_spec = pl.BlockSpec(memory_space=pl.ANY)
        vmem_spec = pl.BlockSpec(memory_space=pltpu.VMEM)
        dma = pltpu.SemaphoreType.DMA
        vm = pltpu.VMEM
        dx_all, tot, pack = pl.pallas_call(
            functools.partial(main_kernel, 1.0 / batch_total),
            out_shape=[vm((rows, width), BF16), vm((392, width), F32), vm((16, width), F32)],
            in_specs=[any_spec] * 8,
            out_specs=[vmem_spec] * 3,
            scratch_shapes=[
                vm((ext, width), BF16), vm((ext, width), BF16),
                vm((ext, width), F32), vm((ext, width), F32), vm((ext, PAIR), F32),
                vm((4, ext, LANE), BF16),
                vm((3, width, width), BF16),
                vm((3, 4, 1, LANE), F32),
                vm((ext, width), BF16), vm((BIG_ROWS, width), BF16), vm((BIG_ROWS, width), BF16),
                vm((SHARED_ROWS, width), BF16),
                vm((3, 2, LANE, width), F32), vm((2, 2, 2, LANE, width), F32),
                vm((3, LANE, width), F32), vm((2, LANE, width), F32), vm((2, LANE, width), F32),
                vm((LANE, width), F32), vm((LANE, width), F32),
                vm((264, width), F32), vm((264, width), F32),
                vm((2, 8, width), F32), vm((2, 2, 8, width), F32),
                vm((8, width), F32), vm((8, width), F32), vm((8, width), F32), vm((8, width), F32),
                vm((3, 8, width), F32),
                vm((2, LAST, width), BF16), vm((2, LAST, LANE), BF16), vm((2, LAST, width), BF16),
                vm((2, 8, LANE), F32), vm((6, 8, LANE), F32),
                dma(()), dma((3, 3)), dma(()), dma(()),
                dma((N_PLAIN + N_SHARED,)), dma(()), dma(()), dma(()), dma((6,)),
                dma(()), dma((N_SHARED,)), dma((3,)), dma(()), dma((3,)),
                dma(()), dma(()), dma(()), dma(()),
            ],
            compiler_params=pltpu.CompilerParams(
                collective_id=0, has_side_effects=True, vmem_limit_bytes=55 * 2**20),
            name="fused_step",
        )(x_in, w_in, w_mid, w_out, u_in.reshape(1, LANE), u_mid.reshape(1, LANE), u_out.reshape(1, LANE), target)

        f32 = lambda *shape: jax.ShapeDtypeStruct(shape, F32)
        finals = pl.pallas_call(
            functools.partial(finish_kernel, 0.5 / batch_total),
            out_shape=[jax.ShapeDtypeStruct((rows, width), BF16)] + [f32(LANE, width)] * 3 + [f32(1, width)] * 3 + [
                f32(1, LANE)] * 3 + [f32(1, 3), f32(1, 1)],
            in_specs=[vmem_spec] * 3,
            out_specs=[any_spec] * 12,
            scratch_shapes=[vm((3, LANE, width), F32), vm((1, 3), F32), vm((1, 1), F32), dma((4,)), dma((11,))],
            compiler_params=pltpu.CompilerParams(vmem_limit_bytes=8 * 2**20),
            name="finish",
        )(dx_all, tot, pack)
        grad_x, dw0, dw1, dw2, v0, v1, v2, n0, n1, n2, sig, loss = finals
        return (loss.reshape(1), grad_x, dw0, dw1, dw2, n0.reshape(LANE), n1.reshape(LANE), n2.reshape(LANE),
                v0.reshape(width), v1.reshape(width), v2.reshape(width), sig.reshape(3))

    in_specs = (batch_spec, row_spec, row_spec, row_spec, vec_spec, vec_spec, vec_spec, target_spec)
    out_specs = (part_spec, batch_spec, row_spec, row_spec, row_spec, vec_spec, vec_spec, vec_spec, part_spec, part_spec, part_spec, part_spec)
    return jax.shard_map(local_step, mesh=mesh, in_specs=in_specs, out_specs=out_specs, check_vma=False)
```
